512 devices in a mesh: bx: 16 (over y_hi, z), by: 32 (over x, y_lo, core).
Axes of the slice: x: 4, y: 8 (y_hi: 2, y_lo: 4; y = y_hi * 4 + y_lo), z: 8, core: 2. Of those that a mesh axis runs over, the one named last changes fastest.
Arguments:
- incident: float32 [2, 96, 16, 32, 128], P(None, None, 'bx', 'by'), may hold values from -6 to 6
- mie: float32 [2, 12, 16, 32, 128], P(None, None, 'bx', 'by'), may hold values from -1 to 1
- offsets: float32 [3, 16, 32, 128], P(None, 'bx', 'by'), may hold values from -1 to 1
- sphere_box: int32 [16, 32, 128], P('bx', 'by'), may hold values from 0 to 15
- near_table: bfloat16 [16, 2, 96, 96], replicated, may hold values from -0.078125 to 0.078125
- near_src: int32 [16, 32, 16, 256], P('bx', 'by'), may hold values from 0 to 1151
- near_dst: int32 [16, 32, 16, 256], P('bx', 'by'), may hold values from 0 to 127
- pattern: bfloat16 [2, 128, 96], replicated, may hold values from -0.84 to 0.84
- receive: bfloat16 [2, 96, 128], replicated, may hold values from -0.375 to 0.375
- leaf_transfer: float32 [32, 2, 128], replicated, may hold values from -0.15 to 0.15
- far_src: int32 [16, 32, 16, 24], P('bx', 'by'), may hold values from 0 to 143
- far_cls: int32 [16, 32, 16, 24], P('bx', 'by'), may hold values from 0 to 31
- coarse_transfer: float32 [2, 31, 63, 128], replicated, may hold values from -0.012 to 0.012
Outputs:
- solution: float32 [2, 96, 16, 32, 128], P(None, None, 'bx', 'by')
- residual: float32 [2, 96, 16, 32, 128], P(None, None, 'bx', 'by')
The draws below stay inside these ranges and needn't reach their ends.
All inputs are finite; a program needn't handle non-finite values.
Results may differ from the reference program's by a relative error of at most 0.0095.
Values may be sent and summed in bfloat16 or wider, within the bound.
No kernel may reach another device: no remote copies, remote signals or barrier semaphores. Data moves between devices by JAX's collectives and lax.ppermute only.
A program may use at most 64 MiB of HBM per device.

```python
import math
import jax
import jax.numpy as jnp
import numpy as np
from jax import lax

NCOEF = 96
MIE = 12
DIRS = 128
SPH_DEV = 128
LEAF_BOX = 16
NEAR_CLS = 16
PAIRS = 256
LIST_LEN = 24
LEAF_CLS = 32
ITERS = 2
GRID_X = 16
GRID_Y = 32
N_BX = 16
N_BY = 32


DECAY_BASE = 0.6


MIE_TOP = 0.8


def order_gains(coef_count):
    half_count = coef_count // 2
    degrees = np.array([math.isqrt(number % half_count + 1) for number in range(coef_count)])
    raw_gain = DECAY_BASE ** (degrees - 1)
    scale_fix = math.sqrt(half_count / float(np.sum(raw_gain[:half_count] ** 2)))
    return (raw_gain * scale_fix).astype(np.float32)


def draw_mie(key, part):
    size_key = jax.random.fold_in(key, 11)
    angle_key = jax.random.fold_in(key, 12)
    shape = (MIE, GRID_X, GRID_Y, SPH_DEV)
    power = jax.random.uniform(size_key, shape, jnp.float32, 0.0, 1.0)
    factor = 0.5 * jnp.exp(power * math.log(2.5))
    factor = jnp.clip(factor, 0.5, 1.25)
    orders = np.arange(MIE) % (MIE // 2)
    decay = jnp.asarray((MIE_TOP * DECAY_BASE ** orders).astype(np.float32)).reshape(MIE, 1, 1, 1)
    angle = jax.random.uniform(angle_key, shape, jnp.float32, -math.pi, math.pi)
    magnitude = decay * factor
    return jnp.stack([magnitude * jnp.cos(angle), magnitude * jnp.sin(angle)]).astype(jnp.float32)


def draw_pattern(key, part):
    entry_key = jax.random.fold_in(key, 21)
    shape = (2, DIRS, NCOEF)
    values = jnp.clip(jax.random.normal(entry_key, shape, jnp.float32), -3.0, 3.0)
    gains = jnp.asarray(order_gains(NCOEF)).reshape(1, 1, NCOEF)
    return (values * gains / math.sqrt(NCOEF)).astype(jnp.bfloat16)


def set_ends(values, stream_key, least, high):
    longest = values.shape.index(max(values.shape))
    spots = []
    for shift in (0, 1):
        where = [jax.random.randint(jax.random.fold_in(stream_key, axis), (), 0, length) for axis, length in enumerate(values.shape)]
        where[longest] = (where[longest] + shift) % values.shape[longest]
        spots.append(tuple(where))
    return values.at[spots[0]].set(least).at[spots[1]].set(high)


def block_scale(key, shape, shards, least, high):
    gain = 1.0
    for position, shards_of in shards:
        steps = jax.random.uniform(jax.random.fold_in(jax.random.fold_in(key, 6), position), (shards_of,), jnp.float32, least / len(shards), high / len(shards))
        gain = gain * jnp.repeat(jnp.exp(steps), shape[position] // shards_of).reshape((-1,) + (1,) * (len(shape) - 1 - position))
    return gain


def noise(rng, shape, width, limit, pieces=(), held_as=jnp.bfloat16):
    values = jax.random.normal(rng, shape, jnp.float32) * width
    if len(pieces) > 0:
        values = block_scale(rng, shape, pieces, -0.22, 0.18) * values
    return jnp.clip(values, min=-limit, max=limit).astype(held_as)


def setup_inputs(seed: int = 0) -> dict:
    streams_of = jax.random.split(jax.random.key(seed), 14)
    incident = noise(streams_of[0], (2, NCOEF, GRID_X, GRID_Y, SPH_DEV), 1.0, 6.0, ((2, 16), (3, 32)), jnp.float32)
    mie = draw_mie(jax.random.fold_in(streams_of[13], 71), 0)
    offsets = jnp.clip(jax.random.uniform(streams_of[2], (3, GRID_X, GRID_Y, SPH_DEV), jnp.float32, -1.0, 1.0) * block_scale(streams_of[2], (3, GRID_X, GRID_Y, SPH_DEV), ((1, 16), (2, 32)), -0.4, 0.0), -1.0, 1.0)
    sphere_box = set_ends(jax.random.randint(streams_of[3], (GRID_X, GRID_Y, SPH_DEV), 0, LEAF_BOX), jax.random.fold_in(streams_of[3], 1), 0, LEAF_BOX - 1).astype(jnp.int32)
    near_table = noise(streams_of[4], (NEAR_CLS, 2, NCOEF, NCOEF), (2 * NCOEF * NEAR_CLS * PAIRS // SPH_DEV) ** -0.5, 0.078125)
    near_src = set_ends(jax.random.randint(streams_of[5], (GRID_X, GRID_Y, NEAR_CLS, PAIRS), 0, 9 * SPH_DEV), jax.random.fold_in(streams_of[5], 1), 0, (9 * SPH_DEV) - 1).astype(jnp.int32)
    near_dst = set_ends(jax.random.randint(streams_of[6], (GRID_X, GRID_Y, NEAR_CLS, PAIRS), 0, SPH_DEV), jax.random.fold_in(streams_of[6], 1), 0, SPH_DEV - 1).astype(jnp.int32)
    pattern = draw_pattern(jax.random.fold_in(streams_of[13], 71), 0)
    receive = noise(streams_of[8], (2, NCOEF, DIRS), (2 * DIRS) ** -0.5, 0.375)
    leaf_transfer = noise(streams_of[9], (LEAF_CLS, 2, DIRS), 0.025, 0.15, (), jnp.float32)
    far_src = set_ends(jax.random.randint(streams_of[10], (GRID_X, GRID_Y, LEAF_BOX, LIST_LEN), 0, 9 * LEAF_BOX), jax.random.fold_in(streams_of[10], 1), 0, (9 * LEAF_BOX) - 1).astype(jnp.int32)
    far_cls = set_ends(jax.random.randint(streams_of[11], (GRID_X, GRID_Y, LEAF_BOX, LIST_LEN), 0, LEAF_CLS), jax.random.fold_in(streams_of[11], 1), 0, LEAF_CLS - 1).astype(jnp.int32)
    coarse_transfer = noise(streams_of[12], (2, 2 * GRID_X - 1, 2 * GRID_Y - 1, DIRS), 0.002, 0.012, (), jnp.float32)
    return {"incident": incident, "mie": mie, "offsets": offsets, "sphere_box": sphere_box, "near_table": near_table, "near_src": near_src, "near_dst": near_dst, "pattern": pattern, "receive": receive, "leaf_transfer": leaf_transfer, "far_src": far_src, "far_cls": far_cls, "coarse_transfer": coarse_transfer}


HIGHEST = lax.Precision.HIGHEST
KAPPA = 1.5
GOLDEN = 2.399963229728653

def int_starts(values):
    return tuple((jnp.asarray(value).astype(jnp.int32) for value in values))

def directions(number):
    ordinal = jnp.arange(number).astype(jnp.float32)
    height = 1.0 - (2.0 * ordinal + 1.0) / number
    radius = jnp.sqrt(1.0 - height * height)
    return jnp.stack([radius * jnp.cos(GOLDEN * ordinal), radius * jnp.sin(GOLDEN * ordinal), height])

def leaf_centers(number):
    ordinal = jnp.arange(number, dtype=jnp.int32)
    first_c = 2.0 * (ordinal % 2).astype(jnp.float32) - 1.0
    second_c = 2.0 * (ordinal // 2 % 2).astype(jnp.float32) - 1.0
    third_c = 2.0 * (ordinal // 4).astype(jnp.float32) - (number // 4 - 1)
    return jnp.stack([first_c, second_c, third_c])

def mie_spread(coef_count, mie_count):
    half_count = coef_count // 2
    table = np.zeros((coef_count, mie_count), np.float32)
    for number in range(coef_count):
        within = number % half_count
        degree = math.isqrt(within + 1)
        table[number, number // half_count * (mie_count // 2) + degree - 1] = 1.0
    return table

def complex_block(matrix):
    real_part = matrix[..., 0, :, :]
    imag_part = matrix[..., 1, :, :]
    upper = jnp.concatenate([real_part, -imag_part], axis=-1)
    bottom = jnp.concatenate([imag_part, real_part], axis=-1)
    return jnp.concatenate([upper, bottom], axis=-2)

def rotate(real_part, imag_part, cosines, sine_vals):
    return (real_part * cosines - imag_part * sine_vals, real_part * sine_vals + imag_part * cosines)

def far_mask(first_pos, second_pos, across_x, across_y):
    ordinal = jnp.arange(across_x * across_y, dtype=jnp.int32)
    apart_x = jnp.abs(ordinal // across_y - first_pos)
    apart_y = jnp.abs(ordinal % across_y - second_pos)
    return ((apart_x >= 2) | (apart_y >= 2)).astype(jnp.float32)

def small_solve(normal, rhs_vec, size_count):
    lower_tri = jnp.linalg.cholesky(normal)
    middle = []
    for row_num in range(size_count):
        accum = rhs_vec[row_num]
        for col_num in range(row_num):
            accum = accum - lower_tri[row_num, col_num] * middle[col_num]
        middle.append(accum / lower_tri[row_num, row_num])
    weights = [None] * size_count
    for row_num in reversed(range(size_count)):
        accum = middle[row_num]
        for col_num in range(row_num + 1, size_count):
            accum = accum - lower_tri[col_num, row_num] * weights[col_num]
        weights[row_num] = accum / lower_tri[row_num, row_num]
    return weights

def reference(incident, mie, offsets, sphere_box, near_table, near_src, near_dst, pattern, receive, leaf_transfer, far_src, far_cls, coarse_transfer):
    total_cols = N_BX * N_BY
    block_rows = 2 * NCOEF
    flat_len = total_cols * SPH_DEV
    blocks = complex_block(near_table).astype(jnp.float32)
    send_block = complex_block(pattern)
    take_block = complex_block(receive)
    planes = directions(DIRS)
    phases = KAPPA * jnp.dot(planes.T, offsets.reshape(3, flat_len), precision=HIGHEST)
    cos_sphere, sin_sphere = (jnp.cos(phases), jnp.sin(phases))
    centre = KAPPA * jnp.dot(planes.T, leaf_centers(LEAF_BOX), precision=HIGHEST)
    cos_leaf, sin_leaf = (jnp.cos(centre), jnp.sin(centre))
    member = (sphere_box.reshape(total_cols, 1, SPH_DEV) == jnp.arange(LEAF_BOX, dtype=jnp.int32).reshape(1, LEAF_BOX, 1)).astype(jnp.float32)
    mie_full = jnp.einsum('nk,rks->rns', jnp.asarray(mie_spread(NCOEF, MIE)), mie.reshape(2, MIE, flat_len), precision=HIGHEST)
    cols_index = jnp.arange(total_cols, dtype=jnp.int32)

    def apply_operator(vector):
        rounded = vector.astype(jnp.bfloat16)
        padded = jnp.pad(rounded, ((0, 0), (0, 0), (1, 1), (1, 1), (0, 0)))

        def near_one(item):
            column, sources, targets = item
            first_pos, second_pos = (column // N_BY, column % N_BY)
            window = lax.dynamic_slice(padded, int_starts((0, 0, first_pos, second_pos, 0)), (2, NCOEF, 3, 3, SPH_DEV)).reshape(block_rows, 9 * SPH_DEV)
            picked = jnp.take(window, sources.reshape(-1), axis=1).reshape(block_rows, NEAR_CLS, PAIRS).astype(jnp.float32)
            contrib = jnp.einsum('kab,bkm->akm', blocks, picked, precision=HIGHEST)
            return jnp.zeros((block_rows, SPH_DEV), jnp.float32).at[:, targets.reshape(-1)].add(contrib.reshape(block_rows, NEAR_CLS * PAIRS))
        near = lax.map(near_one, (cols_index, near_src.reshape(total_cols, NEAR_CLS, PAIRS), near_dst.reshape(total_cols, NEAR_CLS, PAIRS)))
        near = near.transpose(1, 0, 2).reshape(block_rows, flat_len)
        signature = jnp.dot(send_block.astype(jnp.float32), rounded.reshape(block_rows, flat_len).astype(jnp.float32), preferred_element_type=jnp.float32)
        out_real, out_imag = rotate(signature[:DIRS], signature[DIRS:], cos_sphere, -sin_sphere)
        outgoing = jnp.concatenate([out_real, out_imag]).reshape(2 * DIRS, total_cols, SPH_DEV)
        leaf_out = jnp.einsum('rds,dbs->rdb', outgoing, member, precision=HIGHEST)
        leaf_pad = jnp.pad(leaf_out.reshape(2, DIRS, N_BX, N_BY, LEAF_BOX), ((0, 0), (0, 0), (1, 1), (1, 1), (0, 0)))

        def leaf_one(item):
            column, sources, classes = item
            first_pos, second_pos = (column // N_BY, column % N_BY)
            window = lax.dynamic_slice(leaf_pad, int_starts((0, 0, first_pos, second_pos, 0)), (2, DIRS, 3, 3, LEAF_BOX)).reshape(2, DIRS, 9 * LEAF_BOX)
            picked = jnp.take(window, sources.reshape(-1), axis=2)
            class_hot = (jnp.arange(LEAF_CLS, dtype=jnp.int32)[:, None] == classes.reshape(1, -1)).astype(jnp.float32)
            chosen = jnp.dot(leaf_transfer.reshape(LEAF_CLS, 2 * DIRS).T, class_hot, precision=HIGHEST).reshape(2, DIRS, LEAF_BOX * LIST_LEN)
            prod_real, prod_imag = rotate(picked[0], picked[1], chosen[0], chosen[1])
            return jnp.stack([prod_real, prod_imag]).reshape(2, DIRS, LEAF_BOX, LIST_LEN).sum(axis=3)
        leaf_in = lax.map(leaf_one, (cols_index, far_src.reshape(total_cols, LEAF_BOX, LIST_LEN), far_cls.reshape(total_cols, LEAF_BOX, LIST_LEN)))
        up_real, up_imag = rotate(leaf_out[:DIRS], leaf_out[DIRS:], cos_leaf[:, None, :], -sin_leaf[:, None, :])
        column_out = jnp.stack([up_real.sum(axis=2), up_imag.sum(axis=2)])

        def coarse_one(column):
            first_pos, second_pos = (column // N_BY, column % N_BY)
            window = lax.dynamic_slice(coarse_transfer, int_starts((0, N_BX - 1 - first_pos, N_BY - 1 - second_pos, 0)), (2, N_BX, N_BY, DIRS)).reshape(2, total_cols, DIRS)
            window = window.transpose(0, 2, 1) * far_mask(first_pos, second_pos, N_BX, N_BY)
            prod_real, prod_imag = rotate(column_out[0], column_out[1], window[0], window[1])
            return jnp.stack([prod_real.sum(axis=1), prod_imag.sum(axis=1)])
        column_in = lax.map(coarse_one, cols_index)
        down_real, down_imag = rotate(column_in[:, 0, :, None], column_in[:, 1, :, None], cos_leaf[None], sin_leaf[None])
        incoming = leaf_in + jnp.stack([down_real, down_imag], axis=1)
        spread = jnp.einsum('dxqb,dbs->xqds', incoming, member, precision=HIGHEST).reshape(2, DIRS, flat_len)
        in_real, in_imag = rotate(spread[0], spread[1], cos_sphere, sin_sphere)
        arriving = jnp.concatenate([in_real, in_imag]).astype(jnp.bfloat16)
        far = jnp.dot(take_block.astype(jnp.float32), arriving.astype(jnp.float32), preferred_element_type=jnp.float32)
        field_sum = near + far
        source = vector.reshape(2, NCOEF, flat_len)
        prod_real, prod_imag = rotate(field_sum[:NCOEF], field_sum[NCOEF:], mie_full[0], mie_full[1])
        return jnp.stack([source[0] - prod_real, source[1] - prod_imag]).reshape(vector.shape)
    beta_norm = jnp.sqrt(jnp.sum(incident * incident))
    basis_list = [incident / beta_norm]
    hess_mat = jnp.zeros((ITERS + 1, ITERS), jnp.float32)
    for col_num in range(ITERS):
        krylov_vec = apply_operator(basis_list[col_num])
        heights = [jnp.sum(krylov_vec * basis_item) for basis_item in basis_list]
        for row_num in range(col_num + 1):
            krylov_vec = krylov_vec - heights[row_num] * basis_list[row_num]
            hess_mat = hess_mat.at[row_num, col_num].set(heights[row_num])
        length = jnp.sqrt(jnp.sum(krylov_vec * krylov_vec))
        hess_mat = hess_mat.at[col_num + 1, col_num].set(length)
        basis_list.append(krylov_vec / length)
    normal = jnp.dot(hess_mat.T, hess_mat, precision=HIGHEST)
    weights = small_solve(normal, beta_norm * hess_mat[0], ITERS)
    solution = jnp.zeros_like(incident)
    for col_num in range(ITERS):
        solution = solution + weights[col_num] * basis_list[col_num]
    fitted = jnp.dot(hess_mat, jnp.stack(weights), precision=HIGHEST)
    residual = beta_norm * basis_list[0]
    for row_num in range(ITERS + 1):
        residual = residual - fitted[row_num] * basis_list[row_num]
    return (solution, residual)
```

```python
import functools
import math

import jax
import jax.numpy as jnp
import numpy as np
from jax import lax
from jax.experimental import pallas as pl
from jax.experimental.pallas import tpu as pltpu
from jax.sharding import Mesh
from jax.sharding import PartitionSpec as P

BX = ("bx_0", "bx_1")
BY = ("by_0", "by_1", "by_2")
FIRST = ("bx_0", "by_1", "by_2")
SECOND = ("bx_1", "by_0")

HIGHEST = lax.Precision.HIGHEST
KAPPA = 1.5
GOLDEN = 2.399963229728653
F32 = jnp.float32
BF16 = jnp.bfloat16
NT = (((1,), (1,)), ((), ()))
TN = (((0,), (0,)), ((), ()))
INTERPRET = False


def call(kernel, out_shape, operands, name, flops=0, **kw):
    if not kw.get("grid") and not kw.get("grid_spec"):
        kw["in_specs"] = [
            pl.BlockSpec(memory_space=pltpu.SMEM if op.ndim == 1 else pltpu.VMEM)
            for op in operands
        ]
    return pl.pallas_call(
        kernel,
        out_shape=out_shape,
        name=name,
        interpret=INTERPRET,
        cost_estimate=pl.CostEstimate(flops=flops, transcendentals=0, bytes_accessed=1 << 20),
        **kw,
    )(*operands)


def shape(dims, dtype=F32):
    return jax.ShapeDtypeStruct(dims, dtype)


def directions(number):
    ordinal = np.arange(number, dtype=np.float64)
    height = 1.0 - (2.0 * ordinal + 1.0) / number
    radius = np.sqrt(1.0 - height * height)
    return np.stack([radius * np.cos(GOLDEN * ordinal), radius * np.sin(GOLDEN * ordinal), height])


def leaf_centers(number):
    ordinal = np.arange(number)
    return np.stack(
        [
            2.0 * (ordinal % 2) - 1.0,
            2.0 * (ordinal // 2 % 2) - 1.0,
            2.0 * (ordinal // 4) - (number // 4 - 1),
        ]
    )


def mie_spread(coef_count, mie_count):
    half_count = coef_count // 2
    table = np.zeros((coef_count, mie_count), np.float32)
    for number in range(coef_count):
        degree = math.isqrt(number % half_count + 1)
        table[number, number // half_count * (mie_count // 2) + degree - 1] = 1.0
    return table


def dot(a, b, dims=(((1,), (0,)), ((), ())), precision=None):
    return lax.dot_general(a, b, dims, precision=precision, preferred_element_type=F32)


def split(x):
    high = x.astype(BF16)
    return high, (x - high.astype(F32)).astype(BF16)


def one_hot(rows, row):
    ordinal = lax.broadcasted_iota(jnp.int32, (rows, row.shape[1]), 0)
    return jnp.where(ordinal == row, 1.0, 0.0)


def emit(vector, pattern, cosines, sines, member, leaf_cos, leaf_sin, halo_ref, column_ref):
    coefs = vector.shape[0] // 2
    boxes, dirs = leaf_cos.shape
    rounded = vector.astype(BF16)
    halo_ref[0, : 2 * coefs, :] = rounded
    by_real = dot(pattern, rounded[:coefs])
    by_imag = dot(pattern, rounded[coefs:])
    real = by_real[:dirs] - by_imag[dirs:]
    imag = by_real[dirs:] + by_imag[:dirs]
    out = jnp.concatenate([real * cosines + imag * sines, imag * cosines - real * sines], axis=0)
    high, low = split(out)
    leaf = dot(member, high, NT) + dot(member, low, NT)
    leaf_real, leaf_imag = leaf[:, :dirs], leaf[:, dirs:]
    halo_ref[0, 2 * coefs : 2 * coefs + boxes, :] = leaf_real.astype(BF16)
    halo_ref[0, 2 * coefs + boxes :, :] = leaf_imag.astype(BF16)
    column_real = jnp.sum(leaf_real * leaf_cos + leaf_imag * leaf_sin, axis=0, keepdims=True)
    column_imag = jnp.sum(leaf_imag * leaf_cos - leaf_real * leaf_sin, axis=0, keepdims=True)
    pair = jnp.concatenate([column_real, column_imag], axis=0)
    column_ref[...] = jnp.broadcast_to(pair[None], column_ref.shape)


def lanes(values):
    lane = lax.broadcasted_iota(jnp.int32, (1, 128), 1)
    row = jnp.zeros((1, 128), F32)
    for place, value in values:
        row = row + jnp.where(lane == place, value, 0.0)
    return row


def inner(a, b):
    return jnp.sum(jnp.sum(a * b, axis=0, keepdims=True), axis=1, keepdims=True)


def first_kernel(
    vector, pattern, offsets, planes, box, leaf_cos, leaf_sin, halo, column, cos_ref, sin_ref
):
    phases = KAPPA * (
        planes[0] * offsets[0:1, :] + planes[1] * offsets[1:2, :] + planes[2] * offsets[2:3, :]
    )
    cosines, sines = jnp.cos(phases), jnp.sin(phases)
    cos_ref[...] = cosines
    sin_ref[...] = sines
    member = one_hot(leaf_cos.shape[0], box[...]).astype(BF16)
    emit(
        vector[...], pattern[...], cosines, sines, member, leaf_cos[...], leaf_sin[...], halo, column
    )


def count_kernel(sources, targets, counts):
    source_hot = one_hot(counts.shape[0], sources[0]).astype(BF16)
    target_hot = one_hot(counts.shape[1], targets[0]).astype(BF16)
    counts[...] = dot(source_hot, target_hot, NT).astype(BF16)


def table_kernel(sources, classes, transfer, mie, spread, select, chosen, mie_full):
    number = select.shape[1]
    source_hot = one_hot(number, sources[...]).astype(BF16)
    row = lax.broadcasted_iota(jnp.int32, (number, number), 0)
    col = lax.broadcasted_iota(jnp.int32, (number, number), 1)
    unit = jnp.where(row == col, 1.0, 0.0).astype(BF16)
    select[...] = dot(source_hot, unit, TN).astype(BF16)
    class_hot = one_hot(transfer.shape[0], classes[...])
    chosen[...] = dot(class_hot, transfer[...], TN, HIGHEST)
    mie_full[0] = dot(spread[...], mie[0], precision=HIGHEST)
    mie_full[1] = dot(spread[...], mie[1], precision=HIGHEST)


def window_kernel(place, transfer, window, *, near_z, near_x, groups, run, top_x, top_y):
    high, depth, across, lane = (place[i] for i in range(4))
    ordinal = lax.broadcasted_iota(jnp.int32, (run, 128), 0)
    for z in range(near_z):
        for x in range(near_x):
            start = (across - x) * run - lane + top_y
            apart_y = jnp.abs(ordinal + (start - top_y))
            for group in range(groups):
                shift = (group - high) * near_z + depth - z
                keep = (apart_y >= 2) | (jnp.abs(shift) >= 2)
                for part in range(2):
                    rows = transfer[part, shift + top_x, pl.ds(start, run), :]
                    window[part, z * near_x + x, group * run : (group + 1) * run, :] = jnp.where(
                        keep, rows, 0.0
                    )


def coarse_kernel(columns, window, partial):
    real, imag = columns[:, 0, :][None], columns[:, 1, :][None]
    partial[:, 0, :] = jnp.sum(real * window[0] - imag * window[1], axis=1)
    partial[:, 1, :] = jnp.sum(imag * window[0] + real * window[1], axis=1)


def near_kernel(before, own, after, counts, table, select, chosen, near, leaf_in, columns):
    coefs = near.shape[0] // 2
    classes = table.shape[0]
    spheres = near.shape[1] // 2
    boxes, dirs = leaf_in.shape[0], leaf_in.shape[1] // 2

    @pl.when(pl.program_id(0) == 0)
    def _():
        leaves = []
        for row, part in enumerate((before, own, after)):
            for col in range(3):
                place = (row * 3 + col) * spheres
                columns[:, place : place + spheres] = part[col, : 2 * coefs, :]
                leaves.append(part[col, 2 * coefs :, :])
        around = jnp.concatenate(
            [
                jnp.concatenate([leaf[:boxes] for leaf in leaves], axis=0),
                jnp.concatenate([leaf[boxes:] for leaf in leaves], axis=0),
            ],
            axis=1,
        )
        picked = dot(select[...], around)
        pick_real, pick_imag = picked[:, :dirs], picked[:, dirs:]
        move_real, move_imag = chosen[:, :dirs], chosen[:, dirs:]
        got_real = pick_real * move_real - pick_imag * move_imag
        got_imag = pick_imag * move_real + pick_real * move_imag
        leaf_in[:, :dirs] = jnp.sum(got_real.reshape(boxes, -1, dirs), axis=1)
        leaf_in[:, dirs:] = jnp.sum(got_imag.reshape(boxes, -1, dirs), axis=1)
        near[...] = jnp.zeros(near.shape, F32)

    gathered = dot(columns[...], counts[...]).astype(BF16)
    total = near[...]
    for item in range(classes):
        at = slice(item * spheres, (item + 1) * spheres)
        pair = jnp.concatenate([gathered[:coefs, at], gathered[coefs:, at]], axis=1)
        total = total + dot(table[item], pair)
    near[...] = total


def arrive(partial, near, leaf_in, receive, cosines, sines, member, leaf_cos, leaf_sin, mie_full):
    boxes, dirs = leaf_cos.shape
    coefs = near.shape[0] // 2
    column_real = jnp.sum(partial[:, 0, :], axis=0, keepdims=True)
    column_imag = jnp.sum(partial[:, 1, :], axis=0, keepdims=True)
    incoming = leaf_in + jnp.concatenate(
        [
            column_real * leaf_cos - column_imag * leaf_sin,
            column_real * leaf_sin + column_imag * leaf_cos,
        ],
        axis=1,
    )
    high, low = split(incoming)
    spread = dot(high, member, TN) + dot(low, member, TN)
    real, imag = spread[:dirs], spread[dirs:]
    arriving = jnp.concatenate(
        [real * cosines - imag * sines, real * sines + imag * cosines], axis=1
    ).astype(BF16)
    total = near + dot(receive, arriving)
    half = total.shape[1] // 2
    field_real = total[:coefs, :half] - total[coefs:, half:]
    field_imag = total[coefs:, :half] + total[:coefs, half:]
    mie_real, mie_imag = mie_full[0], mie_full[1]
    return jnp.concatenate(
        [
            field_real * mie_real - field_imag * mie_imag,
            field_real * mie_imag + field_imag * mie_real,
        ],
        axis=0,
    )


def middle_kernel(
    vector,
    partial,
    near,
    leaf_in,
    receive,
    pattern,
    cosines,
    sines,
    box,
    leaf_cos,
    leaf_sin,
    mie_full,
    applied,
    halo,
    column,
    sums,
):
    member = one_hot(leaf_cos.shape[0], box[...]).astype(BF16)
    scattered = arrive(
        partial[...],
        near[...],
        leaf_in[...],
        receive[...],
        cosines[...],
        sines[...],
        member,
        leaf_cos[...],
        leaf_sin[...],
        mie_full[...],
    )
    applied[...] = scattered
    emit(
        scattered,
        pattern[...],
        cosines[...],
        sines[...],
        member,
        leaf_cos[...],
        leaf_sin[...],
        halo,
        column,
    )
    start = vector[...]
    sums[...] = lanes(
        [(0, inner(start, start)), (1, inner(start, scattered)), (2, inner(scattered, scattered))]
    )


def last_kernel(
    vector,
    scattered,
    partial,
    near,
    leaf_in,
    receive,
    cosines,
    sines,
    box,
    leaf_cos,
    leaf_sin,
    mie_full,
    sums,
    applied,
    everyone,
):
    member = one_hot(leaf_cos.shape[0], box[...]).astype(BF16)
    twice = arrive(
        partial[...],
        near[...],
        leaf_in[...],
        receive[...],
        cosines[...],
        sines[...],
        member,
        leaf_cos[...],
        leaf_sin[...],
        mie_full[...],
    )
    applied[...] = twice
    row = sums[...] + lanes(
        [(3, inner(vector[...], twice)), (4, inner(scattered[...], twice)), (5, inner(twice, twice))]
    )
    everyone[...] = jnp.broadcast_to(row[None], everyone.shape)


def relay_kernel(parts, everyone):
    everyone[...] = jnp.broadcast_to(jnp.sum(parts[...], axis=0, keepdims=True), everyone.shape)


def solve_kernel(parts, vector, scattered, twice, solution, residual):
    row = jnp.sum(parts[...], axis=0)
    lane = lax.broadcasted_iota(jnp.int32, row.shape, 1)

    def total(place):
        value = jnp.sum(jnp.where(lane == place, row, 0.0), axis=1, keepdims=True)
        return jnp.broadcast_to(value, (8, 128))

    uu, ud, dd, ue, de, ee = (total(place) for place in range(6))
    beta = jnp.sqrt(uu)
    along = ud / uu
    across = dd - along * ud
    size = jnp.sqrt(across)
    h00 = 1.0 - along
    h10 = size / beta
    turned = de - along * ue
    h01 = (ue - along * ud) / (size * beta)
    h11 = 1.0 + along - turned / across
    rest_u = ue / uu
    rest_d = turned / across
    left = ee - rest_u * ue - rest_d * turned
    h21 = jnp.sqrt(left) / size
    n00 = h00 * h00 + h10 * h10
    n01 = h00 * h01 + h10 * h11
    n11 = h01 * h01 + h11 * h11 + h21 * h21
    l00 = jnp.sqrt(n00)
    l10 = n01 / l00
    l11 = jnp.sqrt(n11 - l10 * l10)
    m0 = beta * h00 / l00
    m1 = (beta * h01 - l10 * m0) / l11
    y1 = m1 / l11
    y0 = (m0 - l10 * y1) / l00
    z0 = h00 * y0 + h01 * y1
    z1 = h10 * y0 + h11 * y1
    step = y1 / size
    sol_u = y0 / beta + step * along
    sol_d = -step
    res_u = (beta - z0) / beta - z1 / size * along + step * (rest_u - rest_d * along)
    res_d = z1 / size + step * rest_d
    res_e = -step
    u, d, e = vector[...], scattered[...], twice[...]
    solution[...] = sol_u[0:1] * u + sol_d[0:1] * d
    residual[...] = res_u[0:1] * u + res_d[0:1] * d + res_e[0:1] * e


def beside(x, axes):
    devices = lax.axis_size(axes)
    up = [(i, i + 1) for i in range(devices - 1)]
    down = [(j, i) for i, j in up]
    return lax.ppermute(x, axes, up), lax.ppermute(x, axes, down)


def exchange(x, axes):
    return lax.all_to_all(x, axes, split_axis=0, concat_axis=0, tiled=True)


def local(
    incident,
    mie,
    offsets,
    sphere_box,
    near_table,
    near_src,
    near_dst,
    pattern,
    receive,
    leaf_transfer,
    far_src,
    far_cls,
    coarse_transfer,
):
    coefs = incident.shape[1]
    spheres = incident.shape[4]
    rows = 2 * coefs
    dirs = pattern.shape[1]
    boxes, entries = far_src.shape[2:]
    classes, pairs = near_src.shape[2:]
    leaf_classes = leaf_transfer.shape[0]
    high_count, near_z = lax.axis_size("bx_0"), lax.axis_size("bx_1")
    near_x = lax.axis_size("by_0")
    run = lax.axis_size(("by_1", "by_2"))
    first_count, second_count = lax.axis_size(FIRST), lax.axis_size(SECOND)
    place = jnp.stack(
        [
            lax.axis_index("bx_0"),
            lax.axis_index("bx_1"),
            lax.axis_index("by_0"),
            lax.axis_index(("by_1", "by_2")),
        ]
    ).astype(jnp.int32)

    planes = jnp.asarray(directions(dirs)[:, :, None].astype(np.float32))
    centre = KAPPA * (leaf_centers(boxes).T @ directions(dirs))
    leaf_cos = jnp.asarray(np.cos(centre).astype(np.float32))
    leaf_sin = jnp.asarray(np.sin(centre).astype(np.float32))

    vector = incident.reshape(rows, spheres)
    box = sphere_box.reshape(1, spheres)
    pattern = pattern.reshape(2 * dirs, coefs)
    receive = receive.reshape(rows, dirs)
    table = near_table.reshape(classes, rows, coefs)

    halo_shape = shape((1, rows + 2 * boxes, spheres), BF16)
    column_shape = shape((first_count, 2, dirs))
    halo, column, cosines, sines = call(
        first_kernel,
        (halo_shape, column_shape, shape((dirs, spheres)), shape((dirs, spheres))),
        (vector, pattern, offsets.reshape(3, spheres), planes, box, leaf_cos, leaf_sin),
        "first",
        flops=1 << 26,
    )
    counts = call(
        count_kernel,
        shape((9 * spheres, classes * spheres), BF16),
        (near_src.reshape(classes, 1, pairs), near_dst.reshape(classes, 1, pairs)),
        "counts",
        flops=1 << 31,
        grid=(classes,),
        in_specs=[pl.BlockSpec((1, 1, pairs), lambda k: (k, 0, 0))] * 2,
        out_specs=pl.BlockSpec((9 * spheres, spheres), lambda k: (0, k)),
    )
    select, chosen, mie_full = call(
        table_kernel,
        (
            shape((boxes * entries, 9 * boxes), BF16),
            shape((boxes * entries, 2 * dirs)),
            shape((2, coefs, spheres)),
        ),
        (
            far_src.reshape(1, boxes * entries),
            far_cls.reshape(1, boxes * entries),
            leaf_transfer.reshape(leaf_classes, 2 * dirs),
            mie.reshape(2, mie.shape[1], spheres),
            jnp.asarray(mie_spread(coefs, mie.shape[1])),
        ),
        "tables",
        flops=1 << 28,
    )
    window = call(
        functools.partial(
            window_kernel,
            near_z=near_z,
            near_x=near_x,
            groups=high_count,
            run=run,
            top_x=high_count * near_z - 1,
            top_y=near_x * run - 1,
        ),
        shape((2, second_count, first_count, dirs)),
        (place, coarse_transfer),
        "window",
        flops=1 << 28,
    )

    chunk = 4 if classes % 4 == 0 else 1
    whole3 = pl.BlockSpec((3, rows + 2 * boxes, spheres), lambda k: (0, 0, 0))

    def apply(halo, column):
        before, after = beside(halo, BY)
        line = jnp.concatenate([before, halo, after], axis=0)
        columns = exchange(column, FIRST)
        up, down = beside(line, BX)
        partial = call(
            coarse_kernel, shape((second_count, 2, dirs)), (columns, window), "coarse", 1 << 24
        )
        partial = exchange(partial, SECOND)
        near, leaf_in = call(
            near_kernel,
            (shape((rows, 2 * spheres)), shape((boxes, 2 * dirs))),
            (up, line, down, counts, table, select, chosen),
            "near",
            flops=1 << 31,
            grid=(classes // chunk,),
            in_specs=[
                whole3,
                whole3,
                whole3,
                pl.BlockSpec((9 * spheres, chunk * spheres), lambda k: (0, k)),
                pl.BlockSpec((chunk, rows, coefs), lambda k: (k, 0, 0)),
                pl.BlockSpec((boxes * entries, 9 * boxes), lambda k: (0, 0)),
                pl.BlockSpec((boxes * entries, 2 * dirs), lambda k: (0, 0)),
            ],
            out_specs=(
                pl.BlockSpec((rows, 2 * spheres), lambda k: (0, 0)),
                pl.BlockSpec((boxes, 2 * dirs), lambda k: (0, 0)),
            ),
            scratch_shapes=[pltpu.VMEM((rows, 9 * spheres), BF16)],
        )
        return partial, near, leaf_in

    partial, near, leaf_in = apply(halo, column)
    once, halo, column, sums = call(
        middle_kernel,
        (shape((rows, spheres)), halo_shape, column_shape, shape((1, 128))),
        (
            vector,
            partial,
            near,
            leaf_in,
            receive,
            pattern,
            cosines,
            sines,
            box,
            leaf_cos,
            leaf_sin,
            mie_full,
        ),
        "middle",
        flops=1 << 26,
    )
    partial, near, leaf_in = apply(halo, column)
    twice, everyone = call(
        last_kernel,
        (shape((rows, spheres)), shape((first_count, 1, 128))),
        (
            vector,
            once,
            partial,
            near,
            leaf_in,
            receive,
            cosines,
            sines,
            box,
            leaf_cos,
            leaf_sin,
            mie_full,
            sums,
        ),
        "last",
        flops=1 << 26,
    )
    everyone = call(
        relay_kernel, shape((second_count, 1, 128)), (exchange(everyone, FIRST),), "relay", 1 << 20
    )
    solved, residual = call(
        solve_kernel,
        (shape((rows, spheres)), shape((rows, spheres))),
        (exchange(everyone, SECOND), vector, once, twice),
        "solve",
        flops=1 << 24,
    )
    return solved.reshape(incident.shape), residual.reshape(incident.shape)


def build(devices, sizes):
    torus = Mesh(devices.reshape(sizes), BX + BY)
    placed = (
        P(None, None, BX, BY, None),
        P(None, None, BX, BY, None),
        P(None, BX, BY, None),
        P(BX, BY, None),
        P(),
        P(BX, BY, None, None),
        P(BX, BY, None, None),
        P(),
        P(),
        P(),
        P(BX, BY, None, None),
        P(BX, BY, None, None),
        P(),
    )
    return jax.shard_map(
        local,
        mesh=torus,
        in_specs=placed,
        out_specs=(P(None, None, BX, BY, None), P(None, None, BX, BY, None)),
        check_vma=False,
    )


def solution(mesh):
    return build(mesh.devices, (2, 8, 4, 4, 2))
```

```python
import functools
import math

import jax
import jax.numpy as jnp
import numpy as np
from jax import lax
from jax.experimental import pallas as pl
from jax.experimental.pallas import tpu as pltpu
from jax.sharding import Mesh
from jax.sharding import PartitionSpec as P

BX = ("bx_0", "bx_1")
BY = ("by_0", "by_1", "by_2")
FIRST = ("bx_0", "by_1", "by_2")
SECOND = ("bx_1", "by_0")

HIGHEST = lax.Precision.HIGHEST
KAPPA = 1.5
GOLDEN = 2.399963229728653
F32 = jnp.float32
BF16 = jnp.bfloat16
NT = (((1,), (1,)), ((), ()))
TN = (((0,), (0,)), ((), ()))
INTERPRET = False


def call(kernel, out_shape, operands, flops=0, **kw):
    if "grid" not in kw:
        kw["in_specs"] = [
            pl.BlockSpec(memory_space=pltpu.SMEM if op.ndim == 1 else pltpu.VMEM)
            for op in operands
        ]
    return pl.pallas_call(
        kernel,
        out_shape=out_shape,
        interpret=INTERPRET,
        cost_estimate=pl.CostEstimate(flops=flops, transcendentals=0, bytes_accessed=1 << 20),
        **kw,
    )(*operands)


def resident(x):
    return x if INTERPRET else pltpu.with_memory_space_constraint(x, pltpu.VMEM)


def kept(dims, dtype=F32):
    return shape(dims, dtype) if INTERPRET else pltpu.VMEM(dims, dtype)


def shape(dims, dtype=F32):
    return jax.ShapeDtypeStruct(dims, dtype)


def directions(number):
    ordinal = np.arange(number, dtype=np.float64)
    height = 1.0 - (2.0 * ordinal + 1.0) / number
    radius = np.sqrt(1.0 - height * height)
    return np.stack([radius * np.cos(GOLDEN * ordinal), radius * np.sin(GOLDEN * ordinal), height])


def leaf_centers(number):
    ordinal = np.arange(number)
    return np.stack(
        [
            2.0 * (ordinal % 2) - 1.0,
            2.0 * (ordinal // 2 % 2) - 1.0,
            2.0 * (ordinal // 4) - (number // 4 - 1),
        ]
    )


def mie_spread(coef_count, mie_count):
    half_count = coef_count // 2
    table = np.zeros((coef_count, mie_count), np.float32)
    for number in range(coef_count):
        degree = math.isqrt(number % half_count + 1)
        table[number, number // half_count * (mie_count // 2) + degree - 1] = 1.0
    return table


def dot(a, b, dims=(((1,), (0,)), ((), ())), precision=None):
    return lax.dot_general(a, b, dims, precision=precision, preferred_element_type=F32)


def split(x):
    high = x.astype(BF16)
    return high, (x - high.astype(F32)).astype(BF16)


def one_hot(rows, row):
    ordinal = lax.broadcasted_iota(jnp.int32, (rows, row.shape[1]), 0)
    return jnp.where(ordinal == row, 1.0, 0.0)


def emit(vector, pattern, cosines, sines, member, leaf_cos, leaf_sin, halo_ref, column_ref):
    coefs = vector.shape[0] // 2
    boxes, dirs = leaf_cos.shape
    rounded = vector.astype(BF16)
    halo_ref[0, : 2 * coefs, :] = rounded
    both = jnp.concatenate([pattern[0], pattern[1]], axis=1)
    by_real = dot(both, rounded[:coefs], TN)
    by_imag = dot(both, rounded[coefs:], TN)
    real = by_real[:dirs] - by_imag[dirs:]
    imag = by_real[dirs:] + by_imag[:dirs]
    out = jnp.concatenate([real * cosines + imag * sines, imag * cosines - real * sines], axis=0)
    high, low = split(out)
    leaf = dot(member, high, NT) + dot(member, low, NT)
    leaf_real, leaf_imag = leaf[:, :dirs], leaf[:, dirs:]
    halo_ref[0, 2 * coefs : 2 * coefs + boxes, :] = leaf_real.astype(BF16)
    halo_ref[0, 2 * coefs + boxes :, :] = leaf_imag.astype(BF16)
    column_real = jnp.sum(leaf_real * leaf_cos + leaf_imag * leaf_sin, axis=0, keepdims=True)
    column_imag = jnp.sum(leaf_imag * leaf_cos - leaf_real * leaf_sin, axis=0, keepdims=True)
    pair = jnp.concatenate([column_real, column_imag], axis=0)
    column_ref[...] = jnp.broadcast_to(pair[None], column_ref.shape)


def lanes(values):
    lane = lax.broadcasted_iota(jnp.int32, (1, 128), 1)
    row = jnp.zeros((1, 128), F32)
    for place, value in values:
        row = row + jnp.where(lane == place, value, 0.0)
    return row


def inner(a, b):
    return jnp.sum(jnp.sum(a * b, axis=0, keepdims=True), axis=1, keepdims=True)


def first_kernel(
    vector, pattern, offsets, planes, box, leaf_cos, leaf_sin, halo, column, cos_ref, sin_ref
):
    phases = KAPPA * (
        planes[0] * offsets[0] + planes[1] * offsets[1] + planes[2] * offsets[2]
    )
    cosines, sines = jnp.cos(phases), jnp.sin(phases)
    cos_ref[...] = cosines
    sin_ref[...] = sines
    member = one_hot(leaf_cos.shape[0], box[...]).astype(BF16)
    emit(
        vector[...], pattern[...], cosines, sines, member, leaf_cos[...], leaf_sin[...], halo, column
    )


def mirrored(sources, width, flip_x, flip_y):
    line = 3 * width
    flat = jnp.where(sources < line, 0, jnp.where(sources < 2 * line, 1, 2))
    within = sources - line * flat
    side = jnp.where(within < width, 0, jnp.where(within < 2 * width, 1, 2))
    return sources + flip_x * (2 - 2 * flat) * line + flip_y * (2 - 2 * side) * width


def count_kernel(place, sources, targets, counts):
    spheres = counts.shape[0] // 9
    chunk = counts.shape[1] // spheres
    for item in range(chunk):
        at = pl.ds(pl.program_id(0) * chunk + item, 1)
        source_hot = one_hot(9 * spheres, mirrored(sources[at, :], spheres, place[4], place[5]))
        target_hot = one_hot(spheres, targets[at, :])
        counts[:, item * spheres : (item + 1) * spheres] = dot(
            source_hot.astype(BF16), target_hot.astype(BF16), NT
        ).astype(BF16)


def table_kernel(place, sources, classes, transfer, mie, spread, select, chosen, mie_full):
    boxes, entries = sources.shape
    row = lax.broadcasted_iota(jnp.int32, (boxes, boxes), 0)
    col = lax.broadcasted_iota(jnp.int32, (boxes, boxes), 1)
    unit = jnp.where(row == col, 1.0, 0.0).astype(BF16)
    around = mirrored(sources[...], boxes, place[4], place[5])
    around = dot(around.astype(F32).astype(BF16), unit, TN)
    kinds = dot(classes[...].astype(F32).astype(BF16), unit, TN)
    box_lane = lax.broadcasted_iota(jnp.int32, (entries, select.shape[1]), 1).astype(F32)
    kind_lane = lax.broadcasted_iota(jnp.int32, (entries, transfer.shape[0]), 1).astype(F32)
    hots = []
    for item in range(boxes):
        at = slice(item * entries, (item + 1) * entries)
        hots.append(jnp.where(kinds[:, item : item + 1] == kind_lane, 1.0, 0.0))
        select[at, :] = jnp.where(around[:, item : item + 1] == box_lane, 1.0, 0.0).astype(BF16)
    hot = jnp.concatenate(hots, axis=0)
    dirs = transfer.shape[2]
    chosen[:, :dirs] = dot(hot, transfer[:, 0, :], precision=HIGHEST)
    chosen[:, dirs:] = dot(hot, transfer[:, 1, :], precision=HIGHEST)
    mie_full[...] = dot(spread[...], mie[...], precision=HIGHEST)


def window_kernel(place, transfer, window, *, near_z, near_x, groups, run, top_x, top_y):
    high, depth, across, lane = (place[i] for i in range(4))
    ordinal = lax.broadcasted_iota(jnp.int32, (run, 128), 0)
    for z in range(near_z):
        for x in range(near_x):
            start = (across - x) * run - lane + top_y
            apart_y = jnp.abs(ordinal + (start - top_y))
            for group in range(groups):
                shift = (group - high) * near_z + depth - z
                keep = (apart_y >= 2) | (jnp.abs(shift) >= 2)
                for part in range(2):
                    rows = transfer[shift + top_x, pl.ds(start, run), part, :]
                    window[part, z * near_x + x, group * run : (group + 1) * run, :] = jnp.where(
                        keep, rows, 0.0
                    )


def coarse_kernel(columns, window, partial):
    real, imag = columns[:, 0, :][None], columns[:, 1, :][None]
    partial[:, 0, :] = jnp.sum(real * window[0] - imag * window[1], axis=1)
    partial[:, 1, :] = jnp.sum(imag * window[0] + real * window[1], axis=1)


def near_kernel(before, own, after, counts, table, select, chosen, near, leaf_in, columns):
    coefs = near.shape[0] // 2
    classes = table.shape[0]
    spheres = near.shape[1] // 2
    boxes, dirs = leaf_in.shape[0], leaf_in.shape[1] // 2

    @pl.when(pl.program_id(0) == 0)
    def _():
        leaves = []
        for row in range(3):
            for col, part in enumerate((before, own, after)):
                place = (row * 3 + col) * spheres
                columns[:, place : place + spheres] = part[row, : 2 * coefs, :]
                leaves.append(part[row, 2 * coefs :, :])
        around = jnp.concatenate(
            [
                jnp.concatenate([leaf[:boxes] for leaf in leaves], axis=0),
                jnp.concatenate([leaf[boxes:] for leaf in leaves], axis=0),
            ],
            axis=1,
        )
        picked = dot(select[...], around)
        pick_real, pick_imag = picked[:, :dirs], picked[:, dirs:]
        move_real, move_imag = chosen[:, :dirs], chosen[:, dirs:]
        got_real = pick_real * move_real - pick_imag * move_imag
        got_imag = pick_imag * move_real + pick_real * move_imag
        leaf_in[:, :dirs] = jnp.sum(got_real.reshape(boxes, -1, dirs), axis=1)
        leaf_in[:, dirs:] = jnp.sum(got_imag.reshape(boxes, -1, dirs), axis=1)
        near[...] = jnp.zeros(near.shape, F32)

    gathered = dot(columns[...], counts[...]).astype(BF16)
    total = near[...]
    for item in range(classes):
        at = slice(item * spheres, (item + 1) * spheres)
        pair = jnp.concatenate([gathered[:coefs, at], gathered[coefs:, at]], axis=1)
        total = total + dot(table[item], pair)
    near[...] = total


def arrive(partial, near, leaf_in, receive, cosines, sines, member, leaf_cos, leaf_sin, mie_full):
    _, dirs = leaf_cos.shape
    coefs = near.shape[0] // 2
    column_real = jnp.sum(partial[:, 0, :], axis=0, keepdims=True)
    column_imag = jnp.sum(partial[:, 1, :], axis=0, keepdims=True)
    incoming = leaf_in + jnp.concatenate(
        [
            column_real * leaf_cos - column_imag * leaf_sin,
            column_real * leaf_sin + column_imag * leaf_cos,
        ],
        axis=1,
    )
    high, low = split(incoming)
    spread = dot(high, member, TN) + dot(low, member, TN)
    real, imag = spread[:dirs], spread[dirs:]
    arriving = jnp.concatenate(
        [real * cosines - imag * sines, real * sines + imag * cosines], axis=1
    ).astype(BF16)
    total = near + dot(receive, arriving)
    half = total.shape[1] // 2
    field_real = total[:coefs, :half] - total[coefs:, half:]
    field_imag = total[coefs:, :half] + total[:coefs, half:]
    mie_real, mie_imag = mie_full[:coefs], mie_full[coefs:]
    return jnp.concatenate(
        [
            field_real * mie_real - field_imag * mie_imag,
            field_real * mie_imag + field_imag * mie_real,
        ],
        axis=0,
    )


def middle_kernel(
    vector,
    partial,
    near,
    leaf_in,
    pattern,
    receive,
    cosines,
    sines,
    box,
    leaf_cos,
    leaf_sin,
    mie_full,
    applied,
    halo,
    column,
    sums,
):
    member = one_hot(leaf_cos.shape[0], box[...]).astype(BF16)
    scattered = arrive(
        partial[...],
        near[...],
        leaf_in[...],
        receive[...],
        cosines[...],
        sines[...],
        member,
        leaf_cos[...],
        leaf_sin[...],
        mie_full[...],
    )
    applied[...] = scattered
    emit(
        scattered,
        pattern[...],
        cosines[...],
        sines[...],
        member,
        leaf_cos[...],
        leaf_sin[...],
        halo,
        column,
    )
    start = vector[...]
    sums[...] = lanes(
        [(0, inner(start, start)), (1, inner(start, scattered)), (2, inner(scattered, scattered))]
    )


def last_kernel(
    vector,
    scattered,
    partial,
    near,
    leaf_in,
    receive,
    cosines,
    sines,
    box,
    leaf_cos,
    leaf_sin,
    mie_full,
    sums,
    applied,
    everyone,
):
    member = one_hot(leaf_cos.shape[0], box[...]).astype(BF16)
    twice = arrive(
        partial[...],
        near[...],
        leaf_in[...],
        receive[...],
        cosines[...],
        sines[...],
        member,
        leaf_cos[...],
        leaf_sin[...],
        mie_full[...],
    )
    applied[...] = twice
    row = sums[...] + lanes(
        [(3, inner(vector[...], twice)), (4, inner(scattered[...], twice)), (5, inner(twice, twice))]
    )
    everyone[...] = jnp.broadcast_to(row[None], everyone.shape)


def relay_kernel(parts, everyone):
    everyone[...] = jnp.broadcast_to(jnp.sum(parts[...], axis=0, keepdims=True), everyone.shape)


def solve_kernel(parts, vector, scattered, twice, solution, residual):
    row = jnp.sum(parts[...], axis=0)
    lane = lax.broadcasted_iota(jnp.int32, row.shape, 1)

    def total(place):
        value = jnp.sum(jnp.where(lane == place, row, 0.0), axis=1, keepdims=True)
        return jnp.broadcast_to(value, (8, 128))

    uu, ud, dd, ue, de, ee = (total(place) for place in range(6))
    beta = jnp.sqrt(uu)
    along = ud / uu
    across = dd - along * ud
    size = jnp.sqrt(across)
    h00 = 1.0 - along
    h10 = size / beta
    turned = de - along * ue
    h01 = (ue - along * ud) / (size * beta)
    h11 = 1.0 + along - turned / across
    rest_u = ue / uu
    rest_d = turned / across
    left = ee - rest_u * ue - rest_d * turned
    h21 = jnp.sqrt(left) / size
    n00 = h00 * h00 + h10 * h10
    n01 = h00 * h01 + h10 * h11
    n11 = h01 * h01 + h11 * h11 + h21 * h21
    l00 = jnp.sqrt(n00)
    l10 = n01 / l00
    l11 = jnp.sqrt(n11 - l10 * l10)
    m0 = beta * h00 / l00
    m1 = (beta * h01 - l10 * m0) / l11
    y1 = m1 / l11
    y0 = (m0 - l10 * y1) / l00
    z0 = h00 * y0 + h01 * y1
    z1 = h10 * y0 + h11 * y1
    step = y1 / size
    sol_u = y0 / beta + step * along
    sol_d = -step
    res_u = (beta - z0) / beta - z1 / size * along + step * (rest_u - rest_d * along)
    res_d = z1 / size + step * rest_d
    res_e = -step
    u, d, e = vector[...], scattered[...], twice[...]
    solution[...] = sol_u[0:1] * u + sol_d[0:1] * d
    residual[...] = res_u[0:1] * u + res_d[0:1] * d + res_e[0:1] * e


def swap(x, axes, first):
    pairs = [(i, i + 1) for i in range(first, lax.axis_size(axes) - 1, 2)]
    return lax.ppermute(x, axes, pairs + [(j, i) for i, j in pairs])


def exchange(x, axes):
    return lax.all_to_all(x, axes, split_axis=0, concat_axis=0, tiled=True)


def local(
    incident,
    mie,
    offsets,
    sphere_box,
    near_table,
    near_src,
    near_dst,
    pattern,
    receive,
    leaf_transfer,
    far_src,
    far_cls,
    coarse_transfer,
):
    coefs = incident.shape[1]
    spheres = incident.shape[4]
    rows = 2 * coefs
    dirs = pattern.shape[1]
    boxes, entries = far_src.shape[2:]
    classes, pairs = near_src.shape[2:]
    high_count, near_z = lax.axis_size("bx_0"), lax.axis_size("bx_1")
    near_x = lax.axis_size("by_0")
    run = lax.axis_size(("by_1", "by_2"))
    first_count, second_count = lax.axis_size(FIRST), lax.axis_size(SECOND)
    place = jnp.stack(
        [
            lax.axis_index("bx_0"),
            lax.axis_index("bx_1"),
            lax.axis_index("by_0"),
            lax.axis_index(("by_1", "by_2")),
            lax.axis_index(BX) % 2,
            lax.axis_index(BY) % 2,
        ]
    ).astype(jnp.int32)

    planes = jnp.asarray(directions(dirs)[:, :, None].astype(np.float32))
    centre = KAPPA * (leaf_centers(boxes).T @ directions(dirs))
    leaf_cos = jnp.asarray(np.cos(centre).astype(np.float32))
    leaf_sin = jnp.asarray(np.sin(centre).astype(np.float32))

    vector = incident.reshape(rows, spheres)
    box = sphere_box.reshape(1, spheres)
    pattern = pattern.transpose(0, 2, 1)
    receive = receive.reshape(rows, dirs)

    halo_shape = kept((1, rows + 2 * boxes, spheres), BF16)
    column_shape = kept((first_count, 2, dirs))
    halo, column, cosines, sines = call(
        first_kernel,
        (halo_shape, column_shape, kept((dirs, spheres)), kept((dirs, spheres))),
        (vector, pattern, offsets.reshape(3, 1, spheres), planes, box, leaf_cos, leaf_sin),
        flops=1 << 26,
    )
    chunk = 4 if classes % 4 == 0 else 1

    def prepare():
        counts = call(
            count_kernel,
            shape((9 * spheres, classes * spheres), BF16),
            (place, near_src.reshape(classes, pairs), near_dst.reshape(classes, pairs)),
            flops=1 << 31,
            grid=(classes // chunk,),
            in_specs=[
                pl.BlockSpec(memory_space=pltpu.SMEM),
                pl.BlockSpec((classes, pairs), lambda k: (0, 0)),
                pl.BlockSpec((classes, pairs), lambda k: (0, 0)),
            ],
            out_specs=pl.BlockSpec((9 * spheres, chunk * spheres), lambda k: (0, k)),
        )
        spread = mie_spread(coefs, mie.shape[1])
        zero = np.zeros_like(spread)
        select, chosen, mie_full = call(
            table_kernel,
            (
                shape((boxes * entries, 9 * boxes), BF16),
                shape((boxes * entries, 2 * dirs)),
                kept((rows, spheres)),
            ),
            (
                place,
                far_src.reshape(boxes, entries),
                far_cls.reshape(boxes, entries),
                leaf_transfer,
                mie.reshape(2 * mie.shape[1], spheres),
                jnp.asarray(np.block([[spread, zero], [zero, spread]])),
            ),
            flops=1 << 28,
        )
        return counts, select, chosen, mie_full

    def windows():
        return call(
            functools.partial(
                window_kernel,
                near_z=near_z,
                near_x=near_x,
                groups=high_count,
                run=run,
                top_x=high_count * near_z - 1,
                top_y=near_x * run - 1,
            ),
            shape((2, second_count, first_count, dirs)),
            (place, coarse_transfer.transpose(1, 2, 0, 3)),
            flops=1 << 28,
        )

    whole3 = pl.BlockSpec((3, rows + 2 * boxes, spheres), lambda k: (0, 0, 0))

    def apply(halo, column, window, counts, select, chosen):
        columns = exchange(column, FIRST)
        ahead = swap(halo, BX, 0)
        behind = swap(halo, BX, 1)
        line = jnp.concatenate([behind, halo, ahead], axis=0)
        right = swap(line, BY, 0)
        left = swap(line, BY, 1)
        partial = call(
            coarse_kernel, kept((second_count, 2, dirs)), (resident(columns), window), 1 << 24
        )
        partial = exchange(partial, SECOND)
        near, leaf_in = call(
            near_kernel,
            (kept((rows, 2 * spheres)), kept((boxes, 2 * dirs))),
            (left, line, right, counts, near_table.reshape(classes, rows, coefs), select, chosen),
            flops=1 << 31,
            grid=(classes // chunk,),
            in_specs=[
                whole3,
                whole3,
                whole3,
                pl.BlockSpec((9 * spheres, chunk * spheres), lambda k: (0, k)),
                pl.BlockSpec((chunk, rows, coefs), lambda k: (k, 0, 0)),
                pl.BlockSpec((boxes * entries, 9 * boxes), lambda k: (0, 0)),
                pl.BlockSpec((boxes * entries, 2 * dirs), lambda k: (0, 0)),
            ],
            out_specs=(
                pl.BlockSpec((rows, 2 * spheres), lambda k: (0, 0)),
                pl.BlockSpec((boxes, 2 * dirs), lambda k: (0, 0)),
            ),
            scratch_shapes=[pltpu.VMEM((rows, 9 * spheres), BF16)],
        )
        return resident(partial), near, leaf_in

    window = windows()
    counts, select, chosen, mie_full = prepare()
    partial, near, leaf_in = apply(halo, column, window, counts, select, chosen)
    far = (receive, cosines, sines, box, leaf_cos, leaf_sin, mie_full)
    once, halo, column, sums = call(
        middle_kernel,
        (kept((rows, spheres)), halo_shape, column_shape, kept((1, 128))),
        (vector, partial, near, leaf_in, pattern) + far,
        flops=1 << 26,
    )
    partial, near, leaf_in = apply(halo, column, window, counts, select, chosen)
    twice, everyone = call(
        last_kernel,
        (kept((rows, spheres)), kept((first_count, 1, 128))),
        (vector, once, partial, near, leaf_in) + far + (sums,),
        flops=1 << 26,
    )
    everyone = call(
        relay_kernel, kept((second_count, 1, 128)), (resident(exchange(everyone, FIRST)),), 1 << 20
    )
    solved, residual = call(
        solve_kernel,
        (shape((rows, spheres)), shape((rows, spheres))),
        (resident(exchange(everyone, SECOND)), vector, once, twice),
        flops=1 << 24,
    )
    return solved.reshape(incident.shape), residual.reshape(incident.shape)


def build(devices, sizes):
    torus = Mesh(devices.reshape(sizes), BX + BY)
    placed = (
        P(None, None, BX, BY, None),
        P(None, None, BX, BY, None),
        P(None, BX, BY, None),
        P(BX, BY, None),
        P(),
        P(BX, BY, None, None),
        P(BX, BY, None, None),
        P(),
        P(),
        P(),
        P(BX, BY, None, None),
        P(BX, BY, None, None),
        P(),
    )
    return jax.shard_map(
        local,
        mesh=torus,
        in_specs=placed,
        out_specs=(P(None, None, BX, BY, None), P(None, None, BX, BY, None)),
        check_vma=False,
    )


def solution(mesh):
    return build(mesh.devices, (2, 8, 4, 4, 2))
```

```python
import functools
import math

import jax
import jax.numpy as jnp
import numpy as np
from jax import lax
from jax.experimental import pallas as pl
from jax.experimental.pallas import tpu as pltpu
from jax.sharding import Mesh
from jax.sharding import PartitionSpec as P

BX = ("bx_0", "bx_1")
BY = ("by_0", "by_1", "by_2")
FIRST = ("bx_0", "by_1", "by_2")
SECOND = ("bx_1", "by_0")

HIGHEST = lax.Precision.HIGHEST
KAPPA = 1.5
GOLDEN = 2.399963229728653
F32 = jnp.float32
BF16 = jnp.bfloat16
NT = (((1,), (1,)), ((), ()))
TN = (((0,), (0,)), ((), ()))
INTERPRET = False


def call(kernel, out_shape, operands, flops=0, **kw):
    if "grid" not in kw:
        kw["in_specs"] = [
            pl.BlockSpec(memory_space=pltpu.SMEM if op.ndim == 1 else pltpu.VMEM)
            for op in operands
        ]
    return pl.pallas_call(
        kernel,
        out_shape=out_shape,
        interpret=INTERPRET,
        cost_estimate=pl.CostEstimate(flops=flops, transcendentals=0, bytes_accessed=1 << 20),
        **kw,
    )(*operands)


def resident(x):
    return x if INTERPRET else pltpu.with_memory_space_constraint(x, pltpu.VMEM)


def kept(dims, dtype=F32):
    return shape(dims, dtype) if INTERPRET else pltpu.VMEM(dims, dtype)


def shape(dims, dtype=F32):
    return jax.ShapeDtypeStruct(dims, dtype)


def directions(number):
    ordinal = np.arange(number, dtype=np.float64)
    height = 1.0 - (2.0 * ordinal + 1.0) / number
    radius = np.sqrt(1.0 - height * height)
    return np.stack([radius * np.cos(GOLDEN * ordinal), radius * np.sin(GOLDEN * ordinal), height])


def leaf_centers(number):
    ordinal = np.arange(number)
    return np.stack(
        [
            2.0 * (ordinal % 2) - 1.0,
            2.0 * (ordinal // 2 % 2) - 1.0,
            2.0 * (ordinal // 4) - (number // 4 - 1),
        ]
    )


def mie_spread(coef_count, mie_count):
    half_count = coef_count // 2
    table = np.zeros((coef_count, mie_count), np.float32)
    for number in range(coef_count):
        degree = math.isqrt(number % half_count + 1)
        table[number, number // half_count * (mie_count // 2) + degree - 1] = 1.0
    return table


def dot(a, b, dims=(((1,), (0,)), ((), ())), precision=None):
    return lax.dot_general(a, b, dims, precision=precision, preferred_element_type=F32)


def split(x):
    high = x.astype(BF16)
    return high, (x - high.astype(F32)).astype(BF16)


def one_hot(rows, row):
    ordinal = lax.broadcasted_iota(jnp.int32, (rows, row.shape[1]), 0)
    return jnp.where(ordinal == row, 1.0, 0.0)


def emit(vector, pattern, cosines, sines, member, leaf_cos, leaf_sin, halo_ref, column_ref):
    coefs = vector.shape[0] // 2
    boxes, dirs = leaf_cos.shape
    rounded = vector.astype(BF16)
    halo_ref[0, : 2 * coefs, :] = rounded
    by_real = dot(pattern, rounded[:coefs])
    by_imag = dot(pattern, rounded[coefs:])
    real = by_real[:dirs] - by_imag[dirs:]
    imag = by_real[dirs:] + by_imag[:dirs]
    out = jnp.concatenate([real * cosines + imag * sines, imag * cosines - real * sines], axis=0)
    high, low = split(out)
    leaf = dot(member, high, NT) + dot(member, low, NT)
    leaf_real, leaf_imag = leaf[:, :dirs], leaf[:, dirs:]
    halo_ref[0, 2 * coefs : 2 * coefs + boxes, :] = leaf_real.astype(BF16)
    halo_ref[0, 2 * coefs + boxes :, :] = leaf_imag.astype(BF16)
    column_real = jnp.sum(leaf_real * leaf_cos + leaf_imag * leaf_sin, axis=0, keepdims=True)
    column_imag = jnp.sum(leaf_imag * leaf_cos - leaf_real * leaf_sin, axis=0, keepdims=True)
    pair = jnp.concatenate([column_real, column_imag], axis=0)
    column_ref[...] = jnp.broadcast_to(pair[None], column_ref.shape)


def lanes(values):
    lane = lax.broadcasted_iota(jnp.int32, (1, 128), 1)
    row = jnp.zeros((1, 128), F32)
    for place, value in values:
        row = row + jnp.where(lane == place, value, 0.0)
    return row


def inner(a, b):
    return jnp.sum(jnp.sum(a * b, axis=0, keepdims=True), axis=1, keepdims=True)


def first_kernel(
    vector, pattern, offsets, planes, box, leaf_cos, leaf_sin, halo, column, cos_ref, sin_ref, send
):
    turned = jnp.concatenate([pattern[0].T, pattern[1].T], axis=0)
    send[...] = turned
    phases = KAPPA * (
        planes[0] * offsets[0] + planes[1] * offsets[1] + planes[2] * offsets[2]
    )
    cosines, sines = jnp.cos(phases), jnp.sin(phases)
    cos_ref[...] = cosines
    sin_ref[...] = sines
    member = one_hot(leaf_cos.shape[0], box[...]).astype(BF16)
    emit(vector[...], turned, cosines, sines, member, leaf_cos[...], leaf_sin[...], halo, column)


def mirrored(sources, width, flip_x, flip_y):
    line = 3 * width
    flat = jnp.where(sources < line, 0, jnp.where(sources < 2 * line, 1, 2))
    within = sources - line * flat
    side = jnp.where(within < width, 0, jnp.where(within < 2 * width, 1, 2))
    return sources + flip_x * (2 - 2 * flat) * line + flip_y * (2 - 2 * side) * width


def count_kernel(
    index,
    sources,
    targets,
    far_sources,
    kinds,
    transfer,
    mie,
    spread,
    counts,
    select,
    chosen,
    mie_full,
    *,
    across_y,
):
    flips = lax.rem(lax.div(index[0], across_y), 2), lax.rem(index[0], 2)

    @pl.when(pl.program_id(0) == 0)
    def _():
        fill_tables(flips, far_sources, kinds, transfer, mie, spread, select, chosen, mie_full)

    spheres = counts.shape[0] // 9
    chunk = counts.shape[1] // spheres
    for item in range(chunk):
        at = pl.ds(pl.program_id(0) * chunk + item, 1)
        source_hot = one_hot(9 * spheres, mirrored(sources[at, :], spheres, *flips))
        target_hot = one_hot(spheres, targets[at, :])
        counts[:, item * spheres : (item + 1) * spheres] = dot(
            source_hot.astype(BF16), target_hot.astype(BF16), NT
        ).astype(BF16)


def fill_tables(flips, sources, classes, transfer, mie, spread, select, chosen, mie_full):
    boxes, entries = sources.shape
    row = lax.broadcasted_iota(jnp.int32, (boxes, boxes), 0)
    col = lax.broadcasted_iota(jnp.int32, (boxes, boxes), 1)
    unit = jnp.where(row == col, 1.0, 0.0).astype(BF16)
    around = mirrored(sources[...], boxes, *flips)
    around = dot(around.astype(F32).astype(BF16), unit, TN)
    kinds = dot(classes[...].astype(F32).astype(BF16), unit, TN)
    box_lane = lax.broadcasted_iota(jnp.int32, (entries, select.shape[1]), 1).astype(F32)
    kind_lane = lax.broadcasted_iota(jnp.int32, (entries, transfer.shape[0]), 1).astype(F32)
    hots = []
    for item in range(boxes):
        at = slice(item * entries, (item + 1) * entries)
        hots.append(jnp.where(kinds[:, item : item + 1] == kind_lane, 1.0, 0.0))
        select[at, :] = jnp.where(around[:, item : item + 1] == box_lane, 1.0, 0.0).astype(BF16)
    hot = jnp.concatenate(hots, axis=0)
    dirs = transfer.shape[2]
    chosen[:, :dirs] = dot(hot, transfer[:, 0, :], precision=HIGHEST)
    chosen[:, dirs:] = dot(hot, transfer[:, 1, :], precision=HIGHEST)
    mie_full[...] = dot(spread[...], mie[...], precision=HIGHEST)


def window_kernel(index, transfer, window, *, near_z, near_x, groups, run, top_x, top_y):
    row, col = lax.div(index[0], near_x * run), lax.rem(index[0], near_x * run)
    high, depth = lax.div(row, near_z), lax.rem(row, near_z)
    across, lane = lax.div(col, run), lax.rem(col, run)
    ordinal = lax.broadcasted_iota(jnp.int32, (run, 128), 0)
    for z in range(near_z):
        for x in range(near_x):
            start = (across - x) * run - lane + top_y
            apart_y = jnp.abs(ordinal + (start - top_y))
            for group in range(groups):
                shift = (group - high) * near_z + depth - z
                keep = (apart_y >= 2) | (jnp.abs(shift) >= 2)
                for part in range(2):
                    rows = transfer[shift + top_x, pl.ds(start, run), part, :]
                    window[part, z * near_x + x, group * run : (group + 1) * run, :] = jnp.where(
                        keep, rows, 0.0
                    )


def coarse_kernel(columns, window, partial):
    real, imag = columns[:, 0, :][None], columns[:, 1, :][None]
    partial[:, 0, :] = jnp.sum(real * window[0] - imag * window[1], axis=1)
    partial[:, 1, :] = jnp.sum(imag * window[0] + real * window[1], axis=1)


def near_kernel(before, own, after, counts, table, select, chosen, near, leaf_in, columns):
    coefs = near.shape[0] // 2
    classes = table.shape[0]
    spheres = near.shape[1] // 2
    boxes, dirs = leaf_in.shape[0], leaf_in.shape[1] // 2

    @pl.when(pl.program_id(0) == 0)
    def _():
        leaves = []
        for row in range(3):
            for col, part in enumerate((before, own, after)):
                place = (row * 3 + col) * spheres
                columns[:, place : place + spheres] = part[row, : 2 * coefs, :]
                leaves.append(part[row, 2 * coefs :, :])
        around = jnp.concatenate(
            [
                jnp.concatenate([leaf[:boxes] for leaf in leaves], axis=0),
                jnp.concatenate([leaf[boxes:] for leaf in leaves], axis=0),
            ],
            axis=1,
        )
        picked = dot(select[...], around)
        pick_real, pick_imag = picked[:, :dirs], picked[:, dirs:]
        move_real, move_imag = chosen[:, :dirs], chosen[:, dirs:]
        got_real = pick_real * move_real - pick_imag * move_imag
        got_imag = pick_imag * move_real + pick_real * move_imag
        leaf_in[:, :dirs] = jnp.sum(got_real.reshape(boxes, -1, dirs), axis=1)
        leaf_in[:, dirs:] = jnp.sum(got_imag.reshape(boxes, -1, dirs), axis=1)
        near[...] = jnp.zeros(near.shape, F32)

    gathered = dot(columns[...], counts[...]).astype(BF16)
    total = near[...]
    for item in range(classes):
        at = slice(item * spheres, (item + 1) * spheres)
        pair = jnp.concatenate([gathered[:coefs, at], gathered[coefs:, at]], axis=1)
        total = total + dot(table[item], pair)
    near[...] = total


def arrive(partial, near, leaf_in, receive, cosines, sines, member, leaf_cos, leaf_sin, mie_full):
    _, dirs = leaf_cos.shape
    coefs = near.shape[0] // 2
    column_real = jnp.sum(partial[:, 0, :], axis=0, keepdims=True)
    column_imag = jnp.sum(partial[:, 1, :], axis=0, keepdims=True)
    incoming = leaf_in + jnp.concatenate(
        [
            column_real * leaf_cos - column_imag * leaf_sin,
            column_real * leaf_sin + column_imag * leaf_cos,
        ],
        axis=1,
    )
    high, low = split(incoming)
    spread = dot(high, member, TN) + dot(low, member, TN)
    real, imag = spread[:dirs], spread[dirs:]
    arriving = jnp.concatenate(
        [real * cosines - imag * sines, real * sines + imag * cosines], axis=1
    ).astype(BF16)
    total = near + dot(receive, arriving)
    half = total.shape[1] // 2
    field_real = total[:coefs, :half] - total[coefs:, half:]
    field_imag = total[coefs:, :half] + total[:coefs, half:]
    mie_real, mie_imag = mie_full[:coefs], mie_full[coefs:]
    return jnp.concatenate(
        [
            field_real * mie_real - field_imag * mie_imag,
            field_real * mie_imag + field_imag * mie_real,
        ],
        axis=0,
    )


def sums_kernel(vector, scattered, sums):
    u, d = vector[...], scattered[...]
    sums[...] = lanes([(0, inner(u, u)), (1, inner(u, d)), (2, inner(d, d))])


def middle_kernel(
    partial,
    near,
    leaf_in,
    pattern,
    receive,
    cosines,
    sines,
    box,
    leaf_cos,
    leaf_sin,
    mie_full,
    applied,
    halo,
    column,
):
    member = one_hot(leaf_cos.shape[0], box[...]).astype(BF16)
    scattered = arrive(
        partial[...],
        near[...],
        leaf_in[...],
        receive[...],
        cosines[...],
        sines[...],
        member,
        leaf_cos[...],
        leaf_sin[...],
        mie_full[...],
    )
    applied[...] = scattered
    emit(
        scattered,
        pattern[...],
        cosines[...],
        sines[...],
        member,
        leaf_cos[...],
        leaf_sin[...],
        halo,
        column,
    )


def last_kernel(
    vector,
    scattered,
    partial,
    near,
    leaf_in,
    receive,
    cosines,
    sines,
    box,
    leaf_cos,
    leaf_sin,
    mie_full,
    sums,
    applied,
    everyone,
):
    member = one_hot(leaf_cos.shape[0], box[...]).astype(BF16)
    twice = arrive(
        partial[...],
        near[...],
        leaf_in[...],
        receive[...],
        cosines[...],
        sines[...],
        member,
        leaf_cos[...],
        leaf_sin[...],
        mie_full[...],
    )
    applied[...] = twice
    row = sums[...] + lanes(
        [(3, inner(vector[...], twice)), (4, inner(scattered[...], twice)), (5, inner(twice, twice))]
    )
    everyone[...] = jnp.broadcast_to(row[None], everyone.shape)


def relay_kernel(parts, everyone):
    everyone[...] = jnp.broadcast_to(jnp.sum(parts[...], axis=0, keepdims=True), everyone.shape)


def solve_kernel(parts, vector, scattered, twice, solution, residual):
    row = jnp.sum(parts[...], axis=0)
    lane = lax.broadcasted_iota(jnp.int32, row.shape, 1)

    def total(place):
        value = jnp.sum(jnp.where(lane == place, row, 0.0), axis=1, keepdims=True)
        return jnp.broadcast_to(value, (8, 128))

    uu, ud, dd, ue, de, ee = (total(place) for place in range(6))
    beta = jnp.sqrt(uu)
    along = ud / uu
    across = dd - along * ud
    size = jnp.sqrt(across)
    h00 = 1.0 - along
    h10 = size / beta
    turned = de - along * ue
    h01 = (ue - along * ud) / (size * beta)
    h11 = 1.0 + along - turned / across
    rest_u = ue / uu
    rest_d = turned / across
    left = ee - rest_u * ue - rest_d * turned
    h21 = jnp.sqrt(left) / size
    n00 = h00 * h00 + h10 * h10
    n01 = h00 * h01 + h10 * h11
    n11 = h01 * h01 + h11 * h11 + h21 * h21
    l00 = jnp.sqrt(n00)
    l10 = n01 / l00
    l11 = jnp.sqrt(n11 - l10 * l10)
    m0 = beta * h00 / l00
    m1 = (beta * h01 - l10 * m0) / l11
    y1 = m1 / l11
    y0 = (m0 - l10 * y1) / l00
    z0 = h00 * y0 + h01 * y1
    z1 = h10 * y0 + h11 * y1
    step = y1 / size
    sol_u = y0 / beta + step * along
    sol_d = -step
    res_u = (beta - z0) / beta - z1 / size * along + step * (rest_u - rest_d * along)
    res_d = z1 / size + step * rest_d
    res_e = -step
    u, d, e = vector[...], scattered[...], twice[...]
    solution[...] = sol_u[0:1] * u + sol_d[0:1] * d
    residual[...] = res_u[0:1] * u + res_d[0:1] * d + res_e[0:1] * e


def swap(x, axes, first):
    pairs = [(i, i + 1) for i in range(first, lax.axis_size(axes) - 1, 2)]
    return lax.ppermute(x, axes, pairs + [(j, i) for i, j in pairs])


def exchange(x, axes):
    return lax.all_to_all(x, axes, split_axis=0, concat_axis=0, tiled=True)


def local(
    incident,
    mie,
    offsets,
    sphere_box,
    near_table,
    near_src,
    near_dst,
    pattern,
    receive,
    leaf_transfer,
    far_src,
    far_cls,
    coarse_transfer,
):
    coefs = incident.shape[1]
    spheres = incident.shape[4]
    rows = 2 * coefs
    dirs = pattern.shape[1]
    boxes, entries = far_src.shape[2:]
    classes, pairs = near_src.shape[2:]
    high_count, near_z = lax.axis_size("bx_0"), lax.axis_size("bx_1")
    near_x = lax.axis_size("by_0")
    run = lax.axis_size(("by_1", "by_2"))
    first_count, second_count = lax.axis_size(FIRST), lax.axis_size(SECOND)
    index = lax.axis_index(BX + BY).astype(jnp.int32).reshape(1)

    planes = jnp.asarray(directions(dirs)[:, :, None].astype(np.float32))
    centre = KAPPA * (leaf_centers(boxes).T @ directions(dirs))
    leaf_cos = jnp.asarray(np.cos(centre).astype(np.float32))
    leaf_sin = jnp.asarray(np.sin(centre).astype(np.float32))

    vector = incident.reshape(rows, spheres)
    box = sphere_box.reshape(1, spheres)
    pattern = pattern.transpose(0, 2, 1)
    receive = receive.reshape(rows, dirs)

    halo_shape = kept((1, rows + 2 * boxes, spheres), BF16)
    column_shape = kept((first_count, 2, dirs))
    halo, column, cosines, sines, send = call(
        first_kernel,
        (
            halo_shape,
            column_shape,
            kept((dirs, spheres)),
            kept((dirs, spheres)),
            kept((2 * dirs, coefs), BF16),
        ),
        (vector, pattern, offsets.reshape(3, 1, spheres), planes, box, leaf_cos, leaf_sin),
        flops=1 << 26,
    )
    chunk = classes // 2
    whole = pl.BlockSpec(memory_space=pltpu.VMEM)

    def prepare():
        spread = mie_spread(coefs, mie.shape[1])
        zero = np.zeros_like(spread)
        return call(
            functools.partial(count_kernel, across_y=near_x * run),
            (
                shape((9 * spheres, classes * spheres), BF16),
                kept((boxes * entries, 9 * boxes), BF16),
                kept((boxes * entries, 2 * dirs)),
                kept((rows, spheres)),
            ),
            (
                index,
                near_src.reshape(classes, pairs),
                near_dst.reshape(classes, pairs),
                far_src.reshape(boxes, entries),
                far_cls.reshape(boxes, entries),
                leaf_transfer,
                mie.reshape(2 * mie.shape[1], spheres),
                jnp.asarray(np.block([[spread, zero], [zero, spread]])),
            ),
            flops=1 << 31,
            grid=(classes // chunk,),
            in_specs=[pl.BlockSpec(memory_space=pltpu.SMEM)] + [whole] * 7,
            out_specs=(
                pl.BlockSpec((9 * spheres, chunk * spheres), lambda k: (0, k)),
                whole,
                whole,
                whole,
            ),
        )

    def windows():
        return call(
            functools.partial(
                window_kernel,
                near_z=near_z,
                near_x=near_x,
                groups=high_count,
                run=run,
                top_x=high_count * near_z - 1,
                top_y=near_x * run - 1,
            ),
            kept((2, second_count, first_count, dirs)),
            (index, coarse_transfer.transpose(1, 2, 0, 3)),
            flops=1 << 28,
        )

    def apply(halo, column, window, counts, select, chosen):
        columns = exchange(column, FIRST)
        ahead = swap(halo, BX, 0)
        behind = swap(halo, BX, 1)
        line = jnp.concatenate([behind, halo, ahead], axis=0)
        right = swap(line, BY, 0)
        left = swap(line, BY, 1)
        partial = call(
            coarse_kernel,
            kept((second_count, 2, dirs)),
            (resident(columns), resident(window)),
            1 << 24,
        )
        partial = exchange(partial, SECOND)
        near, leaf_in = call(
            near_kernel,
            (kept((rows, 2 * spheres)), kept((boxes, 2 * dirs))),
            (
                resident(left),
                resident(line),
                resident(right),
                counts,
                near_table.reshape(classes, rows, coefs),
                resident(select),
                resident(chosen),
            ),
            flops=1 << 31,
            grid=(classes // chunk,),
            in_specs=[
                whole,
                whole,
                whole,
                pl.BlockSpec((9 * spheres, chunk * spheres), lambda k: (0, k)),
                pl.BlockSpec((chunk, rows, coefs), lambda k: (k, 0, 0)),
                whole,
                whole,
            ],
            out_specs=(whole, whole),
            scratch_shapes=[pltpu.VMEM((rows, 9 * spheres), BF16)],
        )
        return resident(partial), resident(near), resident(leaf_in)

    window = windows()
    counts, select, chosen, mie_full = prepare()
    partial, near, leaf_in = apply(halo, column, window, counts, select, chosen)
    far = (
        receive,
        resident(cosines),
        resident(sines),
        box,
        leaf_cos,
        leaf_sin,
        resident(mie_full),
    )
    once, halo, column = call(
        middle_kernel,
        (kept((rows, spheres)), halo_shape, column_shape),
        (partial, near, leaf_in, resident(send)) + far,
        flops=1 << 26,
    )
    sums = call(sums_kernel, kept((1, 128)), (vector, resident(once)), 1 << 24)
    partial, near, leaf_in = apply(halo, column, window, counts, select, chosen)
    once = resident(once)
    twice, everyone = call(
        last_kernel,
        (kept((rows, spheres)), kept((first_count, 1, 128))),
        (vector, once, partial, near, leaf_in) + far + (resident(sums),),
        flops=1 << 26,
    )
    everyone = call(
        relay_kernel, kept((second_count, 1, 128)), (resident(exchange(everyone, FIRST)),), 1 << 20
    )
    solved, residual = call(
        solve_kernel,
        (shape((rows, spheres)), shape((rows, spheres))),
        (resident(exchange(everyone, SECOND)), vector, once, resident(twice)),
        flops=1 << 24,
    )
    return solved.reshape(incident.shape), residual.reshape(incident.shape)


def build(devices, sizes):
    torus = Mesh(devices.reshape(sizes), BX + BY)
    placed = (
        P(None, None, BX, BY, None),
        P(None, None, BX, BY, None),
        P(None, BX, BY, None),
        P(BX, BY, None),
        P(),
        P(BX, BY, None, None),
        P(BX, BY, None, None),
        P(),
        P(),
        P(),
        P(BX, BY, None, None),
        P(BX, BY, None, None),
        P(),
    )
    return jax.shard_map(
        local,
        mesh=torus,
        in_specs=placed,
        out_specs=(P(None, None, BX, BY, None), P(None, None, BX, BY, None)),
        check_vma=False,
    )


def solution(mesh):
    return build(mesh.devices, (2, 8, 4, 4, 2))
```

```python
import functools
import math

import jax
import jax.numpy as jnp
import numpy as np
from jax import lax
from jax.experimental import pallas as pl
from jax.experimental.pallas import tpu as pltpu
from jax.sharding import Mesh
from jax.sharding import PartitionSpec as P

BX = ("bx_0", "bx_1")
BY = ("by_0", "by_1", "by_2")
FIRST = ("bx_0", "by_1", "by_2")
SECOND = ("bx_1", "by_0")

HIGHEST = lax.Precision.HIGHEST
KAPPA = 1.5
GOLDEN = 2.399963229728653
F32 = jnp.float32
BF16 = jnp.bfloat16
NT = (((1,), (1,)), ((), ()))
TN = (((0,), (0,)), ((), ()))
INTERPRET = False


def call(kernel, out_shape, operands, flops=0, **kw):
    if "grid" not in kw:
        kw["in_specs"] = [
            pl.BlockSpec(memory_space=pltpu.SMEM if op.ndim == 1 else pltpu.VMEM)
            for op in operands
        ]
    return pl.pallas_call(
        kernel,
        out_shape=out_shape,
        interpret=INTERPRET,
        cost_estimate=pl.CostEstimate(flops=flops, transcendentals=0, bytes_accessed=1 << 20),
        **kw,
    )(*operands)


def resident(x):
    return x if INTERPRET else pltpu.with_memory_space_constraint(x, pltpu.VMEM)


def kept(dims, dtype=F32):
    return shape(dims, dtype) if INTERPRET else pltpu.VMEM(dims, dtype)


def shape(dims, dtype=F32):
    return jax.ShapeDtypeStruct(dims, dtype)


def directions(number):
    ordinal = np.arange(number, dtype=np.float64)
    height = 1.0 - (2.0 * ordinal + 1.0) / number
    radius = np.sqrt(1.0 - height * height)
    return np.stack([radius * np.cos(GOLDEN * ordinal), radius * np.sin(GOLDEN * ordinal), height])


def leaf_centers(number):
    ordinal = np.arange(number)
    return np.stack(
        [
            2.0 * (ordinal % 2) - 1.0,
            2.0 * (ordinal // 2 % 2) - 1.0,
            2.0 * (ordinal // 4) - (number // 4 - 1),
        ]
    )


def mie_spread(coef_count, mie_count):
    half_count = coef_count // 2
    table = np.zeros((coef_count, mie_count), np.float32)
    for number in range(coef_count):
        degree = math.isqrt(number % half_count + 1)
        table[number, number // half_count * (mie_count // 2) + degree - 1] = 1.0
    return table


def dot(a, b, dims=(((1,), (0,)), ((), ())), precision=None):
    return lax.dot_general(a, b, dims, precision=precision, preferred_element_type=F32)


def split(x):
    high = x.astype(BF16)
    return high, (x - high.astype(F32)).astype(BF16)


def one_hot(rows, row):
    ordinal = lax.broadcasted_iota(jnp.int32, (rows, row.shape[1]), 0)
    return jnp.where(ordinal == row, 1.0, 0.0)


def emit(vector, pattern, cosines, sines, member, leaf_cos, leaf_sin, halo_ref, column_ref):
    coefs = vector.shape[0] // 2
    boxes, dirs = leaf_cos.shape
    rounded = vector.astype(BF16)
    halo_ref[0, : 2 * coefs, :] = rounded
    by_real = dot(pattern, rounded[:coefs])
    by_imag = dot(pattern, rounded[coefs:])
    real = by_real[:dirs] - by_imag[dirs:]
    imag = by_real[dirs:] + by_imag[:dirs]
    out = jnp.concatenate([real * cosines + imag * sines, imag * cosines - real * sines], axis=0)
    high, low = split(out)
    leaf = dot(member, high, NT) + dot(member, low, NT)
    leaf_real, leaf_imag = leaf[:, :dirs], leaf[:, dirs:]
    halo_ref[0, 2 * coefs : 2 * coefs + boxes, :] = leaf_real.astype(BF16)
    halo_ref[0, 2 * coefs + boxes :, :] = leaf_imag.astype(BF16)
    column_real = jnp.sum(leaf_real * leaf_cos + leaf_imag * leaf_sin, axis=0, keepdims=True)
    column_imag = jnp.sum(leaf_imag * leaf_cos - leaf_real * leaf_sin, axis=0, keepdims=True)
    tile = (16, dirs)
    even = lax.rem(lax.broadcasted_iota(jnp.int32, tile, 0), 2) == 0
    pairs = jnp.where(
        even, jnp.broadcast_to(column_real, tile), jnp.broadcast_to(column_imag, tile)
    ).astype(BF16)
    for item in range(column_ref.shape[0] // 16):
        column_ref[item * 16 : (item + 1) * 16, :] = pairs


def lanes(values):
    lane = lax.broadcasted_iota(jnp.int32, (1, 128), 1)
    row = jnp.zeros((1, 128), F32)
    for place, value in values:
        row = row + jnp.where(lane == place, value, 0.0)
    return row


def inner(a, b):
    return jnp.sum(jnp.sum(a * b, axis=0, keepdims=True), axis=1, keepdims=True)


def first_kernel(
    vector, pattern, offsets, planes, box, leaf_cos, leaf_sin, halo, column, cos_ref, sin_ref, send
):
    turned = jnp.concatenate([pattern[0].T, pattern[1].T], axis=0)
    send[...] = turned
    phases = KAPPA * (
        planes[0] * offsets[0] + planes[1] * offsets[1] + planes[2] * offsets[2]
    )
    cosines, sines = jnp.cos(phases), jnp.sin(phases)
    cos_ref[...] = cosines
    sin_ref[...] = sines
    member = one_hot(leaf_cos.shape[0], box[...]).astype(BF16)
    emit(vector[...], turned, cosines, sines, member, leaf_cos[...], leaf_sin[...], halo, column)


def mirrored(sources, width, flip_x, flip_y):
    line = 3 * width
    flat = jnp.where(sources < line, 0, jnp.where(sources < 2 * line, 1, 2))
    within = sources - line * flat
    side = jnp.where(within < width, 0, jnp.where(within < 2 * width, 1, 2))
    return sources + flip_x * (2 - 2 * flat) * line + flip_y * (2 - 2 * side) * width


def count_kernel(
    index,
    sources,
    targets,
    far_sources,
    kinds,
    transfer,
    mie,
    spread,
    counts,
    select,
    chosen,
    mie_full,
    *,
    across_y,
):
    flips = lax.rem(lax.div(index[0], across_y), 2), lax.rem(index[0], 2)

    @pl.when(pl.program_id(0) == 0)
    def _():
        fill_tables(flips, far_sources, kinds, transfer, mie, spread, select, chosen, mie_full)

    spheres = counts.shape[0] // 9
    chunk = counts.shape[1] // spheres
    for item in range(chunk):
        at = pl.ds(pl.program_id(0) * chunk + item, 1)
        source_hot = one_hot(9 * spheres, mirrored(sources[at, :], spheres, *flips))
        target_hot = one_hot(spheres, targets[at, :])
        counts[:, item * spheres : (item + 1) * spheres] = dot(
            source_hot.astype(BF16), target_hot.astype(BF16), NT
        ).astype(BF16)


def fill_tables(flips, sources, classes, transfer, mie, spread, select, chosen, mie_full):
    boxes, entries = sources.shape
    row = lax.broadcasted_iota(jnp.int32, (boxes, boxes), 0)
    col = lax.broadcasted_iota(jnp.int32, (boxes, boxes), 1)
    unit = jnp.where(row == col, 1.0, 0.0).astype(BF16)
    around = mirrored(sources[...], boxes, *flips)
    around = dot(around.astype(F32).astype(BF16), unit, TN)
    kinds = dot(classes[...].astype(F32).astype(BF16), unit, TN)
    box_lane = lax.broadcasted_iota(jnp.int32, (entries, select.shape[1]), 1).astype(F32)
    kind_lane = lax.broadcasted_iota(jnp.int32, (entries, transfer.shape[0]), 1).astype(F32)
    hots = []
    for item in range(boxes):
        at = slice(item * entries, (item + 1) * entries)
        hots.append(jnp.where(kinds[:, item : item + 1] == kind_lane, 1.0, 0.0))
        select[at, :] = jnp.where(around[:, item : item + 1] == box_lane, 1.0, 0.0).astype(BF16)
    hot = jnp.concatenate(hots, axis=0)
    dirs = transfer.shape[2]
    chosen[:, :dirs] = dot(hot, transfer[:, 0, :], precision=HIGHEST)
    chosen[:, dirs:] = dot(hot, transfer[:, 1, :], precision=HIGHEST)
    mie_full[...] = dot(spread[...], mie[...], precision=HIGHEST)


def near_kernel(before, own, after, counts, table, select, chosen, near, leaf_in, columns):
    coefs = near.shape[0] // 2
    classes = table.shape[0]
    spheres = near.shape[1] // 2
    boxes, dirs = leaf_in.shape[0], leaf_in.shape[1] // 2

    @pl.when(pl.program_id(0) == 0)
    def _():
        leaves = []
        for row in range(3):
            for col, part in enumerate((before, own, after)):
                place = (row * 3 + col) * spheres
                columns[:, place : place + spheres] = part[row, : 2 * coefs, :]
                leaves.append(part[row, 2 * coefs :, :])
        around = jnp.concatenate(
            [
                jnp.concatenate([leaf[:boxes] for leaf in leaves], axis=0),
                jnp.concatenate([leaf[boxes:] for leaf in leaves], axis=0),
            ],
            axis=1,
        )
        picked = dot(select[...], around)
        pick_real, pick_imag = picked[:, :dirs], picked[:, dirs:]
        move_real, move_imag = chosen[:, :dirs], chosen[:, dirs:]
        got_real = pick_real * move_real - pick_imag * move_imag
        got_imag = pick_imag * move_real + pick_real * move_imag
        leaf_in[:, :dirs] = jnp.sum(got_real.reshape(boxes, -1, dirs), axis=1)
        leaf_in[:, dirs:] = jnp.sum(got_imag.reshape(boxes, -1, dirs), axis=1)
        near[...] = jnp.zeros(near.shape, F32)

    gathered = dot(columns[...], counts[...]).astype(BF16)
    total = near[...]
    for item in range(classes):
        at = slice(item * spheres, (item + 1) * spheres)
        pair = jnp.concatenate([gathered[:coefs, at], gathered[coefs:, at]], axis=1)
        total = total + dot(table[item], pair)
    near[...] = total


def coarse(columns, window):
    rows = columns.shape[0]
    values = columns.astype(F32)
    even = lax.rem(lax.broadcasted_iota(jnp.int32, values.shape, 0), 2) == 0
    turned = jnp.where(even, pltpu.roll(values, rows - 1, 0), pltpu.roll(values, 1, 0))
    real = window * jnp.where(even, values, -values)
    imag = window * turned
    return jnp.sum(real, axis=0, keepdims=True), jnp.sum(imag, axis=0, keepdims=True)


def arrive(columns, window, near, leaf_in, receive, cosines, sines, member, leaf_cos, leaf_sin, mie_full):
    _, dirs = leaf_cos.shape
    coefs = near.shape[0] // 2
    column_real, column_imag = coarse(columns, window)
    incoming = leaf_in + jnp.concatenate(
        [
            column_real * leaf_cos - column_imag * leaf_sin,
            column_real * leaf_sin + column_imag * leaf_cos,
        ],
        axis=1,
    )
    high, low = split(incoming)
    spread = dot(high, member, TN) + dot(low, member, TN)
    real, imag = spread[:dirs], spread[dirs:]
    arriving = jnp.concatenate(
        [real * cosines - imag * sines, real * sines + imag * cosines], axis=1
    ).astype(BF16)
    total = near + dot(receive, arriving)
    half = total.shape[1] // 2
    field_real = total[:coefs, :half] - total[coefs:, half:]
    field_imag = total[coefs:, :half] + total[:coefs, half:]
    mie_real, mie_imag = mie_full[:coefs], mie_full[coefs:]
    return jnp.concatenate(
        [
            field_real * mie_real - field_imag * mie_imag,
            field_real * mie_imag + field_imag * mie_real,
        ],
        axis=0,
    )


def sums_kernel(vector, scattered, sums):
    u, d = vector[...], scattered[...]
    sums[...] = lanes([(0, inner(u, u)), (1, inner(u, d)), (2, inner(d, d))])


def middle_kernel(
    columns,
    window,
    near,
    leaf_in,
    pattern,
    receive,
    cosines,
    sines,
    box,
    leaf_cos,
    leaf_sin,
    mie_full,
    applied,
    halo,
    column,
):
    member = one_hot(leaf_cos.shape[0], box[...]).astype(BF16)
    scattered = arrive(
        columns[...],
        window[...],
        near[...],
        leaf_in[...],
        receive[...],
        cosines[...],
        sines[...],
        member,
        leaf_cos[...],
        leaf_sin[...],
        mie_full[...],
    )
    applied[...] = scattered
    emit(
        scattered,
        pattern[...],
        cosines[...],
        sines[...],
        member,
        leaf_cos[...],
        leaf_sin[...],
        halo,
        column,
    )


def last_kernel(
    vector,
    scattered,
    columns,
    window,
    near,
    leaf_in,
    receive,
    cosines,
    sines,
    box,
    leaf_cos,
    leaf_sin,
    mie_full,
    sums,
    applied,
    everyone,
):
    member = one_hot(leaf_cos.shape[0], box[...]).astype(BF16)
    twice = arrive(
        columns[...],
        window[...],
        near[...],
        leaf_in[...],
        receive[...],
        cosines[...],
        sines[...],
        member,
        leaf_cos[...],
        leaf_sin[...],
        mie_full[...],
    )
    applied[...] = twice
    row = sums[...] + lanes(
        [(3, inner(vector[...], twice)), (4, inner(scattered[...], twice)), (5, inner(twice, twice))]
    )
    everyone[...] = jnp.broadcast_to(row[None], everyone.shape)


def relay_kernel(parts, everyone):
    everyone[...] = jnp.broadcast_to(jnp.sum(parts[...], axis=0, keepdims=True), everyone.shape)


def solve_kernel(parts, vector, scattered, twice, solution, residual):
    row = jnp.sum(parts[...], axis=0)
    lane = lax.broadcasted_iota(jnp.int32, row.shape, 1)

    def total(place):
        value = jnp.sum(jnp.where(lane == place, row, 0.0), axis=1, keepdims=True)
        return jnp.broadcast_to(value, (8, 128))

    uu, ud, dd, ue, de, ee = (total(place) for place in range(6))
    beta = jnp.sqrt(uu)
    along = ud / uu
    across = dd - along * ud
    size = jnp.sqrt(across)
    h00 = 1.0 - along
    h10 = size / beta
    turned = de - along * ue
    h01 = (ue - along * ud) / (size * beta)
    h11 = 1.0 + along - turned / across
    rest_u = ue / uu
    rest_d = turned / across
    left = ee - rest_u * ue - rest_d * turned
    h21 = jnp.sqrt(left) / size
    n00 = h00 * h00 + h10 * h10
    n01 = h00 * h01 + h10 * h11
    n11 = h01 * h01 + h11 * h11 + h21 * h21
    l00 = jnp.sqrt(n00)
    l10 = n01 / l00
    l11 = jnp.sqrt(n11 - l10 * l10)
    m0 = beta * h00 / l00
    m1 = (beta * h01 - l10 * m0) / l11
    y1 = m1 / l11
    y0 = (m0 - l10 * y1) / l00
    z0 = h00 * y0 + h01 * y1
    z1 = h10 * y0 + h11 * y1
    step = y1 / size
    sol_u = y0 / beta + step * along
    sol_d = -step
    res_u = (beta - z0) / beta - z1 / size * along + step * (rest_u - rest_d * along)
    res_d = z1 / size + step * rest_d
    res_e = -step
    u, d, e = vector[...], scattered[...], twice[...]
    solution[...] = sol_u[0:1] * u + sol_d[0:1] * d
    residual[...] = res_u[0:1] * u + res_d[0:1] * d + res_e[0:1] * e


def swap(x, axes, first):
    pairs = [(i, i + 1) for i in range(first, lax.axis_size(axes) - 1, 2)]
    return lax.ppermute(x, axes, pairs + [(j, i) for i, j in pairs])


def exchange(x, axes):
    return lax.all_to_all(x, axes, split_axis=0, concat_axis=0, tiled=True)


def local(
    incident,
    mie,
    offsets,
    sphere_box,
    near_table,
    near_src,
    near_dst,
    pattern,
    receive,
    leaf_transfer,
    far_src,
    far_cls,
    coarse_transfer,
):
    coefs = incident.shape[1]
    spheres = incident.shape[4]
    rows = 2 * coefs
    dirs = pattern.shape[1]
    boxes, entries = far_src.shape[2:]
    classes, pairs = near_src.shape[2:]
    across_x, across_y = lax.axis_size(BX), lax.axis_size(BY)
    first_pos, second_pos = lax.axis_index(BX), lax.axis_index(BY)
    first_count, second_count = lax.axis_size(FIRST), lax.axis_size(SECOND)
    index = lax.axis_index(BX + BY).astype(jnp.int32).reshape(1)

    planes = jnp.asarray(directions(dirs)[:, :, None].astype(np.float32))
    centre = KAPPA * (leaf_centers(boxes).T @ directions(dirs))
    leaf_cos = jnp.asarray(np.cos(centre).astype(np.float32))
    leaf_sin = jnp.asarray(np.sin(centre).astype(np.float32))

    vector = incident.reshape(rows, spheres)
    box = sphere_box.reshape(1, spheres)
    pattern = pattern.transpose(0, 2, 1)
    receive = receive.reshape(rows, dirs)

    halo_shape = kept((1, rows + 2 * boxes, spheres), BF16)
    column_shape = kept((2 * across_x * across_y, dirs), BF16)
    halo, column, cosines, sines, send = call(
        first_kernel,
        (
            halo_shape,
            column_shape,
            kept((dirs, spheres)),
            kept((dirs, spheres)),
            kept((2 * dirs, coefs), BF16),
        ),
        (vector, pattern, offsets.reshape(3, 1, spheres), planes, box, leaf_cos, leaf_sin),
        flops=1 << 26,
    )
    chunk = classes // 2
    whole = pl.BlockSpec(memory_space=pltpu.VMEM)

    def prepare():
        spread = mie_spread(coefs, mie.shape[1])
        zero = np.zeros_like(spread)
        return call(
            functools.partial(count_kernel, across_y=across_y),
            (
                shape((9 * spheres, classes * spheres), BF16),
                kept((boxes * entries, 9 * boxes), BF16),
                kept((boxes * entries, 2 * dirs)),
                kept((rows, spheres)),
            ),
            (
                index,
                near_src.reshape(classes, pairs),
                near_dst.reshape(classes, pairs),
                far_src.reshape(boxes, entries),
                far_cls.reshape(boxes, entries),
                leaf_transfer,
                mie.reshape(2 * mie.shape[1], spheres),
                jnp.asarray(np.block([[spread, zero], [zero, spread]])),
            ),
            flops=1 << 31,
            grid=(classes // chunk,),
            in_specs=[pl.BlockSpec(memory_space=pltpu.SMEM)] + [whole] * 7,
            out_specs=(
                pl.BlockSpec((9 * spheres, chunk * spheres), lambda k: (0, k)),
                whole,
                whole,
                whole,
            ),
        )

    def windows():
        taken = lax.dynamic_slice(
            coarse_transfer.transpose(1, 2, 0, 3),
            (across_x - 1 - first_pos, across_y - 1 - second_pos, 0, 0),
            (across_x, across_y, 2, dirs),
        )
        apart_x = jnp.abs(jnp.arange(across_x, dtype=jnp.int32) - first_pos)[:, None]
        apart_y = jnp.abs(jnp.arange(across_y, dtype=jnp.int32) - second_pos)[None]
        keep = (apart_x >= 2) | (apart_y >= 2)
        taken = jnp.where(keep[:, :, None, None], taken, 0.0)
        return taken.reshape(2 * across_x * across_y, dirs)

    def apply(halo, column, counts, select, chosen):
        columns = exchange(column.reshape(-1, 2, dirs), BX + BY).reshape(-1, dirs)
        ahead = swap(halo, BX, 0)
        behind = swap(halo, BX, 1)
        line = jnp.concatenate([behind, halo, ahead], axis=0)
        right = swap(line, BY, 0)
        left = swap(line, BY, 1)
        near, leaf_in = call(
            near_kernel,
            (kept((rows, 2 * spheres)), kept((boxes, 2 * dirs))),
            (
                resident(left),
                resident(line),
                resident(right),
                counts,
                near_table.reshape(classes, rows, coefs),
                resident(select),
                resident(chosen),
            ),
            flops=1 << 31,
            grid=(classes // chunk,),
            in_specs=[
                whole,
                whole,
                whole,
                pl.BlockSpec((9 * spheres, chunk * spheres), lambda k: (0, k)),
                pl.BlockSpec((chunk, rows, coefs), lambda k: (k, 0, 0)),
                whole,
                whole,
            ],
            out_specs=(whole, whole),
            scratch_shapes=[pltpu.VMEM((rows, 9 * spheres), BF16)],
        )
        return resident(columns), resident(window), resident(near), resident(leaf_in)

    window = windows()
    counts, select, chosen, mie_full = prepare()
    inward = apply(halo, column, counts, select, chosen)
    far = (
        receive,
        resident(cosines),
        resident(sines),
        box,
        leaf_cos,
        leaf_sin,
        resident(mie_full),
    )
    once, halo, column = call(
        middle_kernel,
        (kept((rows, spheres)), halo_shape, column_shape),
        inward + (resident(send),) + far,
        flops=1 << 26,
    )
    sums = call(sums_kernel, kept((1, 128)), (vector, resident(once)), 1 << 24)
    inward = apply(halo, column, counts, select, chosen)
    once = resident(once)
    twice, everyone = call(
        last_kernel,
        (kept((rows, spheres)), kept((first_count, 1, 128))),
        (vector, once) + inward + far + (resident(sums),),
        flops=1 << 26,
    )
    everyone = call(
        relay_kernel, kept((second_count, 1, 128)), (resident(exchange(everyone, FIRST)),), 1 << 20
    )
    solved, residual = call(
        solve_kernel,
        (shape((rows, spheres)), shape((rows, spheres))),
        (resident(exchange(everyone, SECOND)), vector, once, resident(twice)),
        flops=1 << 24,
    )
    return solved.reshape(incident.shape), residual.reshape(incident.shape)


def build(devices, sizes):
    torus = Mesh(devices.reshape(sizes), BX + BY)
    placed = (
        P(None, None, BX, BY, None),
        P(None, None, BX, BY, None),
        P(None, BX, BY, None),
        P(BX, BY, None),
        P(),
        P(BX, BY, None, None),
        P(BX, BY, None, None),
        P(),
        P(),
        P(),
        P(BX, BY, None, None),
        P(BX, BY, None, None),
        P(),
    )
    return jax.shard_map(
        local,
        mesh=torus,
        in_specs=placed,
        out_specs=(P(None, None, BX, BY, None), P(None, None, BX, BY, None)),
        check_vma=False,
    )


def solution(mesh):
    return build(mesh.devices, (2, 8, 4, 4, 2))
```

```python
import functools
import math

import jax
import jax.numpy as jnp
import numpy as np
from jax import lax
from jax.experimental import pallas as pl
from jax.experimental.pallas import tpu as pltpu
from jax.sharding import Mesh
from jax.sharding import PartitionSpec as P

BX = ("bx_0", "bx_1")
BY = ("by_0", "by_1", "by_2")
FIRST = ("bx_0", "by_1", "by_2")
SECOND = ("bx_1", "by_0")

HIGHEST = lax.Precision.HIGHEST
KAPPA = 1.5
GOLDEN = 2.399963229728653
F32 = jnp.float32
BF16 = jnp.bfloat16
NT = (((1,), (1,)), ((), ()))
TN = (((0,), (0,)), ((), ()))
INTERPRET = False


def call(kernel, out_shape, operands, flops=0, **kw):
    if "grid" not in kw:
        kw["in_specs"] = [
            pl.BlockSpec(memory_space=pltpu.SMEM if op.ndim == 1 else pltpu.VMEM)
            for op in operands
        ]
    return pl.pallas_call(
        kernel,
        out_shape=out_shape,
        interpret=INTERPRET,
        cost_estimate=pl.CostEstimate(flops=flops, transcendentals=0, bytes_accessed=1 << 20),
        **kw,
    )(*operands)


def resident(x):
    return x if INTERPRET else pltpu.with_memory_space_constraint(x, pltpu.VMEM)


def kept(dims, dtype=F32):
    return shape(dims, dtype) if INTERPRET else pltpu.VMEM(dims, dtype)


def shape(dims, dtype=F32):
    return jax.ShapeDtypeStruct(dims, dtype)


def directions(number):
    ordinal = np.arange(number, dtype=np.float64)
    height = 1.0 - (2.0 * ordinal + 1.0) / number
    radius = np.sqrt(1.0 - height * height)
    return np.stack([radius * np.cos(GOLDEN * ordinal), radius * np.sin(GOLDEN * ordinal), height])


def leaf_centers(number):
    ordinal = np.arange(number)
    return np.stack(
        [
            2.0 * (ordinal % 2) - 1.0,
            2.0 * (ordinal // 2 % 2) - 1.0,
            2.0 * (ordinal // 4) - (number // 4 - 1),
        ]
    )


def mie_spread(coef_count, mie_count):
    half_count = coef_count // 2
    table = np.zeros((coef_count, mie_count), np.float32)
    for number in range(coef_count):
        degree = math.isqrt(number % half_count + 1)
        table[number, number // half_count * (mie_count // 2) + degree - 1] = 1.0
    return table


def dot(a, b, dims=(((1,), (0,)), ((), ())), precision=None):
    return lax.dot_general(a, b, dims, precision=precision, preferred_element_type=F32)


def split(x):
    high = x.astype(BF16)
    return high, (x - high.astype(F32)).astype(BF16)


def one_hot(rows, row):
    ordinal = lax.broadcasted_iota(jnp.int32, (rows, row.shape[1]), 0)
    return jnp.where(ordinal == row, 1.0, 0.0)


def emit(vector, pattern, cosines, sines, member, leaf_cos, leaf_sin, halo_ref, column_ref):
    coefs = vector.shape[0] // 2
    boxes, dirs = leaf_cos.shape
    rounded = vector.astype(BF16)
    halo_ref[0, : 2 * coefs, :] = rounded
    by_real = dot(pattern, rounded[:coefs])
    by_imag = dot(pattern, rounded[coefs:])
    real = by_real[:dirs] - by_imag[dirs:]
    imag = by_real[dirs:] + by_imag[:dirs]
    out = jnp.concatenate([real * cosines + imag * sines, imag * cosines - real * sines], axis=0)
    high, low = split(out)
    leaf = dot(member, high, NT) + dot(member, low, NT)
    leaf_real, leaf_imag = leaf[:, :dirs], leaf[:, dirs:]
    halo_ref[0, 2 * coefs : 2 * coefs + boxes, :] = leaf_real.astype(BF16)
    halo_ref[0, 2 * coefs + boxes :, :] = leaf_imag.astype(BF16)
    column_real = jnp.sum(leaf_real * leaf_cos + leaf_imag * leaf_sin, axis=0, keepdims=True)
    column_imag = jnp.sum(leaf_imag * leaf_cos - leaf_real * leaf_sin, axis=0, keepdims=True)
    pair = jnp.concatenate([column_real, column_imag], axis=0)
    column_ref[...] = jnp.broadcast_to(pair[None], column_ref.shape)


def lanes(values):
    lane = lax.broadcasted_iota(jnp.int32, (1, 128), 1)
    row = jnp.zeros((1, 128), F32)
    for place, value in values:
        row = row + jnp.where(lane == place, value, 0.0)
    return row


def inner(a, b):
    return jnp.sum(jnp.sum(a * b, axis=0, keepdims=True), axis=1, keepdims=True)


def first_kernel(
    vector, pattern, offsets, planes, box, leaf_cos, leaf_sin, halo, column, cos_ref, sin_ref, send
):
    turned = jnp.concatenate([pattern[0].T, pattern[1].T], axis=0)
    send[...] = turned
    phases = KAPPA * (
        planes[0] * offsets[0] + planes[1] * offsets[1] + planes[2] * offsets[2]
    )
    cosines, sines = jnp.cos(phases), jnp.sin(phases)
    cos_ref[...] = cosines
    sin_ref[...] = sines
    member = one_hot(leaf_cos.shape[0], box[...]).astype(BF16)
    emit(vector[...], turned, cosines, sines, member, leaf_cos[...], leaf_sin[...], halo, column)


def mirrored(sources, width, flip_x, flip_y):
    line = 3 * width
    flat = jnp.where(sources < line, 0, jnp.where(sources < 2 * line, 1, 2))
    within = sources - line * flat
    side = jnp.where(within < width, 0, jnp.where(within < 2 * width, 1, 2))
    return sources + flip_x * (2 - 2 * flat) * line + flip_y * (2 - 2 * side) * width


def count_kernel(
    index,
    sources,
    targets,
    far_sources,
    kinds,
    transfer,
    mie,
    spread,
    counts,
    select,
    chosen,
    mie_full,
    *,
    across_y,
):
    flips = lax.rem(lax.div(index[0], across_y), 2), lax.rem(index[0], 2)

    @pl.when(pl.program_id(0) == 0)
    def _():
        fill_tables(flips, far_sources, kinds, transfer, mie, spread, select, chosen, mie_full)

    spheres = counts.shape[0] // 9
    chunk = counts.shape[1] // spheres
    for item in range(chunk):
        at = pl.ds(pl.program_id(0) * chunk + item, 1)
        source_hot = one_hot(9 * spheres, mirrored(sources[at, :], spheres, *flips))
        target_hot = one_hot(spheres, targets[at, :])
        counts[:, item * spheres : (item + 1) * spheres] = dot(
            source_hot.astype(BF16), target_hot.astype(BF16), NT
        ).astype(BF16)


def fill_tables(flips, sources, classes, transfer, mie, spread, select, chosen, mie_full):
    boxes, entries = sources.shape
    row = lax.broadcasted_iota(jnp.int32, (boxes, boxes), 0)
    col = lax.broadcasted_iota(jnp.int32, (boxes, boxes), 1)
    unit = jnp.where(row == col, 1.0, 0.0).astype(BF16)
    around = mirrored(sources[...], boxes, *flips)
    around = dot(around.astype(F32).astype(BF16), unit, TN)
    kinds = dot(classes[...].astype(F32).astype(BF16), unit, TN)
    box_lane = lax.broadcasted_iota(jnp.int32, (entries, select.shape[1]), 1).astype(F32)
    kind_lane = lax.broadcasted_iota(jnp.int32, (entries, transfer.shape[0]), 1).astype(F32)
    hots = []
    for item in range(boxes):
        at = slice(item * entries, (item + 1) * entries)
        hots.append(jnp.where(kinds[:, item : item + 1] == kind_lane, 1.0, 0.0))
        select[at, :] = jnp.where(around[:, item : item + 1] == box_lane, 1.0, 0.0).astype(BF16)
    hot = jnp.concatenate(hots, axis=0)
    dirs = transfer.shape[2]
    chosen[:, :dirs] = dot(hot, transfer[:, 0, :], precision=HIGHEST)
    chosen[:, dirs:] = dot(hot, transfer[:, 1, :], precision=HIGHEST)
    mie_full[...] = dot(spread[...], mie[...], precision=HIGHEST)


def window_kernel(index, transfer, window, *, near_z, near_x, groups, run, top_x, top_y):
    row, col = lax.div(index[0], near_x * run), lax.rem(index[0], near_x * run)
    high, depth = lax.div(row, near_z), lax.rem(row, near_z)
    across, lane = lax.div(col, run), lax.rem(col, run)
    ordinal = lax.broadcasted_iota(jnp.int32, (run, 128), 0)
    for z in range(near_z):
        for x in range(near_x):
            start = (across - x) * run - lane + top_y
            apart_y = jnp.abs(ordinal + (start - top_y))
            for group in range(groups):
                shift = (group - high) * near_z + depth - z
                keep = (apart_y >= 2) | (jnp.abs(shift) >= 2)
                for part in range(2):
                    rows = transfer[shift + top_x, pl.ds(start, run), part, :]
                    window[part, z * near_x + x, group * run : (group + 1) * run, :] = jnp.where(
                        keep, rows, 0.0
                    )


def coarse_kernel(columns, window, partial):
    real, imag = columns[:, 0, :][None], columns[:, 1, :][None]
    partial[:, 0, :] = jnp.sum(real * window[0] - imag * window[1], axis=1)
    partial[:, 1, :] = jnp.sum(imag * window[0] + real * window[1], axis=1)


def near_kernel(before, own, after, counts, table, select, chosen, near, leaf_in, columns):
    coefs = near.shape[0] // 2
    classes = table.shape[0]
    spheres = near.shape[1] // 2
    boxes, dirs = leaf_in.shape[0], leaf_in.shape[1] // 2

    @pl.when(pl.program_id(0) == 0)
    def _():
        leaves = []
        for row in range(3):
            for col, part in enumerate((before, own, after)):
                place = (row * 3 + col) * spheres
                columns[:, place : place + spheres] = part[row, : 2 * coefs, :]
                leaves.append(part[row, 2 * coefs :, :])
        around = jnp.concatenate(
            [
                jnp.concatenate([leaf[:boxes] for leaf in leaves], axis=0),
                jnp.concatenate([leaf[boxes:] for leaf in leaves], axis=0),
            ],
            axis=1,
        )
        picked = dot(select[...], around)
        pick_real, pick_imag = picked[:, :dirs], picked[:, dirs:]
        move_real, move_imag = chosen[:, :dirs], chosen[:, dirs:]
        got_real = pick_real * move_real - pick_imag * move_imag
        got_imag = pick_imag * move_real + pick_real * move_imag
        leaf_in[:, :dirs] = jnp.sum(got_real.reshape(boxes, -1, dirs), axis=1)
        leaf_in[:, dirs:] = jnp.sum(got_imag.reshape(boxes, -1, dirs), axis=1)
        near[...] = jnp.zeros(near.shape, F32)

    gathered = dot(columns[...], counts[...]).astype(BF16)
    total = near[...]
    for item in range(classes):
        at = slice(item * spheres, (item + 1) * spheres)
        pair = jnp.concatenate([gathered[:coefs, at], gathered[coefs:, at]], axis=1)
        total = total + dot(table[item], pair)
    near[...] = total


def arrive(partial, near, leaf_in, receive, cosines, sines, member, leaf_cos, leaf_sin, mie_full):
    _, dirs = leaf_cos.shape
    coefs = near.shape[0] // 2
    column_real = jnp.sum(partial[:, 0, :], axis=0, keepdims=True)
    column_imag = jnp.sum(partial[:, 1, :], axis=0, keepdims=True)
    incoming = leaf_in + jnp.concatenate(
        [
            column_real * leaf_cos - column_imag * leaf_sin,
            column_real * leaf_sin + column_imag * leaf_cos,
        ],
        axis=1,
    )
    high, low = split(incoming)
    spread = dot(high, member, TN) + dot(low, member, TN)
    real, imag = spread[:dirs], spread[dirs:]
    arriving = jnp.concatenate(
        [real * cosines - imag * sines, real * sines + imag * cosines], axis=1
    ).astype(BF16)
    total = near + dot(receive, arriving)
    half = total.shape[1] // 2
    field_real = total[:coefs, :half] - total[coefs:, half:]
    field_imag = total[coefs:, :half] + total[:coefs, half:]
    mie_real, mie_imag = mie_full[:coefs], mie_full[coefs:]
    return jnp.concatenate(
        [
            field_real * mie_real - field_imag * mie_imag,
            field_real * mie_imag + field_imag * mie_real,
        ],
        axis=0,
    )


def sums_kernel(vector, scattered, sums):
    u, d = vector[...], scattered[...]
    sums[...] = lanes([(0, inner(u, u)), (1, inner(u, d)), (2, inner(d, d))])


def middle_kernel(
    partial,
    near,
    leaf_in,
    pattern,
    receive,
    cosines,
    sines,
    box,
    leaf_cos,
    leaf_sin,
    mie_full,
    applied,
    halo,
    column,
):
    member = one_hot(leaf_cos.shape[0], box[...]).astype(BF16)
    scattered = arrive(
        partial[...],
        near[...],
        leaf_in[...],
        receive[...],
        cosines[...],
        sines[...],
        member,
        leaf_cos[...],
        leaf_sin[...],
        mie_full[...],
    )
    applied[...] = scattered
    emit(
        scattered,
        pattern[...],
        cosines[...],
        sines[...],
        member,
        leaf_cos[...],
        leaf_sin[...],
        halo,
        column,
    )


def last_kernel(
    vector,
    scattered,
    partial,
    near,
    leaf_in,
    receive,
    cosines,
    sines,
    box,
    leaf_cos,
    leaf_sin,
    mie_full,
    sums,
    applied,
    everyone,
):
    member = one_hot(leaf_cos.shape[0], box[...]).astype(BF16)
    twice = arrive(
        partial[...],
        near[...],
        leaf_in[...],
        receive[...],
        cosines[...],
        sines[...],
        member,
        leaf_cos[...],
        leaf_sin[...],
        mie_full[...],
    )
    applied[...] = twice
    row = sums[...] + lanes(
        [(3, inner(vector[...], twice)), (4, inner(scattered[...], twice)), (5, inner(twice, twice))]
    )
    everyone[...] = jnp.broadcast_to(row[None], everyone.shape)


def relay_kernel(parts, everyone):
    everyone[...] = jnp.broadcast_to(jnp.sum(parts[...], axis=0, keepdims=True), everyone.shape)


def solve_kernel(parts, vector, scattered, twice, solution, residual):
    row = jnp.sum(parts[...], axis=0)
    lane = lax.broadcasted_iota(jnp.int32, row.shape, 1)

    def total(place):
        value = jnp.sum(jnp.where(lane == place, row, 0.0), axis=1, keepdims=True)
        return jnp.broadcast_to(value, (8, 128))

    uu, ud, dd, ue, de, ee = (total(place) for place in range(6))
    beta = jnp.sqrt(uu)
    along = ud / uu
    across = dd - along * ud
    size = jnp.sqrt(across)
    h00 = 1.0 - along
    h10 = size / beta
    turned = de - along * ue
    h01 = (ue - along * ud) / (size * beta)
    h11 = 1.0 + along - turned / across
    rest_u = ue / uu
    rest_d = turned / across
    left = ee - rest_u * ue - rest_d * turned
    h21 = jnp.sqrt(left) / size
    n00 = h00 * h00 + h10 * h10
    n01 = h00 * h01 + h10 * h11
    n11 = h01 * h01 + h11 * h11 + h21 * h21
    l00 = jnp.sqrt(n00)
    l10 = n01 / l00
    l11 = jnp.sqrt(n11 - l10 * l10)
    m0 = beta * h00 / l00
    m1 = (beta * h01 - l10 * m0) / l11
    y1 = m1 / l11
    y0 = (m0 - l10 * y1) / l00
    z0 = h00 * y0 + h01 * y1
    z1 = h10 * y0 + h11 * y1
    step = y1 / size
    sol_u = y0 / beta + step * along
    sol_d = -step
    res_u = (beta - z0) / beta - z1 / size * along + step * (rest_u - rest_d * along)
    res_d = z1 / size + step * rest_d
    res_e = -step
    u, d, e = vector[...], scattered[...], twice[...]
    solution[...] = sol_u[0:1] * u + sol_d[0:1] * d
    residual[...] = res_u[0:1] * u + res_d[0:1] * d + res_e[0:1] * e


def swap(x, axes, first):
    pairs = [(i, i + 1) for i in range(first, lax.axis_size(axes) - 1, 2)]
    return lax.ppermute(x, axes, pairs + [(j, i) for i, j in pairs])


def exchange(x, axes):
    return lax.all_to_all(x, axes, split_axis=0, concat_axis=0, tiled=True)


def local(
    incident,
    mie,
    offsets,
    sphere_box,
    near_table,
    near_src,
    near_dst,
    pattern,
    receive,
    leaf_transfer,
    far_src,
    far_cls,
    coarse_transfer,
):
    coefs = incident.shape[1]
    spheres = incident.shape[4]
    rows = 2 * coefs
    dirs = pattern.shape[1]
    boxes, entries = far_src.shape[2:]
    classes, pairs = near_src.shape[2:]
    high_count, near_z = lax.axis_size("bx_0"), lax.axis_size("bx_1")
    near_x = lax.axis_size("by_0")
    run = lax.axis_size(("by_1", "by_2"))
    first_count, second_count = lax.axis_size(FIRST), lax.axis_size(SECOND)
    index = lax.axis_index(BX + BY).astype(jnp.int32).reshape(1)

    planes = jnp.asarray(directions(dirs)[:, :, None].astype(np.float32))
    centre = KAPPA * (leaf_centers(boxes).T @ directions(dirs))
    leaf_cos = jnp.asarray(np.cos(centre).astype(np.float32))
    leaf_sin = jnp.asarray(np.sin(centre).astype(np.float32))

    vector = incident.reshape(rows, spheres)
    box = sphere_box.reshape(1, spheres)
    pattern = pattern.transpose(0, 2, 1)
    receive = receive.reshape(rows, dirs)

    halo_shape = kept((1, rows + 2 * boxes, spheres), BF16)
    column_shape = kept((first_count, 2, dirs))
    halo, column, cosines, sines, send = call(
        first_kernel,
        (
            halo_shape,
            column_shape,
            kept((dirs, spheres)),
            kept((dirs, spheres)),
            kept((2 * dirs, coefs), BF16),
        ),
        (vector, pattern, offsets.reshape(3, 1, spheres), planes, box, leaf_cos, leaf_sin),
        flops=1 << 26,
    )
    chunk = classes // 2
    whole = pl.BlockSpec(memory_space=pltpu.VMEM)

    def prepare():
        spread = mie_spread(coefs, mie.shape[1])
        zero = np.zeros_like(spread)
        spread = jnp.asarray(np.block([[spread, zero], [zero, spread]]))
        return call(
            functools.partial(count_kernel, across_y=near_x * run),
            (
                shape((9 * spheres, classes * spheres), BF16),
                kept((boxes * entries, 9 * boxes), BF16),
                kept((boxes * entries, 2 * dirs)),
                kept((rows, spheres)),
            ),
            (
                index,
                near_src.reshape(classes, pairs),
                near_dst.reshape(classes, pairs),
                far_src.reshape(boxes, entries),
                far_cls.reshape(boxes, entries),
                leaf_transfer,
                mie.reshape(2 * mie.shape[1], spheres),
                spread,
            ),
            flops=1 << 31,
            grid=(classes // chunk,),
            in_specs=[pl.BlockSpec(memory_space=pltpu.SMEM)] + [whole] * 7,
            out_specs=(
                pl.BlockSpec((9 * spheres, chunk * spheres), lambda k: (0, k)),
                whole,
                whole,
                whole,
            ),
        )

    def windows():
        return call(
            functools.partial(
                window_kernel,
                near_z=near_z,
                near_x=near_x,
                groups=high_count,
                run=run,
                top_x=high_count * near_z - 1,
                top_y=near_x * run - 1,
            ),
            kept((2, second_count, first_count, dirs)),
            (index, coarse_transfer.transpose(1, 2, 0, 3)),
            flops=1 << 28,
        )

    def apply(halo, column, window, counts, select, chosen):
        columns = exchange(column, FIRST)
        ahead = swap(halo, BX, 0)
        behind = swap(halo, BX, 1)
        line = jnp.concatenate([behind, halo, ahead], axis=0)
        right = swap(line, BY, 0)
        left = swap(line, BY, 1)
        partial = call(
            coarse_kernel,
            kept((second_count, 2, dirs)),
            (resident(columns), resident(window)),
            1 << 24,
        )
        partial = exchange(partial, SECOND)
        near, leaf_in = call(
            near_kernel,
            (kept((rows, 2 * spheres)), kept((boxes, 2 * dirs))),
            (
                resident(left),
                resident(line),
                resident(right),
                counts,
                near_table.reshape(classes, rows, coefs),
                resident(select),
                resident(chosen),
            ),
            flops=1 << 31,
            grid=(classes // chunk,),
            in_specs=[
                whole,
                whole,
                whole,
                pl.BlockSpec((9 * spheres, chunk * spheres), lambda k: (0, k)),
                pl.BlockSpec((chunk, rows, coefs), lambda k: (k, 0, 0)),
                whole,
                whole,
            ],
            out_specs=(whole, whole),
            scratch_shapes=[pltpu.VMEM((rows, 9 * spheres), BF16)],
        )
        return resident(partial), resident(near), resident(leaf_in)

    window = windows()
    counts, select, chosen, mie_full = prepare()
    partial, near, leaf_in = apply(halo, column, window, counts, select, chosen)
    far = tuple(
        resident(item) for item in (receive, cosines, sines, box, leaf_cos, leaf_sin, mie_full)
    )
    vector = resident(vector)
    once, halo, column = call(
        middle_kernel,
        (kept((rows, spheres)), halo_shape, column_shape),
        (partial, near, leaf_in, resident(send)) + far,
        flops=1 << 26,
    )
    sums = call(sums_kernel, kept((1, 128)), (vector, resident(once)), 1 << 24)
    partial, near, leaf_in = apply(halo, column, window, counts, select, chosen)
    once = resident(once)
    twice, everyone = call(
        last_kernel,
        (kept((rows, spheres)), kept((first_count, 1, 128))),
        (vector, once, partial, near, leaf_in) + far + (resident(sums),),
        flops=1 << 26,
    )
    everyone = call(
        relay_kernel, kept((second_count, 1, 128)), (resident(exchange(everyone, FIRST)),), 1 << 20
    )
    solved, residual = call(
        solve_kernel,
        (shape((rows, spheres)), shape((rows, spheres))),
        (resident(exchange(everyone, SECOND)), vector, once, resident(twice)),
        flops=1 << 24,
    )
    return solved.reshape(incident.shape), residual.reshape(incident.shape)


def build(devices, sizes):
    torus = Mesh(devices.reshape(sizes), BX + BY)
    placed = (
        P(None, None, BX, BY, None),
        P(None, None, BX, BY, None),
        P(None, BX, BY, None),
        P(BX, BY, None),
        P(),
        P(BX, BY, None, None),
        P(BX, BY, None, None),
        P(),
        P(),
        P(),
        P(BX, BY, None, None),
        P(BX, BY, None, None),
        P(),
    )
    return jax.shard_map(
        local,
        mesh=torus,
        in_specs=placed,
        out_specs=(P(None, None, BX, BY, None), P(None, None, BX, BY, None)),
        check_vma=False,
    )


def solution(mesh):
    return build(mesh.devices, (2, 8, 4, 4, 2))
```

```python
import functools
import math

import jax
import jax.numpy as jnp
import numpy as np
from jax import lax
from jax.experimental import pallas as pl
from jax.experimental.pallas import tpu as pltpu
from jax.sharding import Mesh
from jax.sharding import PartitionSpec as P

BX = ("bx_0", "bx_1")
BY = ("by_0", "by_1", "by_2")
FIRST = ("bx_0", "by_1", "by_2")
SECOND = ("bx_1", "by_0")

HIGHEST = lax.Precision.HIGHEST
KAPPA = 1.5
GOLDEN = 2.399963229728653
F32 = jnp.float32
BF16 = jnp.bfloat16
NT = (((1,), (1,)), ((), ()))
TN = (((0,), (0,)), ((), ()))
INTERPRET = False


def call(kernel, out_shape, operands, flops=0, **kw):
    if "specs" in kw:
        kw["in_specs"] = kw.pop("specs")
    elif "grid" not in kw:
        kw["in_specs"] = [
            pl.BlockSpec(memory_space=pltpu.SMEM if op.ndim == 1 else pltpu.VMEM)
            for op in operands
        ]
    return pl.pallas_call(
        kernel,
        out_shape=out_shape,
        interpret=INTERPRET,
        cost_estimate=pl.CostEstimate(flops=flops, transcendentals=0, bytes_accessed=1 << 20),
        **kw,
    )(*operands)


def resident(x):
    return x if INTERPRET else pltpu.with_memory_space_constraint(x, pltpu.VMEM)


def kept(dims, dtype=F32):
    return shape(dims, dtype) if INTERPRET else pltpu.VMEM(dims, dtype)


def shape(dims, dtype=F32):
    return jax.ShapeDtypeStruct(dims, dtype)


def directions(number):
    ordinal = np.arange(number, dtype=np.float64)
    height = 1.0 - (2.0 * ordinal + 1.0) / number
    radius = np.sqrt(1.0 - height * height)
    return np.stack([radius * np.cos(GOLDEN * ordinal), radius * np.sin(GOLDEN * ordinal), height])


def leaf_centers(number):
    ordinal = np.arange(number)
    return np.stack(
        [
            2.0 * (ordinal % 2) - 1.0,
            2.0 * (ordinal // 2 % 2) - 1.0,
            2.0 * (ordinal // 4) - (number // 4 - 1),
        ]
    )


def mie_spread(coef_count, mie_count):
    half_count = coef_count // 2
    table = np.zeros((coef_count, mie_count), np.float32)
    for number in range(coef_count):
        degree = math.isqrt(number % half_count + 1)
        table[number, number // half_count * (mie_count // 2) + degree - 1] = 1.0
    return table


def dot(a, b, dims=(((1,), (0,)), ((), ())), precision=None):
    return lax.dot_general(a, b, dims, precision=precision, preferred_element_type=F32)


def split(x):
    high = x.astype(BF16)
    return high, (x - high.astype(F32)).astype(BF16)


def one_hot(rows, row):
    ordinal = lax.broadcasted_iota(jnp.int32, (rows, row.shape[1]), 0)
    return jnp.where(ordinal == row, 1.0, 0.0)


def emit(vector, pattern, cosines, sines, member, leaf_cos, leaf_sin, halo_ref, column_ref):
    coefs = vector.shape[0] // 2
    boxes, dirs = leaf_cos.shape
    rounded = vector.astype(BF16)
    halo_ref[0, : 2 * coefs, :] = rounded
    by_real = dot(pattern, rounded[:coefs])
    by_imag = dot(pattern, rounded[coefs:])
    real = by_real[:dirs] - by_imag[dirs:]
    imag = by_real[dirs:] + by_imag[:dirs]
    out = jnp.concatenate([real * cosines + imag * sines, imag * cosines - real * sines], axis=0)
    high, low = split(out)
    leaf = dot(member, high, NT) + dot(member, low, NT)
    leaf_real, leaf_imag = leaf[:, :dirs], leaf[:, dirs:]
    halo_ref[0, 2 * coefs : 2 * coefs + boxes, :] = leaf_real.astype(BF16)
    halo_ref[0, 2 * coefs + boxes :, :] = leaf_imag.astype(BF16)
    column_real = jnp.sum(leaf_real * leaf_cos + leaf_imag * leaf_sin, axis=0, keepdims=True)
    column_imag = jnp.sum(leaf_imag * leaf_cos - leaf_real * leaf_sin, axis=0, keepdims=True)
    pair = jnp.concatenate([column_real, column_imag], axis=0)
    column_ref[...] = jnp.broadcast_to(pair[None], column_ref.shape)


def lanes(values):
    lane = lax.broadcasted_iota(jnp.int32, (1, 128), 1)
    row = jnp.zeros((1, 128), F32)
    for place, value in values:
        row = row + jnp.where(lane == place, value, 0.0)
    return row


def inner(a, b):
    return jnp.sum(jnp.sum(a * b, axis=0, keepdims=True), axis=1, keepdims=True)


def first_kernel(
    vector, pattern, offsets, planes, box, leaf_cos, leaf_sin, halo, column, cos_ref, sin_ref, send
):
    turned = jnp.concatenate([pattern[0].T, pattern[1].T], axis=0)
    send[...] = turned
    phases = KAPPA * (
        planes[0] * offsets[0] + planes[1] * offsets[1] + planes[2] * offsets[2]
    )
    cosines, sines = jnp.cos(phases), jnp.sin(phases)
    cos_ref[...] = cosines
    sin_ref[...] = sines
    member = one_hot(leaf_cos.shape[0], box[...]).astype(BF16)
    emit(vector[...], turned, cosines, sines, member, leaf_cos[...], leaf_sin[...], halo, column)


def mirrored(sources, width, flip_x, flip_y):
    line = 3 * width
    flat = jnp.where(sources < line, 0, jnp.where(sources < 2 * line, 1, 2))
    within = sources - line * flat
    side = jnp.where(within < width, 0, jnp.where(within < 2 * width, 1, 2))
    return sources + flip_x * (2 - 2 * flat) * line + flip_y * (2 - 2 * side) * width


def fill_tables(sources, classes, transfer, mie, spread, select, chosen, mie_full):
    boxes, entries = sources.shape
    row = lax.broadcasted_iota(jnp.int32, (boxes, boxes), 0)
    col = lax.broadcasted_iota(jnp.int32, (boxes, boxes), 1)
    unit = jnp.where(row == col, 1.0, 0.0).astype(BF16)
    around = dot(sources[...].astype(F32).astype(BF16), unit, TN)
    kinds = dot(classes[...].astype(F32).astype(BF16), unit, TN)
    box_lane = lax.broadcasted_iota(jnp.int32, (entries, select.shape[1]), 1).astype(F32)
    kind_lane = lax.broadcasted_iota(jnp.int32, (entries, transfer.shape[0]), 1).astype(F32)
    hots = []
    for item in range(boxes):
        at = slice(item * entries, (item + 1) * entries)
        hots.append(jnp.where(kinds[:, item : item + 1] == kind_lane, 1.0, 0.0))
        select[at, :] = jnp.where(around[:, item : item + 1] == box_lane, 1.0, 0.0).astype(BF16)
    hot = jnp.concatenate(hots, axis=0)
    dirs = transfer.shape[2]
    chosen[:, :dirs] = dot(hot, transfer[:, 0, :], precision=HIGHEST)
    chosen[:, dirs:] = dot(hot, transfer[:, 1, :], precision=HIGHEST)
    mie_full[...] = dot(spread[...], mie[...], precision=HIGHEST)


def window_kernel(
    index,
    transfer,
    near_sources,
    far_sources,
    *rest,
    spheres,
    boxes,
    near_z,
    near_x,
    groups,
    run,
    top_x,
    top_y,
):
    copied = len(rest) // 2 - 1
    window, near_out, far_out = rest[copied : copied + 3]
    row, col = lax.div(index[0], near_x * run), lax.rem(index[0], near_x * run)
    flips = lax.rem(row, 2), lax.rem(col, 2)
    near_out[...] = mirrored(near_sources[...], spheres, *flips)
    far_out[...] = mirrored(far_sources[...], boxes, *flips)
    for source, target in zip(rest[:copied], rest[copied + 3 :]):
        target[...] = source[...]
    high, depth = lax.div(row, near_z), lax.rem(row, near_z)
    across, lane = lax.div(col, run), lax.rem(col, run)
    ordinal = lax.broadcasted_iota(jnp.int32, (run, 128), 0)
    for z in range(near_z):
        for x in range(near_x):
            start = (across - x) * run - lane + top_y
            apart_y = jnp.abs(ordinal + (start - top_y))
            for group in range(groups):
                shift = (group - high) * near_z + depth - z
                keep = (apart_y >= 2) | (jnp.abs(shift) >= 2)
                for part in range(2):
                    rows = transfer[shift + top_x, pl.ds(start, run), part, :]
                    window[part, z * near_x + x, group * run : (group + 1) * run, :] = jnp.where(
                        keep, rows, 0.0
                    )


def coarse_kernel(columns, window, partial):
    real, imag = columns[:, 0, :][None], columns[:, 1, :][None]
    partial[:, 0, :] = jnp.sum(real * window[0] - imag * window[1], axis=1)
    partial[:, 1, :] = jnp.sum(imag * window[0] + real * window[1], axis=1)


def near_start(before, own, after, select, chosen, near, leaf_in, columns):
    coefs = near.shape[0] // 2
    spheres = near.shape[1] // 2
    boxes, dirs = leaf_in.shape[0], leaf_in.shape[1] // 2
    leaves = []
    for row in range(3):
        for col, part in enumerate((before, own, after)):
            place = (row * 3 + col) * spheres
            columns[:, place : place + spheres] = part[row, : 2 * coefs, :]
            leaves.append(part[row, 2 * coefs :, :])
    around = jnp.concatenate(
        [
            jnp.concatenate([leaf[:boxes] for leaf in leaves], axis=0),
            jnp.concatenate([leaf[boxes:] for leaf in leaves], axis=0),
        ],
        axis=1,
    )
    picked = dot(select[...], around)
    pick_real, pick_imag = picked[:, :dirs], picked[:, dirs:]
    move_real, move_imag = chosen[:, :dirs], chosen[:, dirs:]
    got_real = pick_real * move_real - pick_imag * move_imag
    got_imag = pick_imag * move_real + pick_real * move_imag
    leaf_in[:, :dirs] = jnp.sum(got_real.reshape(boxes, -1, dirs), axis=1)
    leaf_in[:, dirs:] = jnp.sum(got_imag.reshape(boxes, -1, dirs), axis=1)
    near[...] = jnp.zeros(near.shape, F32)


def near_step(columns, counts, table, near):
    coefs = near.shape[0] // 2
    spheres = near.shape[1] // 2
    gathered = dot(columns[...], counts).astype(BF16)
    total = near[...]
    for item in range(table.shape[0]):
        at = slice(item * spheres, (item + 1) * spheres)
        pair = jnp.concatenate([gathered[:coefs, at], gathered[coefs:, at]], axis=1)
        total = total + dot(table[item], pair)
    near[...] = total


def near_kernel(before, own, after, counts, table, select, chosen, near, leaf_in, columns):
    @pl.when(pl.program_id(0) == 0)
    def _():
        near_start(before, own, after, select, chosen, near, leaf_in, columns)

    near_step(columns, counts[...], table, near)


def both_kernel(
    sources,
    far_sources,
    targets,
    kinds,
    transfer,
    mie,
    spread,
    before,
    own,
    after,
    table_hbm,
    near,
    leaf_in,
    counts_hbm,
    select,
    chosen,
    mie_full,
    columns,
    block,
    table,
    sems,
):
    groups, long, wide = block.shape
    spheres = long // 9
    chunk = wide // spheres
    loading = pltpu.make_async_copy(table_hbm, table, sems.at[groups])
    loading.start()
    storing = []
    for group in range(groups):
        for item in range(chunk):
            at = slice(group * chunk + item, group * chunk + item + 1)
            source_hot = one_hot(long, sources[at, :]).astype(BF16)
            target_hot = one_hot(spheres, targets[at, :]).astype(BF16)
            block[group, :, item * spheres : (item + 1) * spheres] = dot(
                source_hot, target_hot, NT
            ).astype(BF16)
        keep = pltpu.make_async_copy(
            block.at[group], counts_hbm.at[:, pl.ds(group * wide, wide)], sems.at[group]
        )
        keep.start()
        storing.append(keep)
        if group == 0:
            fill_tables(far_sources, kinds, transfer, mie, spread, select, chosen, mie_full)
            near_start(before, own, after, select, chosen, near, leaf_in, columns)
            loading.wait()
        near_step(
            columns, block[group], table.at[pl.ds(group * chunk, chunk)], near
        )
    for keep in storing:
        keep.wait()


def arrive(partial, near, leaf_in, receive, cosines, sines, member, leaf_cos, leaf_sin, mie_full):
    _, dirs = leaf_cos.shape
    coefs = near.shape[0] // 2
    column_real = jnp.sum(partial[:, 0, :], axis=0, keepdims=True)
    column_imag = jnp.sum(partial[:, 1, :], axis=0, keepdims=True)
    incoming = leaf_in + jnp.concatenate(
        [
            column_real * leaf_cos - column_imag * leaf_sin,
            column_real * leaf_sin + column_imag * leaf_cos,
        ],
        axis=1,
    )
    high, low = split(incoming)
    spread = dot(high, member, TN) + dot(low, member, TN)
    real, imag = spread[:dirs], spread[dirs:]
    arriving = jnp.concatenate(
        [real * cosines - imag * sines, real * sines + imag * cosines], axis=1
    ).astype(BF16)
    total = near + dot(receive, arriving)
    half = total.shape[1] // 2
    field_real = total[:coefs, :half] - total[coefs:, half:]
    field_imag = total[coefs:, :half] + total[:coefs, half:]
    mie_real, mie_imag = mie_full[:coefs], mie_full[coefs:]
    return jnp.concatenate(
        [
            field_real * mie_real - field_imag * mie_imag,
            field_real * mie_imag + field_imag * mie_real,
        ],
        axis=0,
    )


def sums_kernel(vector, scattered, sums):
    u, d = vector[...], scattered[...]
    sums[...] = lanes([(0, inner(u, u)), (1, inner(u, d)), (2, inner(d, d))])


def middle_kernel(
    partial,
    near,
    leaf_in,
    pattern,
    receive,
    cosines,
    sines,
    box,
    leaf_cos,
    leaf_sin,
    mie_full,
    applied,
    halo,
    column,
):
    member = one_hot(leaf_cos.shape[0], box[...]).astype(BF16)
    scattered = arrive(
        partial[...],
        near[...],
        leaf_in[...],
        receive[...],
        cosines[...],
        sines[...],
        member,
        leaf_cos[...],
        leaf_sin[...],
        mie_full[...],
    )
    applied[...] = scattered
    emit(
        scattered,
        pattern[...],
        cosines[...],
        sines[...],
        member,
        leaf_cos[...],
        leaf_sin[...],
        halo,
        column,
    )


def last_kernel(
    vector,
    scattered,
    partial,
    near,
    leaf_in,
    receive,
    cosines,
    sines,
    box,
    leaf_cos,
    leaf_sin,
    mie_full,
    sums,
    applied,
    everyone,
):
    member = one_hot(leaf_cos.shape[0], box[...]).astype(BF16)
    twice = arrive(
        partial[...],
        near[...],
        leaf_in[...],
        receive[...],
        cosines[...],
        sines[...],
        member,
        leaf_cos[...],
        leaf_sin[...],
        mie_full[...],
    )
    applied[...] = twice
    row = sums[...] + lanes(
        [(3, inner(vector[...], twice)), (4, inner(scattered[...], twice)), (5, inner(twice, twice))]
    )
    everyone[...] = jnp.broadcast_to(row[None], everyone.shape)


def relay_kernel(parts, everyone):
    everyone[...] = jnp.broadcast_to(jnp.sum(parts[...], axis=0, keepdims=True), everyone.shape)


def solve_kernel(parts, vector, scattered, twice, solution, residual):
    row = jnp.sum(parts[...], axis=0)
    lane = lax.broadcasted_iota(jnp.int32, row.shape, 1)

    def total(place):
        value = jnp.sum(jnp.where(lane == place, row, 0.0), axis=1, keepdims=True)
        return jnp.broadcast_to(value, (8, 128))

    uu, ud, dd, ue, de, ee = (total(place) for place in range(6))
    beta = jnp.sqrt(uu)
    along = ud / uu
    across = dd - along * ud
    size = jnp.sqrt(across)
    h00 = 1.0 - along
    h10 = size / beta
    turned = de - along * ue
    h01 = (ue - along * ud) / (size * beta)
    h11 = 1.0 + along - turned / across
    rest_u = ue / uu
    rest_d = turned / across
    left = ee - rest_u * ue - rest_d * turned
    h21 = jnp.sqrt(left) / size
    n00 = h00 * h00 + h10 * h10
    n01 = h00 * h01 + h10 * h11
    n11 = h01 * h01 + h11 * h11 + h21 * h21
    l00 = jnp.sqrt(n00)
    l10 = n01 / l00
    l11 = jnp.sqrt(n11 - l10 * l10)
    m0 = beta * h00 / l00
    m1 = (beta * h01 - l10 * m0) / l11
    y1 = m1 / l11
    y0 = (m0 - l10 * y1) / l00
    z0 = h00 * y0 + h01 * y1
    z1 = h10 * y0 + h11 * y1
    step = y1 / size
    sol_u = y0 / beta + step * along
    sol_d = -step
    res_u = (beta - z0) / beta - z1 / size * along + step * (rest_u - rest_d * along)
    res_d = z1 / size + step * rest_d
    res_e = -step
    u, d, e = vector[...], scattered[...], twice[...]
    solution[...] = sol_u[0:1] * u + sol_d[0:1] * d
    residual[...] = res_u[0:1] * u + res_d[0:1] * d + res_e[0:1] * e


def swap(x, axes, first):
    pairs = [(i, i + 1) for i in range(first, lax.axis_size(axes) - 1, 2)]
    return lax.ppermute(x, axes, pairs + [(j, i) for i, j in pairs])


def exchange(x, axes):
    return lax.all_to_all(x, axes, split_axis=0, concat_axis=0, tiled=True)


def local(
    incident,
    mie,
    offsets,
    sphere_box,
    near_table,
    near_src,
    near_dst,
    pattern,
    receive,
    leaf_transfer,
    far_src,
    far_cls,
    coarse_transfer,
):
    coefs = incident.shape[1]
    spheres = incident.shape[4]
    rows = 2 * coefs
    dirs = pattern.shape[1]
    boxes, entries = far_src.shape[2:]
    classes, pairs = near_src.shape[2:]
    high_count, near_z = lax.axis_size("bx_0"), lax.axis_size("bx_1")
    near_x = lax.axis_size("by_0")
    run = lax.axis_size(("by_1", "by_2"))
    first_count, second_count = lax.axis_size(FIRST), lax.axis_size(SECOND)
    index = lax.axis_index(BX + BY).astype(jnp.int32).reshape(1)

    planes = jnp.asarray(directions(dirs)[:, :, None].astype(np.float32))
    centre = KAPPA * (leaf_centers(boxes).T @ directions(dirs))
    leaf_cos = jnp.asarray(np.cos(centre).astype(np.float32))
    leaf_sin = jnp.asarray(np.sin(centre).astype(np.float32))

    vector = incident.reshape(rows, spheres)
    box = sphere_box.reshape(1, spheres)
    pattern = pattern.transpose(0, 2, 1)
    receive = receive.reshape(rows, dirs)

    halo_shape = kept((1, rows + 2 * boxes, spheres), BF16)
    column_shape = kept((first_count, 2, dirs))
    halo, column, cosines, sines, send = call(
        first_kernel,
        (
            halo_shape,
            column_shape,
            kept((dirs, spheres)),
            kept((dirs, spheres)),
            kept((2 * dirs, coefs), BF16),
        ),
        (vector, pattern, offsets.reshape(3, 1, spheres), planes, box, leaf_cos, leaf_sin),
        flops=1 << 26,
    )
    chunk = classes // 2
    whole = pl.BlockSpec(memory_space=pltpu.VMEM)

    def windows():
        spread = mie_spread(coefs, mie.shape[1])
        zero = np.zeros_like(spread)
        copied = (
            near_dst.reshape(classes, pairs),
            far_cls.reshape(boxes, entries),
            leaf_transfer,
            mie.reshape(2 * mie.shape[1], spheres),
            jnp.asarray(np.block([[spread, zero], [zero, spread]])),
        )
        return call(
            functools.partial(
                window_kernel,
                spheres=spheres,
                boxes=boxes,
                near_z=near_z,
                near_x=near_x,
                groups=high_count,
                run=run,
                top_x=high_count * near_z - 1,
                top_y=near_x * run - 1,
            ),
            (
                kept((2, second_count, first_count, dirs)),
                kept((classes, pairs), jnp.int32),
                kept((boxes, entries), jnp.int32),
            )
            + tuple(kept(item.shape, item.dtype) for item in copied),
            (
                index,
                coarse_transfer.transpose(1, 2, 0, 3),
                near_src.reshape(classes, pairs),
                far_src.reshape(boxes, entries),
            )
            + copied,
            flops=1 << 28,
        )

    def apply(halo, column, window, prepared, tables=None):
        columns = exchange(column, FIRST)
        ahead = swap(halo, BX, 0)
        behind = swap(halo, BX, 1)
        line = jnp.concatenate([behind, halo, ahead], axis=0)
        right = swap(line, BY, 0)
        left = swap(line, BY, 1)
        partial = call(
            coarse_kernel,
            kept((second_count, 2, dirs)),
            (resident(columns), resident(window)),
            1 << 24,
        )
        partial = exchange(partial, SECOND)
        lines = resident(left), resident(line), resident(right)
        table = near_table.reshape(classes, rows, coefs)
        sums = (kept((rows, 2 * spheres)), kept((boxes, 2 * dirs)))
        if tables is None:
            groups = classes // 4
            any_spec = pl.BlockSpec(memory_space=pl.ANY)
            near, leaf_in, *tables = call(
                both_kernel,
                sums
                + (
                    shape((9 * spheres, classes * spheres), BF16),
                    kept((boxes * entries, 9 * boxes), BF16),
                    kept((boxes * entries, 2 * dirs)),
                    kept((rows, spheres)),
                ),
                tuple(resident(item) for item in prepared) + lines + (table,),
                flops=1 << 31,
                specs=[whole] * 10 + [any_spec],
                out_specs=(whole, whole, any_spec, whole, whole, whole),
                scratch_shapes=[
                    pltpu.VMEM((rows, 9 * spheres), BF16),
                    pltpu.VMEM((groups, 9 * spheres, 4 * spheres), BF16),
                    pltpu.VMEM((classes, rows, coefs), BF16),
                    pltpu.SemaphoreType.DMA((groups + 1,)),
                ],
            )
        else:
            counts, select, chosen, _ = tables
            near, leaf_in = call(
                near_kernel,
                sums,
                lines + (counts, table, resident(select), resident(chosen)),
                flops=1 << 31,
                grid=(classes // chunk,),
                in_specs=[
                    whole,
                    whole,
                    whole,
                    pl.BlockSpec((9 * spheres, chunk * spheres), lambda k: (0, k)),
                    pl.BlockSpec((chunk, rows, coefs), lambda k: (k, 0, 0)),
                    whole,
                    whole,
                ],
                out_specs=(whole, whole),
                scratch_shapes=[pltpu.VMEM((rows, 9 * spheres), BF16)],
            )
        return (resident(partial), resident(near), resident(leaf_in)), tables

    window, *prepared = windows()
    inward, tables = apply(halo, column, window, prepared)
    mie_full = tables[3]
    far = tuple(
        resident(item) for item in (receive, cosines, sines, box, leaf_cos, leaf_sin, mie_full)
    )
    vector = resident(vector)
    once, halo, column = call(
        middle_kernel,
        (kept((rows, spheres)), halo_shape, column_shape),
        inward + (resident(send),) + far,
        flops=1 << 26,
    )
    sums = call(sums_kernel, kept((1, 128)), (vector, resident(once)), 1 << 24)
    inward, _ = apply(halo, column, window, None, tables)
    once = resident(once)
    twice, everyone = call(
        last_kernel,
        (kept((rows, spheres)), kept((first_count, 1, 128))),
        (vector, once) + inward + far + (resident(sums),),
        flops=1 << 26,
    )
    everyone = call(
        relay_kernel, kept((second_count, 1, 128)), (resident(exchange(everyone, FIRST)),), 1 << 20
    )
    solved, residual = call(
        solve_kernel,
        (shape((rows, spheres)), shape((rows, spheres))),
        (resident(exchange(everyone, SECOND)), vector, once, resident(twice)),
        flops=1 << 24,
    )
    return solved.reshape(incident.shape), residual.reshape(incident.shape)


def build(devices, sizes):
    torus = Mesh(devices.reshape(sizes), BX + BY)
    placed = (
        P(None, None, BX, BY, None),
        P(None, None, BX, BY, None),
        P(None, BX, BY, None),
        P(BX, BY, None),
        P(),
        P(BX, BY, None, None),
        P(BX, BY, None, None),
        P(),
        P(),
        P(),
        P(BX, BY, None, None),
        P(BX, BY, None, None),
        P(),
    )
    return jax.shard_map(
        local,
        mesh=torus,
        in_specs=placed,
        out_specs=(P(None, None, BX, BY, None), P(None, None, BX, BY, None)),
        check_vma=False,
    )


def solution(mesh):
    return build(mesh.devices, (2, 8, 4, 4, 2))
```

```python
import functools
import math

import jax
import jax.numpy as jnp
import numpy as np
from jax import lax
from jax.experimental import pallas as pl
from jax.experimental.pallas import tpu as pltpu
from jax.sharding import Mesh
from jax.sharding import PartitionSpec as P

BX = ("bx_0", "bx_1")
BY = ("by_0", "by_1", "by_2")
SHORT = ("bx_0", "by_1", "by_2")
LONG = ("by_0", "bx_1")

HIGHEST = lax.Precision.HIGHEST
KAPPA = 1.5
GOLDEN = 2.399963229728653
F32 = jnp.float32
BF16 = jnp.bfloat16
NT = (((1,), (1,)), ((), ()))
TN = (((0,), (0,)), ((), ()))
INTERPRET = False


def call(kernel, out_shape, operands, flops=0, **kw):
    if "specs" in kw:
        kw["in_specs"] = kw.pop("specs")
    elif "grid" not in kw:
        kw["in_specs"] = [
            pl.BlockSpec(memory_space=pltpu.SMEM if op.ndim == 1 else pltpu.VMEM)
            for op in operands
        ]
    return pl.pallas_call(
        kernel,
        out_shape=out_shape,
        interpret=INTERPRET,
        cost_estimate=pl.CostEstimate(flops=flops, transcendentals=0, bytes_accessed=1 << 20),
        **kw,
    )(*operands)


def resident(x):
    return x if INTERPRET else pltpu.with_memory_space_constraint(x, pltpu.VMEM)


def kept(dims, dtype=F32):
    return shape(dims, dtype) if INTERPRET else pltpu.VMEM(dims, dtype)


def shape(dims, dtype=F32):
    return jax.ShapeDtypeStruct(dims, dtype)


def directions(number):
    ordinal = np.arange(number, dtype=np.float64)
    height = 1.0 - (2.0 * ordinal + 1.0) / number
    radius = np.sqrt(1.0 - height * height)
    return np.stack([radius * np.cos(GOLDEN * ordinal), radius * np.sin(GOLDEN * ordinal), height])


def leaf_centers(number):
    ordinal = np.arange(number)
    return np.stack(
        [
            2.0 * (ordinal % 2) - 1.0,
            2.0 * (ordinal // 2 % 2) - 1.0,
            2.0 * (ordinal // 4) - (number // 4 - 1),
        ]
    )


def mie_spread(coef_count, mie_count):
    half_count = coef_count // 2
    table = np.zeros((coef_count, mie_count), np.float32)
    for number in range(coef_count):
        degree = math.isqrt(number % half_count + 1)
        table[number, number // half_count * (mie_count // 2) + degree - 1] = 1.0
    return table


def dot(a, b, dims=(((1,), (0,)), ((), ())), precision=None):
    return lax.dot_general(a, b, dims, precision=precision, preferred_element_type=F32)


def split(x):
    high = x.astype(BF16)
    return high, (x - high.astype(F32)).astype(BF16)


def one_hot(rows, row):
    ordinal = lax.broadcasted_iota(jnp.int32, (rows, row.shape[1]), 0)
    return jnp.where(ordinal == row, 1.0, 0.0)


def emit(vector, pattern, cosines, sines, member, leaf_cos, leaf_sin, halo_ref, column_ref):
    coefs = vector.shape[0] // 2
    boxes, dirs = leaf_cos.shape
    rounded = vector.astype(BF16)
    halo_ref[0, : 2 * coefs, :] = rounded
    by_real = dot(pattern, rounded[:coefs])
    by_imag = dot(pattern, rounded[coefs:])
    real = by_real[:dirs] - by_imag[dirs:]
    imag = by_real[dirs:] + by_imag[:dirs]
    out = jnp.concatenate([real * cosines + imag * sines, imag * cosines - real * sines], axis=0)
    high, low = split(out)
    leaf = dot(member, high, NT) + dot(member, low, NT)
    leaf_real, leaf_imag = leaf[:, :dirs], leaf[:, dirs:]
    halo_ref[0, 2 * coefs : 2 * coefs + boxes, :] = leaf_real.astype(BF16)
    halo_ref[0, 2 * coefs + boxes :, :] = leaf_imag.astype(BF16)
    column_real = jnp.sum(leaf_real * leaf_cos + leaf_imag * leaf_sin, axis=0, keepdims=True)
    column_imag = jnp.sum(leaf_imag * leaf_cos - leaf_real * leaf_sin, axis=0, keepdims=True)
    pair = jnp.concatenate([column_real, column_imag], axis=0)
    column_ref[...] = jnp.broadcast_to(pair[None], column_ref.shape)


def lanes(values):
    lane = lax.broadcasted_iota(jnp.int32, (1, 128), 1)
    row = jnp.zeros((1, 128), F32)
    for place, value in values:
        row = row + jnp.where(lane == place, value, 0.0)
    return row


def inner(a, b):
    return jnp.sum(jnp.sum(a * b, axis=0, keepdims=True), axis=1, keepdims=True)


def first_kernel(
    vector, pattern, offsets, planes, box, leaf_cos, leaf_sin, halo, column, cos_ref, sin_ref, send
):
    turned = jnp.concatenate([pattern[0].T, pattern[1].T], axis=0)
    send[...] = turned
    phases = KAPPA * (
        planes[0] * offsets[0] + planes[1] * offsets[1] + planes[2] * offsets[2]
    )
    cosines, sines = jnp.cos(phases), jnp.sin(phases)
    cos_ref[...] = cosines
    sin_ref[...] = sines
    member = one_hot(leaf_cos.shape[0], box[...]).astype(BF16)
    emit(vector[...], turned, cosines, sines, member, leaf_cos[...], leaf_sin[...], halo, column)


def mirrored(sources, width, flip_x, flip_y):
    line = 3 * width
    flat = jnp.where(sources < line, 0, jnp.where(sources < 2 * line, 1, 2))
    within = sources - line * flat
    side = jnp.where(within < width, 0, jnp.where(within < 2 * width, 1, 2))
    return sources + flip_x * (2 - 2 * flat) * line + flip_y * (2 - 2 * side) * width


def fill_tables(sources, classes, transfer, mie, spread, select, chosen, mie_full):
    boxes, entries = sources.shape
    row = lax.broadcasted_iota(jnp.int32, (boxes, boxes), 0)
    col = lax.broadcasted_iota(jnp.int32, (boxes, boxes), 1)
    unit = jnp.where(row == col, 1.0, 0.0).astype(BF16)
    around = dot(sources[...].astype(F32).astype(BF16), unit, TN)
    kinds = dot(classes[...].astype(F32).astype(BF16), unit, TN)
    box_lane = lax.broadcasted_iota(jnp.int32, (entries, select.shape[1]), 1).astype(F32)
    kind_lane = lax.broadcasted_iota(jnp.int32, (entries, transfer.shape[0]), 1).astype(F32)
    hots = []
    for item in range(boxes):
        at = slice(item * entries, (item + 1) * entries)
        hots.append(jnp.where(kinds[:, item : item + 1] == kind_lane, 1.0, 0.0))
        select[at, :] = jnp.where(around[:, item : item + 1] == box_lane, 1.0, 0.0).astype(BF16)
    hot = jnp.concatenate(hots, axis=0)
    dirs = transfer.shape[2]
    chosen[:, :dirs] = dot(hot, transfer[:, 0, :], precision=HIGHEST)
    chosen[:, dirs:] = dot(hot, transfer[:, 1, :], precision=HIGHEST)
    mie_full[...] = dot(spread[...], mie[...], precision=HIGHEST)


def window_kernel(
    index,
    transfer,
    near_sources,
    far_sources,
    *rest,
    spheres,
    boxes,
    near_z,
    near_x,
    groups,
    run,
    top_x,
    top_y,
):
    copied = len(rest) // 2 - 1
    window, near_out, far_out = rest[copied : copied + 3]
    row, col = lax.div(index[0], near_x * run), lax.rem(index[0], near_x * run)
    flips = lax.rem(row, 2), lax.rem(col, 2)
    near_out[...] = mirrored(near_sources[...], spheres, *flips)
    far_out[...] = mirrored(far_sources[...], boxes, *flips)
    for source, target in zip(rest[:copied], rest[copied + 3 :]):
        target[...] = source[...]
    high, depth = lax.div(row, near_z), lax.rem(row, near_z)
    across, lane = lax.div(col, run), lax.rem(col, run)
    ordinal = lax.broadcasted_iota(jnp.int32, (near_z, 128), 0)
    for group in range(groups):
        start = (high - group) * near_z - depth
        apart_x = jnp.abs(ordinal + start)
        for other in range(run):
            for x in range(near_x):
                shift = (x - across) * run + lane - other
                keep = (apart_x >= 2) | (jnp.abs(shift) >= 2)
                for part in range(2):
                    rows = transfer[pl.ds(start + top_x, near_z), shift + top_y, part, :]
                    window[part, group * run + other, x * near_z : (x + 1) * near_z, :] = jnp.where(
                        keep, rows, 0.0
                    )


def coarse_kernel(columns, window, partial):
    real, imag = columns[:, 0, :][None], columns[:, 1, :][None]
    partial[:, 0, :] = jnp.sum(real * window[0] - imag * window[1], axis=1)
    partial[:, 1, :] = jnp.sum(imag * window[0] + real * window[1], axis=1)


def near_start(before, own, after, select, chosen, near, leaf_in, columns):
    coefs = near.shape[0] // 2
    spheres = near.shape[1] // 2
    boxes, dirs = leaf_in.shape[0], leaf_in.shape[1] // 2
    leaves = []
    for row in range(3):
        for col, part in enumerate((before, own, after)):
            place = (row * 3 + col) * spheres
            columns[:, place : place + spheres] = part[row, : 2 * coefs, :]
            leaves.append(part[row, 2 * coefs :, :])
    around = jnp.concatenate(
        [
            jnp.concatenate([leaf[:boxes] for leaf in leaves], axis=0),
            jnp.concatenate([leaf[boxes:] for leaf in leaves], axis=0),
        ],
        axis=1,
    )
    picked = dot(select[...], around)
    pick_real, pick_imag = picked[:, :dirs], picked[:, dirs:]
    move_real, move_imag = chosen[:, :dirs], chosen[:, dirs:]
    got_real = pick_real * move_real - pick_imag * move_imag
    got_imag = pick_imag * move_real + pick_real * move_imag
    leaf_in[:, :dirs] = jnp.sum(got_real.reshape(boxes, -1, dirs), axis=1)
    leaf_in[:, dirs:] = jnp.sum(got_imag.reshape(boxes, -1, dirs), axis=1)
    near[...] = jnp.zeros(near.shape, F32)


def near_step(columns, counts, table, near):
    coefs = near.shape[0] // 2
    spheres = near.shape[1] // 2
    gathered = dot(columns[...], counts).astype(BF16)
    total = near[...]
    for item in range(table.shape[0]):
        at = slice(item * spheres, (item + 1) * spheres)
        pair = jnp.concatenate([gathered[:coefs, at], gathered[coefs:, at]], axis=1)
        total = total + dot(table[item], pair)
    near[...] = total


def near_kernel(before, own, after, counts, table, select, chosen, near, leaf_in, columns):
    @pl.when(pl.program_id(0) == 0)
    def _():
        near_start(before, own, after, select, chosen, near, leaf_in, columns)

    near_step(columns, counts[...], table, near)


def both_kernel(
    sources,
    far_sources,
    targets,
    kinds,
    transfer,
    mie,
    spread,
    before,
    own,
    after,
    table_hbm,
    near,
    leaf_in,
    counts_hbm,
    select,
    chosen,
    mie_full,
    columns,
    block,
    table,
    sems,
):
    groups, long, wide = block.shape
    spheres = long // 9
    chunk = wide // spheres
    loading = pltpu.make_async_copy(table_hbm, table, sems.at[groups])
    loading.start()
    storing = []
    for group in range(groups):
        for item in range(chunk):
            at = slice(group * chunk + item, group * chunk + item + 1)
            source_hot = one_hot(long, sources[at, :]).astype(BF16)
            target_hot = one_hot(spheres, targets[at, :]).astype(BF16)
            block[group, :, item * spheres : (item + 1) * spheres] = dot(
                source_hot, target_hot, NT
            ).astype(BF16)
        keep = pltpu.make_async_copy(
            block.at[group], counts_hbm.at[:, pl.ds(group * wide, wide)], sems.at[group]
        )
        keep.start()
        storing.append(keep)
        if group == 0:
            fill_tables(far_sources, kinds, transfer, mie, spread, select, chosen, mie_full)
            near_start(before, own, after, select, chosen, near, leaf_in, columns)
            loading.wait()
        near_step(
            columns, block[group], table.at[pl.ds(group * chunk, chunk)], near
        )
    for keep in storing:
        keep.wait()


def arrive(partial, near, leaf_in, receive, cosines, sines, member, leaf_cos, leaf_sin, mie_full):
    _, dirs = leaf_cos.shape
    coefs = near.shape[0] // 2
    column_real = jnp.sum(partial[:, 0, :], axis=0, keepdims=True)
    column_imag = jnp.sum(partial[:, 1, :], axis=0, keepdims=True)
    incoming = leaf_in + jnp.concatenate(
        [
            column_real * leaf_cos - column_imag * leaf_sin,
            column_real * leaf_sin + column_imag * leaf_cos,
        ],
        axis=1,
    )
    high, low = split(incoming)
    spread = dot(high, member, TN) + dot(low, member, TN)
    real, imag = spread[:dirs], spread[dirs:]
    arriving = jnp.concatenate(
        [real * cosines - imag * sines, real * sines + imag * cosines], axis=1
    ).astype(BF16)
    total = near + dot(receive, arriving)
    half = total.shape[1] // 2
    field_real = total[:coefs, :half] - total[coefs:, half:]
    field_imag = total[coefs:, :half] + total[:coefs, half:]
    mie_real, mie_imag = mie_full[:coefs], mie_full[coefs:]
    return jnp.concatenate(
        [
            field_real * mie_real - field_imag * mie_imag,
            field_real * mie_imag + field_imag * mie_real,
        ],
        axis=0,
    )


def sums_kernel(vector, scattered, sums):
    u, d = vector[...], scattered[...]
    sums[...] = lanes([(0, inner(u, u)), (1, inner(u, d)), (2, inner(d, d))])


def middle_kernel(
    partial,
    near,
    leaf_in,
    pattern,
    receive,
    cosines,
    sines,
    box,
    leaf_cos,
    leaf_sin,
    mie_full,
    applied,
    halo,
    column,
):
    member = one_hot(leaf_cos.shape[0], box[...]).astype(BF16)
    scattered = arrive(
        partial[...],
        near[...],
        leaf_in[...],
        receive[...],
        cosines[...],
        sines[...],
        member,
        leaf_cos[...],
        leaf_sin[...],
        mie_full[...],
    )
    applied[...] = scattered
    emit(
        scattered,
        pattern[...],
        cosines[...],
        sines[...],
        member,
        leaf_cos[...],
        leaf_sin[...],
        halo,
        column,
    )


def last_kernel(
    vector,
    scattered,
    partial,
    near,
    leaf_in,
    receive,
    cosines,
    sines,
    box,
    leaf_cos,
    leaf_sin,
    mie_full,
    sums,
    applied,
    everyone,
):
    member = one_hot(leaf_cos.shape[0], box[...]).astype(BF16)
    twice = arrive(
        partial[...],
        near[...],
        leaf_in[...],
        receive[...],
        cosines[...],
        sines[...],
        member,
        leaf_cos[...],
        leaf_sin[...],
        mie_full[...],
    )
    applied[...] = twice
    row = sums[...] + lanes(
        [(3, inner(vector[...], twice)), (4, inner(scattered[...], twice)), (5, inner(twice, twice))]
    )
    everyone[...] = jnp.broadcast_to(row[None], everyone.shape)


def relay_kernel(parts, everyone):
    everyone[...] = jnp.broadcast_to(jnp.sum(parts[...], axis=0, keepdims=True), everyone.shape)


def solve_kernel(parts, vector, scattered, twice, solution, residual):
    row = jnp.sum(parts[...], axis=0)
    lane = lax.broadcasted_iota(jnp.int32, row.shape, 1)

    def total(place):
        value = jnp.sum(jnp.where(lane == place, row, 0.0), axis=1, keepdims=True)
        return jnp.broadcast_to(value, (8, 128))

    uu, ud, dd, ue, de, ee = (total(place) for place in range(6))
    beta = jnp.sqrt(uu)
    along = ud / uu
    across = dd - along * ud
    size = jnp.sqrt(across)
    h00 = 1.0 - along
    h10 = size / beta
    turned = de - along * ue
    h01 = (ue - along * ud) / (size * beta)
    h11 = 1.0 + along - turned / across
    rest_u = ue / uu
    rest_d = turned / across
    left = ee - rest_u * ue - rest_d * turned
    h21 = jnp.sqrt(left) / size
    n00 = h00 * h00 + h10 * h10
    n01 = h00 * h01 + h10 * h11
    n11 = h01 * h01 + h11 * h11 + h21 * h21
    l00 = jnp.sqrt(n00)
    l10 = n01 / l00
    l11 = jnp.sqrt(n11 - l10 * l10)
    m0 = beta * h00 / l00
    m1 = (beta * h01 - l10 * m0) / l11
    y1 = m1 / l11
    y0 = (m0 - l10 * y1) / l00
    z0 = h00 * y0 + h01 * y1
    z1 = h10 * y0 + h11 * y1
    step = y1 / size
    sol_u = y0 / beta + step * along
    sol_d = -step
    res_u = (beta - z0) / beta - z1 / size * along + step * (rest_u - rest_d * along)
    res_d = z1 / size + step * rest_d
    res_e = -step
    u, d, e = vector[...], scattered[...], twice[...]
    solution[...] = sol_u[0:1] * u + sol_d[0:1] * d
    residual[...] = res_u[0:1] * u + res_d[0:1] * d + res_e[0:1] * e


def swap(x, axes, first):
    pairs = [(i, i + 1) for i in range(first, lax.axis_size(axes) - 1, 2)]
    return lax.ppermute(x, axes, pairs + [(j, i) for i, j in pairs])


def exchange(x, axes):
    return lax.all_to_all(x, axes, split_axis=0, concat_axis=0, tiled=True)


def local(
    incident,
    mie,
    offsets,
    sphere_box,
    near_table,
    near_src,
    near_dst,
    pattern,
    receive,
    leaf_transfer,
    far_src,
    far_cls,
    coarse_transfer,
):
    coefs = incident.shape[1]
    spheres = incident.shape[4]
    rows = 2 * coefs
    dirs = pattern.shape[1]
    boxes, entries = far_src.shape[2:]
    classes, pairs = near_src.shape[2:]
    high_count, near_z = lax.axis_size("bx_0"), lax.axis_size("bx_1")
    near_x = lax.axis_size("by_0")
    run = lax.axis_size(("by_1", "by_2"))
    short_count, long_count = lax.axis_size(SHORT), lax.axis_size(LONG)
    index = lax.axis_index(BX + BY).astype(jnp.int32).reshape(1)

    planes = jnp.asarray(directions(dirs)[:, :, None].astype(np.float32))
    centre = KAPPA * (leaf_centers(boxes).T @ directions(dirs))
    leaf_cos = jnp.asarray(np.cos(centre).astype(np.float32))
    leaf_sin = jnp.asarray(np.sin(centre).astype(np.float32))

    vector = incident.reshape(rows, spheres)
    box = sphere_box.reshape(1, spheres)
    pattern = pattern.transpose(0, 2, 1)
    receive = receive.reshape(rows, dirs)

    halo_shape = kept((1, rows + 2 * boxes, spheres), BF16)
    column_shape = kept((long_count, 2, dirs))
    halo, column, cosines, sines, send = call(
        first_kernel,
        (
            halo_shape,
            column_shape,
            kept((dirs, spheres)),
            kept((dirs, spheres)),
            kept((2 * dirs, coefs), BF16),
        ),
        (vector, pattern, offsets.reshape(3, 1, spheres), planes, box, leaf_cos, leaf_sin),
        flops=1 << 26,
    )
    chunk = classes // 2
    whole = pl.BlockSpec(memory_space=pltpu.VMEM)

    def windows():
        spread = mie_spread(coefs, mie.shape[1])
        zero = np.zeros_like(spread)
        copied = (
            near_dst.reshape(classes, pairs),
            far_cls.reshape(boxes, entries),
            leaf_transfer,
            mie.reshape(2 * mie.shape[1], spheres),
            jnp.asarray(np.block([[spread, zero], [zero, spread]])),
        )
        return call(
            functools.partial(
                window_kernel,
                spheres=spheres,
                boxes=boxes,
                near_z=near_z,
                near_x=near_x,
                groups=high_count,
                run=run,
                top_x=high_count * near_z - 1,
                top_y=near_x * run - 1,
            ),
            (
                kept((2, short_count, long_count, dirs)),
                kept((classes, pairs), jnp.int32),
                kept((boxes, entries), jnp.int32),
            )
            + tuple(kept(item.shape, item.dtype) for item in copied),
            (
                index,
                coarse_transfer.transpose(1, 2, 0, 3),
                near_src.reshape(classes, pairs),
                far_src.reshape(boxes, entries),
            )
            + copied,
            flops=1 << 28,
        )

    def apply(halo, column, window, prepared, tables=None):
        columns = exchange(column, LONG)
        ahead = swap(halo, BX, 0)
        behind = swap(halo, BX, 1)
        line = jnp.concatenate([behind, halo, ahead], axis=0)
        right = swap(line, BY, 0)
        left = swap(line, BY, 1)
        partial = call(
            coarse_kernel,
            kept((short_count, 2, dirs)),
            (resident(columns), resident(window)),
            1 << 24,
        )
        partial = exchange(partial, SHORT)
        lines = resident(left), resident(line), resident(right)
        table = near_table.reshape(classes, rows, coefs)
        sums = (kept((rows, 2 * spheres)), kept((boxes, 2 * dirs)))
        if tables is None:
            groups = classes // 4
            any_spec = pl.BlockSpec(memory_space=pl.ANY)
            near, leaf_in, *tables = call(
                both_kernel,
                sums
                + (
                    shape((9 * spheres, classes * spheres), BF16),
                    kept((boxes * entries, 9 * boxes), BF16),
                    kept((boxes * entries, 2 * dirs)),
                    kept((rows, spheres)),
                ),
                tuple(resident(item) for item in prepared) + lines + (table,),
                flops=1 << 31,
                specs=[whole] * 10 + [any_spec],
                out_specs=(whole, whole, any_spec, whole, whole, whole),
                scratch_shapes=[
                    pltpu.VMEM((rows, 9 * spheres), BF16),
                    pltpu.VMEM((groups, 9 * spheres, 4 * spheres), BF16),
                    pltpu.VMEM((classes, rows, coefs), BF16),
                    pltpu.SemaphoreType.DMA((groups + 1,)),
                ],
            )
        else:
            counts, select, chosen, _ = tables
            near, leaf_in = call(
                near_kernel,
                sums,
                lines + (counts, table, resident(select), resident(chosen)),
                flops=1 << 31,
                grid=(classes // chunk,),
                in_specs=[
                    whole,
                    whole,
                    whole,
                    pl.BlockSpec((9 * spheres, chunk * spheres), lambda k: (0, k)),
                    pl.BlockSpec((chunk, rows, coefs), lambda k: (k, 0, 0)),
                    whole,
                    whole,
                ],
                out_specs=(whole, whole),
                scratch_shapes=[pltpu.VMEM((rows, 9 * spheres), BF16)],
            )
        return (resident(partial), resident(near), resident(leaf_in)), tables

    window, *prepared = windows()
    inward, tables = apply(halo, column, window, prepared)
    mie_full = tables[3]
    far = tuple(
        resident(item) for item in (receive, cosines, sines, box, leaf_cos, leaf_sin, mie_full)
    )
    vector = resident(vector)
    once, halo, column = call(
        middle_kernel,
        (kept((rows, spheres)), halo_shape, column_shape),
        inward + (resident(send),) + far,
        flops=1 << 26,
    )
    sums = call(sums_kernel, kept((1, 128)), (vector, resident(once)), 1 << 24)
    inward, _ = apply(halo, column, window, None, tables)
    once = resident(once)
    twice, everyone = call(
        last_kernel,
        (kept((rows, spheres)), kept((short_count, 1, 128))),
        (vector, once) + inward + far + (resident(sums),),
        flops=1 << 26,
    )
    everyone = call(
        relay_kernel, kept((long_count, 1, 128)), (resident(exchange(everyone, SHORT)),), 1 << 20
    )
    solved, residual = call(
        solve_kernel,
        (shape((rows, spheres)), shape((rows, spheres))),
        (resident(exchange(everyone, LONG)), vector, once, resident(twice)),
        flops=1 << 24,
    )
    return solved.reshape(incident.shape), residual.reshape(incident.shape)


def build(devices, sizes):
    torus = Mesh(devices.reshape(sizes), BX + BY)
    placed = (
        P(None, None, BX, BY, None),
        P(None, None, BX, BY, None),
        P(None, BX, BY, None),
        P(BX, BY, None),
        P(),
        P(BX, BY, None, None),
        P(BX, BY, None, None),
        P(),
        P(),
        P(),
        P(BX, BY, None, None),
        P(BX, BY, None, None),
        P(),
    )
    return jax.shard_map(
        local,
        mesh=torus,
        in_specs=placed,
        out_specs=(P(None, None, BX, BY, None), P(None, None, BX, BY, None)),
        check_vma=False,
    )


def solution(mesh):
    return build(mesh.devices, (2, 8, 4, 4, 2))
```

```python
import functools
import math

import jax
import jax.numpy as jnp
import numpy as np
from jax import lax
from jax.experimental import pallas as pl
from jax.experimental.pallas import tpu as pltpu
from jax.sharding import Mesh
from jax.sharding import PartitionSpec as P

BX = ("bx_0", "bx_1")
BY = ("by_0", "by_1", "by_2")
FIRST = ("bx_0", "by_1", "by_2")
SECOND = ("bx_1", "by_0")

HIGHEST = lax.Precision.HIGHEST
KAPPA = 1.5
GOLDEN = 2.399963229728653
F32 = jnp.float32
BF16 = jnp.bfloat16
NT = (((1,), (1,)), ((), ()))
TN = (((0,), (0,)), ((), ()))
INTERPRET = False


def call(kernel, out_shape, operands, flops=0, **kw):
    if "specs" in kw:
        kw["in_specs"] = kw.pop("specs")
    elif "grid" not in kw:
        kw["in_specs"] = [
            pl.BlockSpec(memory_space=pltpu.SMEM if op.ndim == 1 else pltpu.VMEM)
            for op in operands
        ]
    return pl.pallas_call(
        kernel,
        out_shape=out_shape,
        interpret=INTERPRET,
        cost_estimate=pl.CostEstimate(flops=flops, transcendentals=0, bytes_accessed=1 << 20),
        **kw,
    )(*operands)


def resident(x):
    return x if INTERPRET else pltpu.with_memory_space_constraint(x, pltpu.VMEM)


def kept(dims, dtype=F32):
    return shape(dims, dtype) if INTERPRET else pltpu.VMEM(dims, dtype)


def shape(dims, dtype=F32):
    return jax.ShapeDtypeStruct(dims, dtype)


def directions(number):
    ordinal = np.arange(number, dtype=np.float64)
    height = 1.0 - (2.0 * ordinal + 1.0) / number
    radius = np.sqrt(1.0 - height * height)
    return np.stack([radius * np.cos(GOLDEN * ordinal), radius * np.sin(GOLDEN * ordinal), height])


def leaf_centers(number):
    ordinal = np.arange(number)
    return np.stack(
        [
            2.0 * (ordinal % 2) - 1.0,
            2.0 * (ordinal // 2 % 2) - 1.0,
            2.0 * (ordinal // 4) - (number // 4 - 1),
        ]
    )


def mie_spread(coef_count, mie_count):
    half_count = coef_count // 2
    table = np.zeros((coef_count, mie_count), np.float32)
    for number in range(coef_count):
        degree = math.isqrt(number % half_count + 1)
        table[number, number // half_count * (mie_count // 2) + degree - 1] = 1.0
    return table


def dot(a, b, dims=(((1,), (0,)), ((), ())), precision=None):
    return lax.dot_general(a, b, dims, precision=precision, preferred_element_type=F32)


def split(x):
    high = x.astype(BF16)
    return high, (x - high.astype(F32)).astype(BF16)


def one_hot(rows, row):
    ordinal = lax.broadcasted_iota(jnp.int32, (rows, row.shape[1]), 0)
    return jnp.where(ordinal == row, 1.0, 0.0)


def emit(vector, pattern, cosines, sines, member, leaf_cos, leaf_sin, halo_ref, column_ref):
    coefs = vector.shape[0] // 2
    boxes, dirs = leaf_cos.shape
    rounded = vector.astype(BF16)
    halo_ref[0, : 2 * coefs, :] = rounded
    by_real = dot(pattern, rounded[:coefs])
    by_imag = dot(pattern, rounded[coefs:])
    real = by_real[:dirs] - by_imag[dirs:]
    imag = by_real[dirs:] + by_imag[:dirs]
    out = jnp.concatenate([real * cosines + imag * sines, imag * cosines - real * sines], axis=0)
    high, low = split(out)
    leaf = dot(member, high, NT) + dot(member, low, NT)
    leaf_real, leaf_imag = leaf[:, :dirs], leaf[:, dirs:]
    halo_ref[0, 2 * coefs : 2 * coefs + boxes, :] = leaf_real.astype(BF16)
    halo_ref[0, 2 * coefs + boxes :, :] = leaf_imag.astype(BF16)
    column_real = jnp.sum(leaf_real * leaf_cos + leaf_imag * leaf_sin, axis=0, keepdims=True)
    column_imag = jnp.sum(leaf_imag * leaf_cos - leaf_real * leaf_sin, axis=0, keepdims=True)
    pair = jnp.concatenate([column_real, column_imag], axis=0)
    column_ref[...] = jnp.broadcast_to(pair[None], column_ref.shape)


def lanes(values):
    lane = lax.broadcasted_iota(jnp.int32, (1, 128), 1)
    row = jnp.zeros((1, 128), F32)
    for place, value in values:
        row = row + jnp.where(lane == place, value, 0.0)
    return row


def inner(a, b):
    return jnp.sum(jnp.sum(a * b, axis=0, keepdims=True), axis=1, keepdims=True)


def first_kernel(
    vector, pattern, offsets, planes, box, leaf_cos, leaf_sin, halo, column, cos_ref, sin_ref, send
):
    turned = jnp.concatenate([pattern[0].T, pattern[1].T], axis=0)
    send[...] = turned
    phases = KAPPA * (
        planes[0] * offsets[0] + planes[1] * offsets[1] + planes[2] * offsets[2]
    )
    cosines, sines = jnp.cos(phases), jnp.sin(phases)
    cos_ref[...] = cosines
    sin_ref[...] = sines
    member = one_hot(leaf_cos.shape[0], box[...]).astype(BF16)
    emit(vector[...], turned, cosines, sines, member, leaf_cos[...], leaf_sin[...], halo, column)


def mirrored(sources, width, flip_x, flip_y):
    line = 3 * width
    flat = jnp.where(sources < line, 0, jnp.where(sources < 2 * line, 1, 2))
    within = sources - line * flat
    side = jnp.where(within < width, 0, jnp.where(within < 2 * width, 1, 2))
    return sources + flip_x * (2 - 2 * flat) * line + flip_y * (2 - 2 * side) * width


def fill_tables(sources, classes, transfer, mie, spread, select, chosen, mie_full):
    boxes, entries = sources.shape
    row = lax.broadcasted_iota(jnp.int32, (boxes, boxes), 0)
    col = lax.broadcasted_iota(jnp.int32, (boxes, boxes), 1)
    unit = jnp.where(row == col, 1.0, 0.0).astype(BF16)
    around = dot(sources[...].astype(F32).astype(BF16), unit, TN)
    kinds = dot(classes[...].astype(F32).astype(BF16), unit, TN)
    box_lane = lax.broadcasted_iota(jnp.int32, (entries, select.shape[1]), 1).astype(F32)
    kind_lane = lax.broadcasted_iota(jnp.int32, (entries, transfer.shape[0]), 1).astype(F32)
    hots = []
    for item in range(boxes):
        at = slice(item * entries, (item + 1) * entries)
        hots.append(jnp.where(kinds[:, item : item + 1] == kind_lane, 1.0, 0.0))
        select[at, :] = jnp.where(around[:, item : item + 1] == box_lane, 1.0, 0.0).astype(BF16)
    hot = jnp.concatenate(hots, axis=0)
    dirs = transfer.shape[2]
    chosen[:, :dirs] = dot(hot, transfer[:, 0, :], precision=HIGHEST)
    chosen[:, dirs:] = dot(hot, transfer[:, 1, :], precision=HIGHEST)
    mie_full[...] = dot(spread[...], mie[...], precision=HIGHEST)


def window_kernel(
    index,
    transfer,
    near_sources,
    far_sources,
    *rest,
    spheres,
    boxes,
    near_z,
    near_x,
    groups,
    run,
    top_x,
    top_y,
):
    *rest, held, sem = rest
    copied = len(rest) // 2 - 1
    window, near_out, far_out = rest[copied : copied + 3]
    row, col = lax.div(index[0], near_x * run), lax.rem(index[0], near_x * run)
    flips = lax.rem(row, 2), lax.rem(col, 2)
    high, depth = lax.div(row, near_z), lax.rem(row, near_z)
    across, lane = lax.div(col, run), lax.rem(col, run)
    first_shift = depth - high * near_z - (near_z - 1)
    fetch = pltpu.make_async_copy(transfer.at[pl.ds(first_shift + top_x, held.shape[0])], held, sem)
    fetch.start()
    near_out[...] = mirrored(near_sources[...], spheres, *flips)
    far_out[...] = mirrored(far_sources[...], boxes, *flips)
    for source, target in zip(rest[:copied], rest[copied + 3 :]):
        target[...] = source[...]
    fetch.wait()
    ordinal = lax.broadcasted_iota(jnp.int32, (run, 128), 0)
    for z in range(near_z):
        for x in range(near_x):
            start = (across - x) * run - lane + top_y
            apart_y = jnp.abs(ordinal + (start - top_y))
            for group in range(groups):
                shift = (group - high) * near_z + depth - z
                keep = (apart_y >= 2) | (jnp.abs(shift) >= 2)
                for part in range(2):
                    rows = held[group * near_z + near_z - 1 - z, pl.ds(start, run), part, :]
                    window[part, z * near_x + x, group * run : (group + 1) * run, :] = jnp.where(
                        keep, rows, 0.0
                    )


def coarse_kernel(columns, window, partial):
    real, imag = columns[:, 0, :][None], columns[:, 1, :][None]
    partial[:, 0, :] = jnp.sum(real * window[0] - imag * window[1], axis=1)
    partial[:, 1, :] = jnp.sum(imag * window[0] + real * window[1], axis=1)


def near_start(before, own, after, select, chosen, near, leaf_in, columns):
    coefs = near.shape[0] // 2
    spheres = near.shape[1] // 2
    boxes, dirs = leaf_in.shape[0], leaf_in.shape[1] // 2
    leaves = []
    for row in range(3):
        for col, part in enumerate((before, own, after)):
            place = (row * 3 + col) * spheres
            columns[:, place : place + spheres] = part[row, : 2 * coefs, :]
            leaves.append(part[row, 2 * coefs :, :])
    around = jnp.concatenate(
        [
            jnp.concatenate([leaf[:boxes] for leaf in leaves], axis=0),
            jnp.concatenate([leaf[boxes:] for leaf in leaves], axis=0),
        ],
        axis=1,
    )
    picked = dot(select[...], around)
    pick_real, pick_imag = picked[:, :dirs], picked[:, dirs:]
    move_real, move_imag = chosen[:, :dirs], chosen[:, dirs:]
    got_real = pick_real * move_real - pick_imag * move_imag
    got_imag = pick_imag * move_real + pick_real * move_imag
    leaf_in[:, :dirs] = jnp.sum(got_real.reshape(boxes, -1, dirs), axis=1)
    leaf_in[:, dirs:] = jnp.sum(got_imag.reshape(boxes, -1, dirs), axis=1)
    near[...] = jnp.zeros(near.shape, F32)


def near_step(columns, counts, table, near):
    coefs = near.shape[0] // 2
    spheres = near.shape[1] // 2
    gathered = dot(columns[...], counts).astype(BF16)
    total = near[...]
    for item in range(table.shape[0]):
        at = slice(item * spheres, (item + 1) * spheres)
        pair = jnp.concatenate([gathered[:coefs, at], gathered[coefs:, at]], axis=1)
        total = total + dot(table[item], pair)
    near[...] = total


def near_kernel(before, own, after, counts, table, select, chosen, near, leaf_in, columns):
    @pl.when(pl.program_id(0) == 0)
    def _():
        near_start(before, own, after, select, chosen, near, leaf_in, columns)

    near_step(columns, counts[...], table, near)


def both_kernel(
    sources,
    far_sources,
    targets,
    kinds,
    transfer,
    mie,
    spread,
    before,
    own,
    after,
    table_hbm,
    near,
    leaf_in,
    counts_hbm,
    select,
    chosen,
    mie_full,
    columns,
    block,
    table,
    sems,
):
    groups, long, wide = block.shape
    spheres = long // 9
    chunk = wide // spheres
    loading = pltpu.make_async_copy(table_hbm, table, sems.at[groups])
    loading.start()
    storing = []
    for group in range(groups):
        for item in range(chunk):
            at = slice(group * chunk + item, group * chunk + item + 1)
            source_hot = one_hot(long, sources[at, :]).astype(BF16)
            target_hot = one_hot(spheres, targets[at, :]).astype(BF16)
            block[group, :, item * spheres : (item + 1) * spheres] = dot(
                source_hot, target_hot, NT
            ).astype(BF16)
        keep = pltpu.make_async_copy(
            block.at[group], counts_hbm.at[:, pl.ds(group * wide, wide)], sems.at[group]
        )
        keep.start()
        storing.append(keep)
        if group == 0:
            fill_tables(far_sources, kinds, transfer, mie, spread, select, chosen, mie_full)
            near_start(before, own, after, select, chosen, near, leaf_in, columns)
            loading.wait()
        near_step(
            columns, block[group], table.at[pl.ds(group * chunk, chunk)], near
        )
    for keep in storing:
        keep.wait()


def arrive(partial, near, leaf_in, receive, cosines, sines, member, leaf_cos, leaf_sin, mie_full):
    _, dirs = leaf_cos.shape
    coefs = near.shape[0] // 2
    column_real = jnp.sum(partial[:, 0, :], axis=0, keepdims=True)
    column_imag = jnp.sum(partial[:, 1, :], axis=0, keepdims=True)
    incoming = leaf_in + jnp.concatenate(
        [
            column_real * leaf_cos - column_imag * leaf_sin,
            column_real * leaf_sin + column_imag * leaf_cos,
        ],
        axis=1,
    )
    high, low = split(incoming)
    spread = dot(high, member, TN) + dot(low, member, TN)
    real, imag = spread[:dirs], spread[dirs:]
    arriving = jnp.concatenate(
        [real * cosines - imag * sines, real * sines + imag * cosines], axis=1
    ).astype(BF16)
    total = near + dot(receive, arriving)
    half = total.shape[1] // 2
    field_real = total[:coefs, :half] - total[coefs:, half:]
    field_imag = total[coefs:, :half] + total[:coefs, half:]
    mie_real, mie_imag = mie_full[:coefs], mie_full[coefs:]
    return jnp.concatenate(
        [
            field_real * mie_real - field_imag * mie_imag,
            field_real * mie_imag + field_imag * mie_real,
        ],
        axis=0,
    )


def sums_kernel(vector, scattered, sums):
    u, d = vector[...], scattered[...]
    sums[...] = lanes([(0, inner(u, u)), (1, inner(u, d)), (2, inner(d, d))])


def middle_kernel(
    partial,
    near,
    leaf_in,
    pattern,
    receive,
    cosines,
    sines,
    box,
    leaf_cos,
    leaf_sin,
    mie_full,
    applied,
    halo,
    column,
):
    member = one_hot(leaf_cos.shape[0], box[...]).astype(BF16)
    scattered = arrive(
        partial[...],
        near[...],
        leaf_in[...],
        receive[...],
        cosines[...],
        sines[...],
        member,
        leaf_cos[...],
        leaf_sin[...],
        mie_full[...],
    )
    applied[...] = scattered
    emit(
        scattered,
        pattern[...],
        cosines[...],
        sines[...],
        member,
        leaf_cos[...],
        leaf_sin[...],
        halo,
        column,
    )


def last_kernel(
    vector,
    scattered,
    partial,
    near,
    leaf_in,
    receive,
    cosines,
    sines,
    box,
    leaf_cos,
    leaf_sin,
    mie_full,
    sums,
    applied,
    everyone,
):
    member = one_hot(leaf_cos.shape[0], box[...]).astype(BF16)
    twice = arrive(
        partial[...],
        near[...],
        leaf_in[...],
        receive[...],
        cosines[...],
        sines[...],
        member,
        leaf_cos[...],
        leaf_sin[...],
        mie_full[...],
    )
    applied[...] = twice
    row = sums[...] + lanes(
        [(3, inner(vector[...], twice)), (4, inner(scattered[...], twice)), (5, inner(twice, twice))]
    )
    everyone[...] = jnp.broadcast_to(row[None], everyone.shape)


def relay_kernel(parts, everyone):
    everyone[...] = jnp.broadcast_to(jnp.sum(parts[...], axis=0, keepdims=True), everyone.shape)


def solve_kernel(parts, vector, scattered, twice, solution, residual):
    row = jnp.sum(parts[...], axis=0)
    lane = lax.broadcasted_iota(jnp.int32, row.shape, 1)

    def total(place):
        value = jnp.sum(jnp.where(lane == place, row, 0.0), axis=1, keepdims=True)
        return jnp.broadcast_to(value, (8, 128))

    uu, ud, dd, ue, de, ee = (total(place) for place in range(6))
    beta = jnp.sqrt(uu)
    along = ud / uu
    across = dd - along * ud
    size = jnp.sqrt(across)
    h00 = 1.0 - along
    h10 = size / beta
    turned = de - along * ue
    h01 = (ue - along * ud) / (size * beta)
    h11 = 1.0 + along - turned / across
    rest_u = ue / uu
    rest_d = turned / across
    left = ee - rest_u * ue - rest_d * turned
    h21 = jnp.sqrt(left) / size
    n00 = h00 * h00 + h10 * h10
    n01 = h00 * h01 + h10 * h11
    n11 = h01 * h01 + h11 * h11 + h21 * h21
    l00 = jnp.sqrt(n00)
    l10 = n01 / l00
    l11 = jnp.sqrt(n11 - l10 * l10)
    m0 = beta * h00 / l00
    m1 = (beta * h01 - l10 * m0) / l11
    y1 = m1 / l11
    y0 = (m0 - l10 * y1) / l00
    z0 = h00 * y0 + h01 * y1
    z1 = h10 * y0 + h11 * y1
    step = y1 / size
    sol_u = y0 / beta + step * along
    sol_d = -step
    res_u = (beta - z0) / beta - z1 / size * along + step * (rest_u - rest_d * along)
    res_d = z1 / size + step * rest_d
    res_e = -step
    u, d, e = vector[...], scattered[...], twice[...]
    solution[...] = sol_u[0:1] * u + sol_d[0:1] * d
    residual[...] = res_u[0:1] * u + res_d[0:1] * d + res_e[0:1] * e


def swap(x, axes, first):
    pairs = [(i, i + 1) for i in range(first, lax.axis_size(axes) - 1, 2)]
    return lax.ppermute(x, axes, pairs + [(j, i) for i, j in pairs])


def exchange(x, axes):
    return lax.all_to_all(x, axes, split_axis=0, concat_axis=0, tiled=True)


def local(
    incident,
    mie,
    offsets,
    sphere_box,
    near_table,
    near_src,
    near_dst,
    pattern,
    receive,
    leaf_transfer,
    far_src,
    far_cls,
    coarse_transfer,
):
    coefs = incident.shape[1]
    spheres = incident.shape[4]
    rows = 2 * coefs
    dirs = pattern.shape[1]
    boxes, entries = far_src.shape[2:]
    classes, pairs = near_src.shape[2:]
    high_count, near_z = lax.axis_size("bx_0"), lax.axis_size("bx_1")
    near_x = lax.axis_size("by_0")
    run = lax.axis_size(("by_1", "by_2"))
    across_x = high_count * near_z
    first_count, second_count = lax.axis_size(FIRST), lax.axis_size(SECOND)
    index = lax.axis_index(BX + BY).astype(jnp.int32).reshape(1)

    planes = jnp.asarray(directions(dirs)[:, :, None].astype(np.float32))
    centre = KAPPA * (leaf_centers(boxes).T @ directions(dirs))
    leaf_cos = jnp.asarray(np.cos(centre).astype(np.float32))
    leaf_sin = jnp.asarray(np.sin(centre).astype(np.float32))

    vector = incident.reshape(rows, spheres)
    box = sphere_box.reshape(1, spheres)
    pattern = pattern.transpose(0, 2, 1)
    receive = receive.reshape(rows, dirs)

    halo_shape = kept((1, rows + 2 * boxes, spheres), BF16)
    column_shape = kept((first_count, 2, dirs))
    halo, column, cosines, sines, send = call(
        first_kernel,
        (
            halo_shape,
            column_shape,
            kept((dirs, spheres)),
            kept((dirs, spheres)),
            kept((2 * dirs, coefs), BF16),
        ),
        (vector, pattern, offsets.reshape(3, 1, spheres), planes, box, leaf_cos, leaf_sin),
        flops=1 << 26,
    )
    chunk = classes // 2
    whole = pl.BlockSpec(memory_space=pltpu.VMEM)

    def windows():
        spread = mie_spread(coefs, mie.shape[1])
        zero = np.zeros_like(spread)
        copied = (
            near_dst.reshape(classes, pairs),
            far_cls.reshape(boxes, entries),
            leaf_transfer,
            mie.reshape(2 * mie.shape[1], spheres),
            jnp.asarray(np.block([[spread, zero], [zero, spread]])),
        )
        return call(
            functools.partial(
                window_kernel,
                spheres=spheres,
                boxes=boxes,
                near_z=near_z,
                near_x=near_x,
                groups=high_count,
                run=run,
                top_x=high_count * near_z - 1,
                top_y=near_x * run - 1,
            ),
            (
                kept((2, second_count, first_count, dirs)),
                kept((classes, pairs), jnp.int32),
                kept((boxes, entries), jnp.int32),
            )
            + tuple(kept(item.shape, item.dtype) for item in copied),
            (
                index,
                coarse_transfer.transpose(1, 2, 0, 3),
                near_src.reshape(classes, pairs),
                far_src.reshape(boxes, entries),
            )
            + copied,
            flops=1 << 28,
            specs=[pl.BlockSpec(memory_space=pltpu.SMEM), pl.BlockSpec(memory_space=pl.ANY)]
            + [whole] * (2 + len(copied)),
            scratch_shapes=[
                pltpu.VMEM((across_x, coarse_transfer.shape[2], 2, dirs), F32),
                pltpu.SemaphoreType.DMA,
            ],
        )

    def apply(halo, column, window, prepared, tables=None):
        columns = exchange(column, FIRST)
        ahead = swap(halo, BX, 0)
        behind = swap(halo, BX, 1)
        line = jnp.concatenate([behind, halo, ahead], axis=0)
        right = swap(line, BY, 0)
        left = swap(line, BY, 1)
        partial = call(
            coarse_kernel,
            kept((second_count, 2, dirs)),
            (resident(columns), resident(window)),
            1 << 24,
        )
        partial = exchange(partial, SECOND)
        lines = resident(left), resident(line), resident(right)
        table = near_table.reshape(classes, rows, coefs)
        sums = (kept((rows, 2 * spheres)), kept((boxes, 2 * dirs)))
        if tables is None:
            groups = classes // 4
            any_spec = pl.BlockSpec(memory_space=pl.ANY)
            near, leaf_in, *tables = call(
                both_kernel,
                sums
                + (
                    shape((9 * spheres, classes * spheres), BF16),
                    kept((boxes * entries, 9 * boxes), BF16),
                    kept((boxes * entries, 2 * dirs)),
                    kept((rows, spheres)),
                ),
                tuple(resident(item) for item in prepared) + lines + (table,),
                flops=1 << 31,
                specs=[whole] * 10 + [any_spec],
                out_specs=(whole, whole, any_spec, whole, whole, whole),
                scratch_shapes=[
                    pltpu.VMEM((rows, 9 * spheres), BF16),
                    pltpu.VMEM((groups, 9 * spheres, 4 * spheres), BF16),
                    pltpu.VMEM((classes, rows, coefs), BF16),
                    pltpu.SemaphoreType.DMA((groups + 1,)),
                ],
            )
        else:
            counts, select, chosen, _ = tables
            near, leaf_in = call(
                near_kernel,
                sums,
                lines + (counts, table, resident(select), resident(chosen)),
                flops=1 << 31,
                grid=(classes // chunk,),
                in_specs=[
                    whole,
                    whole,
                    whole,
                    pl.BlockSpec((9 * spheres, chunk * spheres), lambda k: (0, k)),
                    pl.BlockSpec((chunk, rows, coefs), lambda k: (k, 0, 0)),
                    whole,
                    whole,
                ],
                out_specs=(whole, whole),
                scratch_shapes=[pltpu.VMEM((rows, 9 * spheres), BF16)],
            )
        return (resident(partial), resident(near), resident(leaf_in)), tables

    window, *prepared = windows()
    inward, tables = apply(halo, column, window, prepared)
    mie_full = tables[3]
    far = tuple(
        resident(item) for item in (receive, cosines, sines, box, leaf_cos, leaf_sin, mie_full)
    )
    vector = resident(vector)
    once, halo, column = call(
        middle_kernel,
        (kept((rows, spheres)), halo_shape, column_shape),
        inward + (resident(send),) + far,
        flops=1 << 26,
    )
    sums = call(sums_kernel, kept((1, 128)), (vector, resident(once)), 1 << 24)
    inward, _ = apply(halo, column, window, None, tables)
    once = resident(once)
    twice, everyone = call(
        last_kernel,
        (kept((rows, spheres)), kept((second_count, 1, 128))),
        (vector, once) + inward + far + (resident(sums),),
        flops=1 << 26,
    )
    everyone = call(
        relay_kernel, kept((first_count, 1, 128)), (resident(exchange(everyone, SECOND)),), 1 << 20
    )
    solved, residual = call(
        solve_kernel,
        (shape((rows, spheres)), shape((rows, spheres))),
        (resident(exchange(everyone, FIRST)), vector, once, resident(twice)),
        flops=1 << 24,
    )
    return solved.reshape(incident.shape), residual.reshape(incident.shape)


def build(devices, sizes):
    torus = Mesh(devices.reshape(sizes), BX + BY)
    placed = (
        P(None, None, BX, BY, None),
        P(None, None, BX, BY, None),
        P(None, BX, BY, None),
        P(BX, BY, None),
        P(),
        P(BX, BY, None, None),
        P(BX, BY, None, None),
        P(),
        P(),
        P(),
        P(BX, BY, None, None),
        P(BX, BY, None, None),
        P(),
    )
    return jax.shard_map(
        local,
        mesh=torus,
        in_specs=placed,
        out_specs=(P(None, None, BX, BY, None), P(None, None, BX, BY, None)),
        check_vma=False,
    )


def solution(mesh):
    return build(mesh.devices, (2, 8, 4, 4, 2))
```

```python
import functools
import math

import jax
import jax.numpy as jnp
import numpy as np
from jax import lax
from jax.experimental import pallas as pl
from jax.experimental.pallas import tpu as pltpu
from jax.sharding import Mesh
from jax.sharding import PartitionSpec as P

BX = ("bx_0", "bx_1")
BY = ("by_0", "by_1", "by_2")
SHORT = ("bx_0", "by_1", "by_2")
LONG = ("by_0", "bx_1")

HIGHEST = lax.Precision.HIGHEST
KAPPA = 1.5
GOLDEN = 2.399963229728653
F32 = jnp.float32
BF16 = jnp.bfloat16
NT = (((1,), (1,)), ((), ()))
TN = (((0,), (0,)), ((), ()))
INTERPRET = False


def call(kernel, out_shape, operands, flops=0, **kw):
    if "specs" in kw:
        kw["in_specs"] = kw.pop("specs")
    elif "grid" not in kw:
        kw["in_specs"] = [
            pl.BlockSpec(memory_space=pltpu.SMEM if op.ndim == 1 else pltpu.VMEM)
            for op in operands
        ]
    return pl.pallas_call(
        kernel,
        out_shape=out_shape,
        interpret=INTERPRET,
        cost_estimate=pl.CostEstimate(flops=flops, transcendentals=0, bytes_accessed=1 << 20),
        **kw,
    )(*operands)


def resident(x):
    return x if INTERPRET else pltpu.with_memory_space_constraint(x, pltpu.VMEM)


def kept(dims, dtype=F32):
    return shape(dims, dtype) if INTERPRET else pltpu.VMEM(dims, dtype)


def shape(dims, dtype=F32):
    return jax.ShapeDtypeStruct(dims, dtype)


def directions(number):
    ordinal = np.arange(number, dtype=np.float64)
    height = 1.0 - (2.0 * ordinal + 1.0) / number
    radius = np.sqrt(1.0 - height * height)
    return np.stack([radius * np.cos(GOLDEN * ordinal), radius * np.sin(GOLDEN * ordinal), height])


def leaf_centers(number):
    ordinal = np.arange(number)
    return np.stack(
        [
            2.0 * (ordinal % 2) - 1.0,
            2.0 * (ordinal // 2 % 2) - 1.0,
            2.0 * (ordinal // 4) - (number // 4 - 1),
        ]
    )


def mie_spread(coef_count, mie_count):
    half_count = coef_count // 2
    table = np.zeros((coef_count, mie_count), np.float32)
    for number in range(coef_count):
        degree = math.isqrt(number % half_count + 1)
        table[number, number // half_count * (mie_count // 2) + degree - 1] = 1.0
    return table


def dot(a, b, dims=(((1,), (0,)), ((), ())), precision=None):
    return lax.dot_general(a, b, dims, precision=precision, preferred_element_type=F32)


def split(x):
    high = x.astype(BF16)
    return high, (x - high.astype(F32)).astype(BF16)


def one_hot(rows, row):
    ordinal = lax.broadcasted_iota(jnp.int32, (rows, row.shape[1]), 0)
    return jnp.where(ordinal == row, 1.0, 0.0)


def emit(vector, pattern, cosines, sines, member, leaf_cos, leaf_sin, halo_ref, column_ref):
    coefs = vector.shape[0] // 2
    boxes, dirs = leaf_cos.shape
    rounded = vector.astype(BF16)
    halo_ref[0, : 2 * coefs, :] = rounded
    by_real = dot(pattern, rounded[:coefs])
    by_imag = dot(pattern, rounded[coefs:])
    real = by_real[:dirs] - by_imag[dirs:]
    imag = by_real[dirs:] + by_imag[:dirs]
    out = jnp.concatenate([real * cosines + imag * sines, imag * cosines - real * sines], axis=0)
    high, low = split(out)
    leaf = dot(member, high, NT) + dot(member, low, NT)
    leaf_real, leaf_imag = leaf[:, :dirs], leaf[:, dirs:]
    halo_ref[0, 2 * coefs : 2 * coefs + boxes, :] = leaf_real.astype(BF16)
    halo_ref[0, 2 * coefs + boxes :, :] = leaf_imag.astype(BF16)
    column_real = jnp.sum(leaf_real * leaf_cos + leaf_imag * leaf_sin, axis=0, keepdims=True)
    column_imag = jnp.sum(leaf_imag * leaf_cos - leaf_real * leaf_sin, axis=0, keepdims=True)
    pair = jnp.concatenate([column_real, column_imag], axis=0)
    column_ref[...] = jnp.broadcast_to(pair[None], column_ref.shape)


def lanes(values):
    lane = lax.broadcasted_iota(jnp.int32, (1, 128), 1)
    row = jnp.zeros((1, 128), F32)
    for place, value in values:
        row = row + jnp.where(lane == place, value, 0.0)
    return row


def inner(a, b):
    return jnp.sum(jnp.sum(a * b, axis=0, keepdims=True), axis=1, keepdims=True)


def first_kernel(
    vector, pattern, offsets, planes, box, leaf_cos, leaf_sin, halo, column, cos_ref, sin_ref, send
):
    turned = jnp.concatenate([pattern[0].T, pattern[1].T], axis=0)
    send[...] = turned
    phases = KAPPA * (
        planes[0] * offsets[0] + planes[1] * offsets[1] + planes[2] * offsets[2]
    )
    cosines, sines = jnp.cos(phases), jnp.sin(phases)
    cos_ref[...] = cosines
    sin_ref[...] = sines
    member = one_hot(leaf_cos.shape[0], box[...]).astype(BF16)
    emit(vector[...], turned, cosines, sines, member, leaf_cos[...], leaf_sin[...], halo, column)


def mirrored(sources, width, flip_x, flip_y):
    line = 3 * width
    flat = jnp.where(sources < line, 0, jnp.where(sources < 2 * line, 1, 2))
    within = sources - line * flat
    side = jnp.where(within < width, 0, jnp.where(within < 2 * width, 1, 2))
    return sources + flip_x * (2 - 2 * flat) * line + flip_y * (2 - 2 * side) * width


def fill_tables(sources, classes, transfer, mie, spread, select, chosen, mie_full):
    boxes, entries = sources.shape
    row = lax.broadcasted_iota(jnp.int32, (boxes, boxes), 0)
    col = lax.broadcasted_iota(jnp.int32, (boxes, boxes), 1)
    unit = jnp.where(row == col, 1.0, 0.0).astype(BF16)
    around = dot(sources[...].astype(F32).astype(BF16), unit, TN)
    kinds = dot(classes[...].astype(F32).astype(BF16), unit, TN)
    box_lane = lax.broadcasted_iota(jnp.int32, (entries, select.shape[1]), 1).astype(F32)
    kind_lane = lax.broadcasted_iota(jnp.int32, (entries, transfer.shape[0]), 1).astype(F32)
    hots = []
    for item in range(boxes):
        at = slice(item * entries, (item + 1) * entries)
        hots.append(jnp.where(kinds[:, item : item + 1] == kind_lane, 1.0, 0.0))
        select[at, :] = jnp.where(around[:, item : item + 1] == box_lane, 1.0, 0.0).astype(BF16)
    hot = jnp.concatenate(hots, axis=0)
    dirs = transfer.shape[2]
    chosen[:, :dirs] = dot(hot, transfer[:, 0, :], precision=HIGHEST)
    chosen[:, dirs:] = dot(hot, transfer[:, 1, :], precision=HIGHEST)
    mie_full[...] = dot(spread[...], mie[...], precision=HIGHEST)


def window_kernel(
    index,
    transfer,
    near_sources,
    far_sources,
    *rest,
    spheres,
    boxes,
    near_z,
    near_x,
    groups,
    run,
    top_x,
    top_y,
):
    copied = len(rest) // 2 - 1
    window, near_out, far_out = rest[copied : copied + 3]
    row, col = lax.div(index[0], near_x * run), lax.rem(index[0], near_x * run)
    flips = lax.rem(row, 2), lax.rem(col, 2)
    near_out[...] = mirrored(near_sources[...], spheres, *flips)
    far_out[...] = mirrored(far_sources[...], boxes, *flips)
    for source, target in zip(rest[:copied], rest[copied + 3 :]):
        target[...] = source[...]
    high, depth = lax.div(row, near_z), lax.rem(row, near_z)
    across, lane = lax.div(col, run), lax.rem(col, run)
    ordinal = lax.broadcasted_iota(jnp.int32, (near_z, 128), 0)
    for group in range(groups):
        start = (high - group) * near_z - depth
        apart_x = jnp.abs(ordinal + start)
        for other in range(run):
            for x in range(near_x):
                shift = (x - across) * run + lane - other
                keep = (apart_x >= 2) | (jnp.abs(shift) >= 2)
                for part in range(2):
                    rows = transfer[pl.ds(start + top_x, near_z), shift + top_y, part, :]
                    window[part, group * run + other, x * near_z : (x + 1) * near_z, :] = jnp.where(
                        keep, rows, 0.0
                    )


def coarse_kernel(columns, window, partial):
    real, imag = columns[:, 0, :][None], columns[:, 1, :][None]
    partial[:, 0, :] = jnp.sum(real * window[0] - imag * window[1], axis=1)
    partial[:, 1, :] = jnp.sum(imag * window[0] + real * window[1], axis=1)


def near_start(before, own, after, select, chosen, near, leaf_in, columns):
    coefs = near.shape[0] // 2
    spheres = near.shape[1] // 2
    boxes, dirs = leaf_in.shape[0], leaf_in.shape[1] // 2
    leaves = []
    for row in range(3):
        for col, part in enumerate((before, own, after)):
            place = (row * 3 + col) * spheres
            columns[:, place : place + spheres] = part[row, : 2 * coefs, :]
            leaves.append(part[row, 2 * coefs :, :])
    around = jnp.concatenate(
        [
            jnp.concatenate([leaf[:boxes] for leaf in leaves], axis=0),
            jnp.concatenate([leaf[boxes:] for leaf in leaves], axis=0),
        ],
        axis=1,
    )
    picked = dot(select[...], around)
    pick_real, pick_imag = picked[:, :dirs], picked[:, dirs:]
    move_real, move_imag = chosen[:, :dirs], chosen[:, dirs:]
    got_real = pick_real * move_real - pick_imag * move_imag
    got_imag = pick_imag * move_real + pick_real * move_imag
    leaf_in[:, :dirs] = jnp.sum(got_real.reshape(boxes, -1, dirs), axis=1)
    leaf_in[:, dirs:] = jnp.sum(got_imag.reshape(boxes, -1, dirs), axis=1)
    near[...] = jnp.zeros(near.shape, F32)


def near_step(columns, counts, table, near):
    coefs = near.shape[0] // 2
    spheres = near.shape[1] // 2
    gathered = dot(columns[...], counts).astype(BF16)
    total = near[...]
    for item in range(table.shape[0]):
        at = slice(item * spheres, (item + 1) * spheres)
        pair = jnp.concatenate([gathered[:coefs, at], gathered[coefs:, at]], axis=1)
        total = total + dot(table[item], pair)
    near[...] = total


def near_kernel(
    before, own, after, counts, table_hbm, select, chosen, near, leaf_in, columns, block, table, sems
):
    groups, _, wide = block.shape
    chunk = table.shape[0] // groups
    loading = pltpu.make_async_copy(table_hbm, table, sems.at[groups])
    loading.start()
    fetching = []
    for group in range(groups):
        fetch = pltpu.make_async_copy(
            counts.at[:, pl.ds(group * wide, wide)], block.at[group], sems.at[group]
        )
        fetch.start()
        fetching.append(fetch)
    near_start(before, own, after, select, chosen, near, leaf_in, columns)
    loading.wait()
    for group in range(groups):
        fetching[group].wait()
        near_step(columns, block[group], table.at[pl.ds(group * chunk, chunk)], near)


def both_kernel(
    sources,
    far_sources,
    targets,
    kinds,
    transfer,
    mie,
    spread,
    before,
    own,
    after,
    table_hbm,
    near,
    leaf_in,
    counts_hbm,
    select,
    chosen,
    mie_full,
    columns,
    block,
    table,
    sems,
):
    groups, long, wide = block.shape
    spheres = long // 9
    chunk = wide // spheres
    loading = pltpu.make_async_copy(table_hbm, table, sems.at[groups])
    loading.start()
    storing = []
    for group in range(groups):
        for item in range(chunk):
            at = slice(group * chunk + item, group * chunk + item + 1)
            source_hot = one_hot(long, sources[at, :]).astype(BF16)
            target_hot = one_hot(spheres, targets[at, :]).astype(BF16)
            block[group, :, item * spheres : (item + 1) * spheres] = dot(
                source_hot, target_hot, NT
            ).astype(BF16)
        keep = pltpu.make_async_copy(
            block.at[group], counts_hbm.at[:, pl.ds(group * wide, wide)], sems.at[group]
        )
        keep.start()
        storing.append(keep)
        if group == 0:
            fill_tables(far_sources, kinds, transfer, mie, spread, select, chosen, mie_full)
            near_start(before, own, after, select, chosen, near, leaf_in, columns)
            loading.wait()
        near_step(
            columns, block[group], table.at[pl.ds(group * chunk, chunk)], near
        )
    for keep in storing:
        keep.wait()


def arrive(partial, near, leaf_in, receive, cosines, sines, member, leaf_cos, leaf_sin, mie_full):
    _, dirs = leaf_cos.shape
    coefs = near.shape[0] // 2
    column_real = jnp.sum(partial[:, 0, :], axis=0, keepdims=True)
    column_imag = jnp.sum(partial[:, 1, :], axis=0, keepdims=True)
    incoming = leaf_in + jnp.concatenate(
        [
            column_real * leaf_cos - column_imag * leaf_sin,
            column_real * leaf_sin + column_imag * leaf_cos,
        ],
        axis=1,
    )
    high, low = split(incoming)
    spread = dot(high, member, TN) + dot(low, member, TN)
    real, imag = spread[:dirs], spread[dirs:]
    arriving = jnp.concatenate(
        [real * cosines - imag * sines, real * sines + imag * cosines], axis=1
    ).astype(BF16)
    total = near + dot(receive, arriving)
    half = total.shape[1] // 2
    field_real = total[:coefs, :half] - total[coefs:, half:]
    field_imag = total[coefs:, :half] + total[:coefs, half:]
    mie_real, mie_imag = mie_full[:coefs], mie_full[coefs:]
    return jnp.concatenate(
        [
            field_real * mie_real - field_imag * mie_imag,
            field_real * mie_imag + field_imag * mie_real,
        ],
        axis=0,
    )


def sums_kernel(vector, scattered, sums):
    u, d = vector[...], scattered[...]
    sums[...] = lanes([(0, inner(u, u)), (1, inner(u, d)), (2, inner(d, d))])


def middle_kernel(
    partial,
    near,
    leaf_in,
    pattern,
    receive,
    cosines,
    sines,
    box,
    leaf_cos,
    leaf_sin,
    mie_full,
    applied,
    halo,
    column,
):
    member = one_hot(leaf_cos.shape[0], box[...]).astype(BF16)
    scattered = arrive(
        partial[...],
        near[...],
        leaf_in[...],
        receive[...],
        cosines[...],
        sines[...],
        member,
        leaf_cos[...],
        leaf_sin[...],
        mie_full[...],
    )
    applied[...] = scattered
    emit(
        scattered,
        pattern[...],
        cosines[...],
        sines[...],
        member,
        leaf_cos[...],
        leaf_sin[...],
        halo,
        column,
    )


def last_kernel(
    vector,
    scattered,
    partial,
    near,
    leaf_in,
    receive,
    cosines,
    sines,
    box,
    leaf_cos,
    leaf_sin,
    mie_full,
    sums,
    applied,
    everyone,
):
    member = one_hot(leaf_cos.shape[0], box[...]).astype(BF16)
    twice = arrive(
        partial[...],
        near[...],
        leaf_in[...],
        receive[...],
        cosines[...],
        sines[...],
        member,
        leaf_cos[...],
        leaf_sin[...],
        mie_full[...],
    )
    applied[...] = twice
    row = sums[...] + lanes(
        [(3, inner(vector[...], twice)), (4, inner(scattered[...], twice)), (5, inner(twice, twice))]
    )
    everyone[...] = jnp.broadcast_to(row[None], everyone.shape)


def relay_kernel(parts, everyone):
    everyone[...] = jnp.broadcast_to(jnp.sum(parts[...], axis=0, keepdims=True), everyone.shape)


def solve_kernel(parts, vector, scattered, twice, solution, residual):
    row = jnp.sum(parts[...], axis=0)
    lane = lax.broadcasted_iota(jnp.int32, row.shape, 1)

    def total(place):
        value = jnp.sum(jnp.where(lane == place, row, 0.0), axis=1, keepdims=True)
        return jnp.broadcast_to(value, (8, 128))

    uu, ud, dd, ue, de, ee = (total(place) for place in range(6))
    beta = jnp.sqrt(uu)
    along = ud / uu
    across = dd - along * ud
    size = jnp.sqrt(across)
    h00 = 1.0 - along
    h10 = size / beta
    turned = de - along * ue
    h01 = (ue - along * ud) / (size * beta)
    h11 = 1.0 + along - turned / across
    rest_u = ue / uu
    rest_d = turned / across
    left = ee - rest_u * ue - rest_d * turned
    h21 = jnp.sqrt(left) / size
    n00 = h00 * h00 + h10 * h10
    n01 = h00 * h01 + h10 * h11
    n11 = h01 * h01 + h11 * h11 + h21 * h21
    l00 = jnp.sqrt(n00)
    l10 = n01 / l00
    l11 = jnp.sqrt(n11 - l10 * l10)
    m0 = beta * h00 / l00
    m1 = (beta * h01 - l10 * m0) / l11
    y1 = m1 / l11
    y0 = (m0 - l10 * y1) / l00
    z0 = h00 * y0 + h01 * y1
    z1 = h10 * y0 + h11 * y1
    step = y1 / size
    sol_u = y0 / beta + step * along
    sol_d = -step
    res_u = (beta - z0) / beta - z1 / size * along + step * (rest_u - rest_d * along)
    res_d = z1 / size + step * rest_d
    res_e = -step
    u, d, e = vector[...], scattered[...], twice[...]
    solution[...] = sol_u[0:1] * u + sol_d[0:1] * d
    residual[...] = res_u[0:1] * u + res_d[0:1] * d + res_e[0:1] * e


def swap(x, axes, first):
    pairs = [(i, i + 1) for i in range(first, lax.axis_size(axes) - 1, 2)]
    return lax.ppermute(x, axes, pairs + [(j, i) for i, j in pairs])


def exchange(x, axes):
    return lax.all_to_all(x, axes, split_axis=0, concat_axis=0, tiled=True)


def local(
    incident,
    mie,
    offsets,
    sphere_box,
    near_table,
    near_src,
    near_dst,
    pattern,
    receive,
    leaf_transfer,
    far_src,
    far_cls,
    coarse_transfer,
):
    coefs = incident.shape[1]
    spheres = incident.shape[4]
    rows = 2 * coefs
    dirs = pattern.shape[1]
    boxes, entries = far_src.shape[2:]
    classes, pairs = near_src.shape[2:]
    high_count, near_z = lax.axis_size("bx_0"), lax.axis_size("bx_1")
    near_x = lax.axis_size("by_0")
    run = lax.axis_size(("by_1", "by_2"))
    short_count, long_count = lax.axis_size(SHORT), lax.axis_size(LONG)
    index = lax.axis_index(BX + BY).astype(jnp.int32).reshape(1)

    planes = jnp.asarray(directions(dirs)[:, :, None].astype(np.float32))
    centre = KAPPA * (leaf_centers(boxes).T @ directions(dirs))
    leaf_cos = jnp.asarray(np.cos(centre).astype(np.float32))
    leaf_sin = jnp.asarray(np.sin(centre).astype(np.float32))

    vector = incident.reshape(rows, spheres)
    box = sphere_box.reshape(1, spheres)
    pattern = pattern.transpose(0, 2, 1)
    receive = receive.reshape(rows, dirs)

    halo_shape = kept((1, rows + 2 * boxes, spheres), BF16)
    column_shape = kept((long_count, 2, dirs))
    halo, column, cosines, sines, send = call(
        first_kernel,
        (
            halo_shape,
            column_shape,
            kept((dirs, spheres)),
            kept((dirs, spheres)),
            kept((2 * dirs, coefs), BF16),
        ),
        (vector, pattern, offsets.reshape(3, 1, spheres), planes, box, leaf_cos, leaf_sin),
        flops=1 << 26,
    )
    whole = pl.BlockSpec(memory_space=pltpu.VMEM)

    def windows():
        spread = mie_spread(coefs, mie.shape[1])
        zero = np.zeros_like(spread)
        copied = (
            near_dst.reshape(classes, pairs),
            far_cls.reshape(boxes, entries),
            leaf_transfer,
            mie.reshape(2 * mie.shape[1], spheres),
            jnp.asarray(np.block([[spread, zero], [zero, spread]])),
        )
        return call(
            functools.partial(
                window_kernel,
                spheres=spheres,
                boxes=boxes,
                near_z=near_z,
                near_x=near_x,
                groups=high_count,
                run=run,
                top_x=high_count * near_z - 1,
                top_y=near_x * run - 1,
            ),
            (
                kept((2, short_count, long_count, dirs)),
                kept((classes, pairs), jnp.int32),
                kept((boxes, entries), jnp.int32),
            )
            + tuple(kept(item.shape, item.dtype) for item in copied),
            (
                index,
                coarse_transfer.transpose(1, 2, 0, 3),
                near_src.reshape(classes, pairs),
                far_src.reshape(boxes, entries),
            )
            + copied,
            flops=1 << 28,
        )

    def apply(halo, column, window, prepared, tables=None):
        columns = exchange(column, LONG)
        ahead = swap(halo, BX, 0)
        behind = swap(halo, BX, 1)
        line = jnp.concatenate([behind, halo, ahead], axis=0)
        right = swap(line, BY, 0)
        left = swap(line, BY, 1)
        partial = call(
            coarse_kernel,
            kept((short_count, 2, dirs)),
            (resident(columns), resident(window)),
            1 << 24,
        )
        partial = exchange(partial, SHORT)
        lines = resident(left), resident(line), resident(right)
        table = near_table.reshape(classes, rows, coefs)
        sums = (kept((rows, 2 * spheres)), kept((boxes, 2 * dirs)))
        groups = classes // 4
        any_spec = pl.BlockSpec(memory_space=pl.ANY)
        scratch = [
            pltpu.VMEM((rows, 9 * spheres), BF16),
            pltpu.VMEM((groups, 9 * spheres, 4 * spheres), BF16),
            pltpu.VMEM((classes, rows, coefs), BF16),
            pltpu.SemaphoreType.DMA((groups + 1,)),
        ]
        if tables is None:
            near, leaf_in, *tables = call(
                both_kernel,
                sums
                + (
                    shape((9 * spheres, classes * spheres), BF16),
                    kept((boxes * entries, 9 * boxes), BF16),
                    kept((boxes * entries, 2 * dirs)),
                    kept((rows, spheres)),
                ),
                tuple(resident(item) for item in prepared) + lines + (table,),
                flops=1 << 31,
                specs=[whole] * 10 + [any_spec],
                out_specs=(whole, whole, any_spec, whole, whole, whole),
                scratch_shapes=scratch,
            )
        else:
            counts, select, chosen, _ = tables
            near, leaf_in = call(
                near_kernel,
                sums,
                lines + (counts, table, resident(select), resident(chosen)),
                flops=1 << 31,
                specs=[whole] * 3 + [any_spec] * 2 + [whole] * 2,
                out_specs=(whole, whole),
                scratch_shapes=scratch,
            )
        return (resident(partial), resident(near), resident(leaf_in)), tables

    window, *prepared = windows()
    inward, tables = apply(halo, column, window, prepared)
    mie_full = tables[3]
    far = tuple(
        resident(item) for item in (receive, cosines, sines, box, leaf_cos, leaf_sin, mie_full)
    )
    vector = resident(vector)
    once, halo, column = call(
        middle_kernel,
        (kept((rows, spheres)), halo_shape, column_shape),
        inward + (resident(send),) + far,
        flops=1 << 26,
    )
    sums = call(sums_kernel, kept((1, 128)), (vector, resident(once)), 1 << 24)
    inward, _ = apply(halo, column, window, None, tables)
    once = resident(once)
    twice, everyone = call(
        last_kernel,
        (kept((rows, spheres)), kept((short_count, 1, 128))),
        (vector, once) + inward + far + (resident(sums),),
        flops=1 << 26,
    )
    everyone = call(
        relay_kernel, kept((long_count, 1, 128)), (resident(exchange(everyone, SHORT)),), 1 << 20
    )
    solved, residual = call(
        solve_kernel,
        (shape((rows, spheres)), shape((rows, spheres))),
        (resident(exchange(everyone, LONG)), vector, once, resident(twice)),
        flops=1 << 24,
    )
    return solved.reshape(incident.shape), residual.reshape(incident.shape)


def build(devices, sizes):
    torus = Mesh(devices.reshape(sizes), BX + BY)
    placed = (
        P(None, None, BX, BY, None),
        P(None, None, BX, BY, None),
        P(None, BX, BY, None),
        P(BX, BY, None),
        P(),
        P(BX, BY, None, None),
        P(BX, BY, None, None),
        P(),
        P(),
        P(),
        P(BX, BY, None, None),
        P(BX, BY, None, None),
        P(),
    )
    return jax.shard_map(
        local,
        mesh=torus,
        in_specs=placed,
        out_specs=(P(None, None, BX, BY, None), P(None, None, BX, BY, None)),
        check_vma=False,
    )


def solution(mesh):
    return build(mesh.devices, (2, 8, 4, 4, 2))
```
